32 devices in a mesh: dp: 2 (over x), expert: 16 (over z, y, core).
Axes of the slice: x: 2, y: 2, z: 4, core: 2. Of those that a mesh axis runs over, the one named last changes fastest.
Arguments:
- inputs: bfloat16 [4, 1024, 2048], P('dp', 'expert'), may hold values from -6 to 6
- segments: int32 [4, 1024], P('dp'), may hold values from 0 to 2, never falling along the last dimension, each value on 1 to 800 neighbouring positions
- expert_picks: int32 [4, 1024, 6], P('dp', 'expert'), may hold values from 0 to 15, all different within a row
- priority: int32 [4, 1024], P('dp', 'expert'), may hold values from 0 to 1023, each once within a row
- cotangent: bfloat16 [4, 1024, 2048], P('dp', 'expert'), may hold values from -6 to 6
- query_weight: bfloat16 [2048, 3072], P(('dp', 'expert')), may hold values from -0.125 to 0.125
- latent_down: bfloat16 [2048, 576], P(('dp', 'expert')), may hold values from -0.125 to 0.125
- latent_up: bfloat16 [512, 4096], P(('dp', 'expert')), may hold values from -0.25 to 0.25
- output_weight: bfloat16 [2048, 2048], P(None, ('dp', 'expert')), may hold values from -0.75 to 0.75
- attn_gain: bfloat16 [2048], P(('dp', 'expert')), may hold values from 0.25 to 1.75
- latent_gain: bfloat16 [512], P(('dp', 'expert')), may hold values from 0.25 to 1.75
- router_weight: bfloat16 [2048, 16], P(('dp', 'expert')), may hold values from -0.25 to 0.25
- shared_gate: bfloat16 [2048, 2816], P(('dp', 'expert')), may hold values from -0.125 to 0.125
- shared_up: bfloat16 [2048, 2816], P(('dp', 'expert')), may hold values from -0.125 to 0.125
- shared_down: bfloat16 [2816, 2048], P(('dp', 'expert')), may hold values from -0.21875 to 0.21875
- moe_gain: bfloat16 [2048], P(('dp', 'expert')), may hold values from 0.25 to 1.75
- expert_gate: bfloat16 [16, 2048, 1408], P('expert', 'dp'), may hold values from -0.125 to 0.125
- expert_up: bfloat16 [16, 2048, 1408], P('expert', 'dp'), may hold values from -0.125 to 0.125
- expert_down: bfloat16 [16, 1408, 2048], P('expert', 'dp'), may hold values from -0.625 to 0.625
Outputs:
- outputs: bfloat16 [4, 1024, 2048], P('dp', 'expert')
- input_grad: bfloat16 [4, 1024, 2048], P('dp', 'expert')
- query_weight_grad: float32 [2048, 3072], P(('dp', 'expert'))
- latent_down_grad: float32 [2048, 576], P(('dp', 'expert'))
- latent_up_grad: float32 [512, 4096], P(('dp', 'expert'))
- output_weight_grad: float32 [2048, 2048], P(None, ('dp', 'expert'))
- attn_gain_grad: float32 [2048], P(('dp', 'expert'))
- latent_gain_grad: float32 [512], P(('dp', 'expert'))
- router_weight_grad: float32 [2048, 16], P(('dp', 'expert'))
- shared_gate_grad: float32 [2048, 2816], P(('dp', 'expert'))
- shared_up_grad: float32 [2048, 2816], P(('dp', 'expert'))
- shared_down_grad: float32 [2816, 2048], P(('dp', 'expert'))
- moe_gain_grad: float32 [2048], P(('dp', 'expert'))
- expert_gate_grad: float32 [16, 2048, 1408], P('expert', 'dp')
- expert_up_grad: float32 [16, 2048, 1408], P('expert', 'dp')
- expert_down_grad: float32 [16, 1408, 2048], P('expert', 'dp')
The draws below stay inside these ranges and needn't reach their ends.
Inputs may be any that keep to these rules, and one draw needn't show every extreme that they name: `segments`: along each sequence the segment numbers never fall; a document has 1 to 800 tokens and some document has exactly 800. `expert_picks`: each token names 6 different experts; every expert is named by some token. `priority`: in each sequence every number of 0 to 1023 appears once.
All inputs are finite; a program needn't handle non-finite values.
Results may differ from the reference program's by a relative error of at most 0.024.
Values may be sent and summed in bfloat16 or wider, within the bound.
A program may use at most 448 MiB of HBM per device.

```python
import math
import jax
import jax.numpy as jnp
import numpy as np
from jax import lax

D = 2048
HEADS = 16
HD = 128
RD = 64
VD = 128
RANK = 512
FF_E = 1408
SHARED = 2816
TOP = 6
DOC_MOST = 800
SPAN = 64
LENGTH = 1024
SEQS = 4
EXPERTS = 16
DOCS = 3
CAP = 27
N_EXPERT = 16


def shard_levels(key, dims, pieces, smallest, largest):
    level = 1.0
    for axis_at, shards_of in pieces:
        heights = jax.random.uniform(jax.random.fold_in(jax.random.fold_in(key, 6), axis_at), (shards_of,), jnp.float32, smallest / len(pieces), largest / len(pieces))
        level = level * jnp.repeat(jnp.exp(heights), dims[axis_at] // shards_of).reshape((-1,) + (1,) * (len(dims) - 1 - axis_at))
    return level


def different_ones(key, rows, amount, top, lift):
    sequence = jax.random.permutation(jax.random.fold_in(key, 1), amount)
    boost = sequence
    for power in range(3):
        boost = boost * boost // amount
    boost = boost * lift // amount
    chance = jax.random.randint(jax.random.fold_in(key, 2), (rows, amount), 0, 4096) + boost
    fixed_rows = jax.random.permutation(jax.random.fold_in(key, 3), rows)[jnp.arange(amount) % rows]
    chance = jnp.where(jnp.arange(rows)[:, None] == fixed_rows[None, :], 1 << 14, chance)
    score = chance * amount + jnp.arange(amount)
    return lax.top_k(score.astype(jnp.int32), top)[1].astype(jnp.int32)


def profile(amount, total, limit, lean):
    weights = [(1 << 20) // math.isqrt(standing ** lean) + 1 for standing in range(2, amount + 1)]
    spare, given = total - limit - (amount - 1), [1] * (amount - 1)
    while spare > 0:
        candidates = [i for i in range(amount - 1) if given[i] < limit]
        pool, remaining = sum([weights[i] for i in candidates]), spare
        for i in candidates:
            extra = min(limit - given[i], max(1, remaining * weights[i] // pool), spare)
            given[i] = given[i] + extra
            spare = spare - extra
    return np.array([limit] + given)


def ragged(rng, amount, total, limit, skew):
    if amount == 2:
        one = jax.random.randint(rng, (), max(1, total - limit), min(limit, total - 1) + 1)
        return jnp.stack([one, total - one])
    lengths = jnp.asarray(profile(amount, total, limit, skew), jnp.int32)
    twos = (amount - 1) // 2
    donor, taker = lengths[1:1 + 2 * twos:2], lengths[2:2 + 2 * twos:2]
    room = jnp.minimum(donor - 1, limit - taker)
    shifted = jax.random.randint(jax.random.fold_in(rng, 1), (twos,), 0, 1 << 20) % (room + 1)
    lengths = lengths.at[1:1 + 2 * twos:2].set(donor - shifted).at[2:2 + 2 * twos:2].set(taker + shifted)
    return lengths[jax.random.permutation(jax.random.fold_in(rng, 2), amount)]


def bell_draw(stream_key, shape, scale, bound, split=(), kind=jnp.bfloat16):
    level = shard_levels(stream_key, shape, split, -0.22, 0.18) if split else 1.0
    array = jax.random.normal(stream_key, shape, jnp.float32) * scale * level
    return jnp.minimum(jnp.maximum(array, -bound), bound).astype(kind)


def setup_inputs(seed: int = 0) -> dict:
    keys = jax.random.split(jax.random.key(seed), 20)
    inputs = bell_draw(keys[0], (SEQS, LENGTH, D), 1.0, 6.0, ((0, 2), (1, 16)))
    segments = jax.vmap(lambda own: jnp.searchsorted(jnp.cumsum(ragged(own, DOCS, LENGTH, DOC_MOST, 2)), jnp.arange(LENGTH), side="right"))(jax.random.split(keys[1], SEQS)).reshape((SEQS, LENGTH)).astype(jnp.int32)
    expert_picks = different_ones(keys[2], SEQS * LENGTH, EXPERTS, TOP, 3072).reshape((SEQS, LENGTH, TOP))
    priority = jax.vmap(lambda own: jax.random.permutation(own, LENGTH))(jax.random.split(keys[3], SEQS)).reshape((SEQS, LENGTH)).astype(jnp.int32)
    cotangent = bell_draw(keys[4], (SEQS, LENGTH, D), 1.0, 6.0, ((0, 2), (1, 16)))
    query_weight = bell_draw(keys[5], (D, HEADS * (HD + RD)), D ** -0.5, 0.125, ((0, 32),))
    latent_down = bell_draw(keys[6], (D, RANK + RD), D ** -0.5, 0.125, ((0, 32),))
    latent_up = bell_draw(keys[7], (RANK, HEADS * (HD + VD)), RANK ** -0.5, 0.25, ((0, 32),))
    output_weight = bell_draw(keys[8], (HEADS * VD, D), (HEADS * VD // 32) ** -0.5, 0.75, ((1, 32),))
    attn_gain = jnp.clip(1.0 + 0.15 * jax.random.normal(keys[9], (D,), jnp.float32), 0.25, 1.75).astype(jnp.bfloat16)
    latent_gain = jnp.clip(1.0 + 0.15 * jax.random.normal(keys[10], (RANK,), jnp.float32), 0.25, 1.75).astype(jnp.bfloat16)
    router_weight = bell_draw(keys[11], (D, EXPERTS), (D // 4) ** -0.5, 0.25, ((0, 32),))
    shared_gate = bell_draw(keys[12], (D, SHARED), D ** -0.5, 0.125, ((0, 32),))
    shared_up = bell_draw(keys[13], (D, SHARED), D ** -0.5, 0.125, ((0, 32),))
    shared_down = bell_draw(keys[14], (SHARED, D), (SHARED // 4) ** -0.5, 0.21875, ((0, 32),))
    moe_gain = jnp.clip(1.0 + 0.15 * jax.random.normal(keys[15], (D,), jnp.float32), 0.25, 1.75).astype(jnp.bfloat16)
    expert_gate = bell_draw(keys[16], (EXPERTS, D, FF_E), D ** -0.5, 0.125, ((0, 16), (1, 2)))
    expert_up = bell_draw(keys[17], (EXPERTS, D, FF_E), D ** -0.5, 0.125, ((0, 16), (1, 2)))
    expert_down = bell_draw(keys[18], (EXPERTS, FF_E, D), (FF_E // 16) ** -0.5, 0.625, ((0, 16), (1, 2)))
    return dict(inputs=inputs, segments=segments, expert_picks=expert_picks, priority=priority, cotangent=cotangent, query_weight=query_weight, latent_down=latent_down, latent_up=latent_up, output_weight=output_weight, attn_gain=attn_gain, latent_gain=latent_gain, router_weight=router_weight, shared_gate=shared_gate, shared_up=shared_up, shared_down=shared_down, moe_gain=moe_gain, expert_gate=expert_gate, expert_up=expert_up, expert_down=expert_down)


epsilon = 1e-06
highest = lax.Precision.HIGHEST
masked_score = -1e+30

@jax.custom_vjp
def low(v):
    return lax.optimization_barrier(v.astype(jnp.bfloat16)).astype(jnp.float32)

@jax.custom_vjp
def low_back(v):
    return v

def low_keep(v):
    return (low(v), None)

def low_pass(kept, grad):
    return (grad,)

def back_keep(v):
    return (v, None)

def back_low(kept, grad):
    return (low(grad),)
low.defvjp(low_keep, low_pass)
low_back.defvjp(back_keep, back_low)

def matmul(left, right):
    return jnp.dot(left, right, precision=highest, preferred_element_type=jnp.float32)

def rms_scale(values, gain):
    return values * lax.rsqrt(lax.optimization_barrier(jnp.mean(values * values, axis=-1, keepdims=True)) + epsilon) * gain

def rotate(values, positions):
    width = values.shape[-1]
    half_width = width // 2
    freqs = jnp.power(10000.0, -2.0 * jnp.arange(half_width, dtype=jnp.float32) / width)
    angles = positions.astype(jnp.float32)[:, None] * freqs[None, :]
    cosine = jnp.cos(angles)
    sine = jnp.sin(angles)
    if values.ndim == 3:
        cosine = cosine[:, None, :]
        sine = sine[:, None, :]
    first = values[..., :half_width]
    second = values[..., half_width:]
    return jnp.concatenate([first * cosine - second * sine, second * cosine + first * sine], axis=-1)

def route_block(picks_rows, order_rows):
    hit = lax.optimization_barrier(jnp.sum((picks_rows[:, :, None] == jnp.arange(EXPERTS, dtype=jnp.int32)[None, None, :]).astype(jnp.float32), axis=1))
    earlier = (order_rows[None, :] < order_rows[:, None]).astype(jnp.float32)
    ranks = matmul(earlier, hit)
    kept = hit * (ranks < CAP).astype(jnp.float32)
    table = kept[:, :, None] * (ranks[:, :, None] == jnp.arange(CAP, dtype=jnp.float32)[None, None, :]).astype(jnp.float32)
    return table.reshape(SPAN, EXPERTS * CAP)

def attend_sequence(tokens_seq, seg_seq, query_weight, latent_down, latent_up, output_weight, attn_gain, latent_gain):
    positions = jnp.arange(LENGTH, dtype=jnp.int32)
    h_one = low(rms_scale(tokens_seq, attn_gain))
    query_raw = low_back(matmul(h_one, query_weight)).reshape(LENGTH, HEADS, HD + RD)
    query = low(jnp.concatenate([query_raw[..., :HD], rotate(query_raw[..., HD:], positions)], axis=-1))
    down = low_back(matmul(h_one, latent_down))
    latent = low(jnp.concatenate([rms_scale(down[:, :RANK], latent_gain), rotate(down[:, RANK:], positions)], axis=-1))
    scale = 1.0 / math.sqrt(HD + RD)

    def one_block(index):
        start = (index * SPAN).astype(jnp.int32)
        query_rows = lax.dynamic_slice_in_dim(query, start, SPAN, 0)
        seg_rows = lax.dynamic_slice_in_dim(seg_seq, start, SPAN, 0)
        expanded = low(low_back(matmul(latent[:, :RANK], latent_up))).reshape(LENGTH, HEADS, HD + VD)
        both = jnp.einsum('chd,lhd->hcl', query_rows[..., :HD], expanded[..., :HD], precision=highest)
        both = both + jnp.einsum('chr,lr->hcl', query_rows[..., HD:], latent[:, RANK:], precision=highest)
        query_pos = start + jnp.arange(SPAN, dtype=jnp.int32)
        key_mask = (positions[None, :] <= query_pos[:, None]) & (seg_seq[None, :] == seg_rows[:, None])
        scores = jnp.where(key_mask[None], low_back(both) * scale, masked_score)
        probs = jax.nn.softmax(scores, axis=-1)
        heads = jnp.einsum('hcl,lhd->chd', low(probs), expanded[..., HD:], precision=highest)
        return heads.reshape(SPAN, HEADS * VD)
    heads_all = lax.map(jax.checkpoint(one_block), jnp.arange(N_EXPERT, dtype=jnp.int32)).reshape(LENGTH, HEADS * VD)
    heads_all = low(low_back(heads_all))
    return tokens_seq + low_back(matmul(heads_all, output_weight))

def forward(inputs, query_weight, latent_down, latent_up, output_weight, attn_gain, latent_gain, router_weight, shared_gate, shared_up, shared_down, moe_gain, expert_gate, expert_up, expert_down, segments, table):

    def one_sequence(pair):
        return attend_sequence(pair[0], pair[1], query_weight, latent_down, latent_up, output_weight, attn_gain, latent_gain)
    x_one = lax.map(jax.checkpoint(one_sequence), (inputs, segments))
    flat = x_one.reshape(SEQS * LENGTH, D)
    h_two = low(rms_scale(flat, moe_gain))
    gate_probs = jax.nn.softmax(low_back(matmul(h_two, router_weight)), axis=-1)
    blocks = SEQS * N_EXPERT
    sent = low_back(jnp.einsum('ntk,ntd->nkd', table, h_two.reshape(blocks, SPAN, D), precision=highest))
    expert_rows = sent.reshape(blocks, EXPERTS, CAP, D).transpose(1, 0, 2, 3).reshape(EXPERTS, blocks * CAP, D)

    def one_expert(group):
        rows_in, gate_e, up_e, down_e = group
        gate_pre = low_back(matmul(rows_in, gate_e))
        up_pre = low_back(matmul(rows_in, up_e))
        hidden = low(jax.nn.silu(gate_pre) * up_pre)
        return low_back(low(matmul(hidden, down_e)))
    results = lax.map(jax.checkpoint(one_expert), (expert_rows, expert_gate, expert_up, expert_down))
    results = results.reshape(EXPERTS, blocks, CAP, D).transpose(1, 0, 2, 3).reshape(blocks, EXPERTS * CAP, D)
    slot_weights = table * jnp.repeat(gate_probs.reshape(blocks, SPAN, EXPERTS), CAP, axis=-1)
    routed = jnp.einsum('ntk,nkd->ntd', slot_weights, results, precision=highest).reshape(SEQS * LENGTH, D)
    shared_a = low_back(matmul(h_two, shared_gate))
    shared_b = low_back(matmul(h_two, shared_up))
    shared_hidden = low(jax.nn.silu(shared_a) * shared_b)
    shared_out = low_back(matmul(shared_hidden, shared_down))
    return (flat + shared_out + routed).reshape(SEQS, LENGTH, D)

def reference(inputs, segments, expert_picks, priority, cotangent, query_weight, latent_down, latent_up, output_weight, attn_gain, latent_gain, router_weight, shared_gate, shared_up, shared_down, moe_gain, expert_gate, expert_up, expert_down):
    blocks = SEQS * N_EXPERT
    table = jax.vmap(route_block)(expert_picks.reshape(blocks, SPAN, TOP), priority.reshape(blocks, SPAN))
    floats = tuple((value.astype(jnp.float32) for value in (inputs, query_weight, latent_down, latent_up, output_weight, attn_gain, latent_gain, router_weight, shared_gate, shared_up, shared_down, moe_gain, expert_gate, expert_up, expert_down)))

    def wrapped(*values):
        return forward(*values, segments, table)
    result, pull = jax.vjp(wrapped, *floats)
    grads = pull(cotangent.astype(jnp.float32))
    return (result.astype(jnp.bfloat16), grads[0].astype(jnp.bfloat16), grads[1], grads[2], grads[3], grads[4], grads[5], grads[6], grads[7], grads[8], grads[9], grads[10], grads[11], grads[12], grads[13], grads[14])
```

```python
import functools
import math

import jax
import jax.numpy as jnp
from jax import lax
from jax.experimental import pallas as pl
from jax.experimental.pallas import tpu as pltpu
from jax.sharding import PartitionSpec as P

HEADS = 16
HD = 128
RD = 64
VD = 128
RANK = 512
TOP = 6

epsilon = 1e-06
masked_score = -1e30
DP = "dp"
EXPERT = "expert"
BOTH = (DP, EXPERT)
TOKENS = P(DP, EXPERT, None)
ROWS = P(BOTH, None)
ROUTED = P(EXPERT, DP, None)
f32 = jnp.float32
bf16 = jnp.bfloat16


def product(left, right):
    return jnp.dot(left, right, preferred_element_type=f32)


def left_product(left, right):
    return lax.dot_general(left, right, (((0,), (0,)), ((), ())), preferred_element_type=f32)


def right_product(left, right):
    return lax.dot_general(left, right, (((1,), (1,)), ((), ())), preferred_element_type=f32)


def einsum(spec, left, right):
    return jnp.einsum(spec, left, right, preferred_element_type=f32)


def norm_parts(values):
    factor = lax.rsqrt(jnp.mean(values * values, axis=-1, keepdims=True) + epsilon)
    return (values * factor, factor)


def norm_back(grad_normed, normed, factor):
    return factor * (grad_normed - normed * jnp.mean(grad_normed * normed, axis=-1, keepdims=True))


def angle_tables(positions, width):
    half = width // 2
    freqs = jnp.power(10000.0, -2.0 * jnp.arange(half, dtype=f32) / width)
    angles = positions.astype(f32)[:, None] * freqs[None, :]
    return (jnp.cos(angles), jnp.sin(angles))


def rotate(values, tables):
    half = values.shape[-1] // 2
    cosine, sine = tables
    first = values[..., :half]
    second = values[..., half:]
    return jnp.concatenate(
        [first * cosine - second * sine, second * cosine + first * sine], axis=-1
    )


def unrotate(grads, tables):
    half = grads.shape[-1] // 2
    cosine, sine = tables
    first = grads[..., :half]
    second = grads[..., half:]
    return jnp.concatenate(
        [first * cosine + second * sine, second * cosine - first * sine], axis=-1
    )


def silu_slope(pre):
    sigma = jax.nn.sigmoid(pre)
    return sigma * (1.0 + pre * (1.0 - sigma))


def dp_swap(value):
    return lax.ppermute(value, DP, [(0, 1), (1, 0)])


def dp_gather(value):
    if lax.axis_size(DP) == 2:
        other = dp_swap(value)
        first = lax.axis_index(DP) == 0
        return jnp.concatenate(
            [jnp.where(first, value, other), jnp.where(first, other, value)], axis=0
        )
    return lax.all_gather(value, DP, axis=0, tiled=True)


def dp_scatter_product(left, right):
    if lax.axis_size(DP) == 2:
        first = lax.axis_index(DP) == 0
        half = left.shape[1] // 2
        low, high = left[:, :half], left[:, half:]
        sent = left_product(jnp.where(first, high, low), right).astype(bf16)
        other = dp_swap(sent)
        return left_product(jnp.where(first, low, high), right) + other.astype(f32)
    return dp_scatter(left_product(left, right))


def dp_scatter(value):
    if lax.axis_size(DP) == 2:
        rows = value.shape[0] // 2
        at = lax.axis_index(DP)
        sent = lax.dynamic_slice_in_dim(value, (1 - at) * rows, rows, 0)
        kept = lax.dynamic_slice_in_dim(value, at * rows, rows, 0)
        return kept + dp_swap(sent.astype(bf16)).astype(f32)
    return lax.psum_scatter(
        value.astype(bf16), DP, scatter_dimension=0, tiled=True
    ).astype(f32)


def expert_swap(value):
    return lax.all_to_all(value, EXPERT, split_axis=0, concat_axis=0, tiled=True)


def gather_rows(value, axes):
    return lax.all_gather(value, axes, axis=0, tiled=True)


def scatter_rows(value, axes):
    return lax.psum_scatter(value, axes, scatter_dimension=0, tiled=True)


MESH = pl.DeviceIdType.MESH


def at_expert(index):
    return {EXPERT: index}


def grid_place():
    me = lax.axis_index(EXPERT)
    return me, me // 4, (me // 2) % 2, me % 2


def greet_neighbours(me, line, pair, core):
    partner = me + 1 - 2 * core
    mate = me + 2 - 4 * pair
    barrier = pltpu.get_barrier_semaphore()
    for other in (partner, mate):
        pl.semaphore_signal(barrier, inc=1, device_id=at_expert(other), device_id_type=MESH)

    @pl.when(line < 3)
    def _():
        pl.semaphore_signal(barrier, inc=1, device_id=at_expert(me + 4), device_id_type=MESH)

    @pl.when(line > 0)
    def _():
        pl.semaphore_signal(barrier, inc=1, device_id=at_expert(me - 4), device_id_type=MESH)

    pl.semaphore_wait(barrier, 3 + jnp.where((line > 0) & (line < 3), 1, 0))
    return partner, mate


def gather_kernel(x_ref, out_ref, own_sem, send_sem, recv_sem):
    me, line, pair, core = grid_place()
    partner, mate = greet_neighbours(me, line, pair, core)
    own = pltpu.make_async_copy(x_ref, out_ref.at[me], own_sem)
    own.start()

    def copy(source, origin, way, to):
        return pltpu.make_async_remote_copy(
            src_ref=source,
            dst_ref=out_ref.at[origin],
            send_sem=send_sem.at[origin, way],
            recv_sem=recv_sem.at[origin],
            device_id=at_expert(to),
            device_id_type=MESH,
        )

    def arrived(origin):
        copy(out_ref.at[origin], origin, 0, partner).wait_recv()

    def along(origin, source, upward, downward, act):
        if upward:

            @pl.when(line < 3)
            def _():
                act(copy(source, origin, 0, me + 4))

        if downward:

            @pl.when(line > 0)
            def _():
                act(copy(source, origin, 1, me - 4))

        act(copy(source, origin, 2, mate))
        act(copy(source, origin, 3, partner))

    def walk(act, wait):
        along(me, x_ref, True, True, act)
        for far in range(1, 5):
            if far < 4:

                @pl.when(line >= far)
                def _():
                    origin = me - 4 * far
                    wait(origin)
                    along(origin, out_ref.at[origin], True, False, act)

                @pl.when(line + far <= 3)
                def _():
                    origin = me + 4 * far
                    wait(origin)
                    along(origin, out_ref.at[origin], False, True, act)

            for sign in (-1, 1) if far > 1 else (1,):
                step = sign * (far - 1)

                @pl.when((line + step >= 0) & (line + step <= 3))
                def _():
                    origin = mate + 4 * step
                    wait(origin)
                    act(copy(out_ref.at[origin], origin, 3, partner))

    walk(lambda c: c.start(), arrived)
    for index in range(8):
        arrived(2 * index + 1 - core)
    walk(lambda c: c.wait_send(), lambda origin: None)
    own.wait()


def ring_gather(value, collective):
    rows, columns = value.shape
    sent = 15 * rows * columns * 2
    out = pl.pallas_call(
        gather_kernel,
        out_shape=jax.ShapeDtypeStruct((16, rows, columns), value.dtype),
        in_specs=[pl.BlockSpec(memory_space=pltpu.VMEM)],
        out_specs=pl.BlockSpec(memory_space=pl.ANY),
        scratch_shapes=[
            pltpu.SemaphoreType.DMA,
            pltpu.SemaphoreType.DMA((16, 4)),
            pltpu.SemaphoreType.DMA((16,)),
        ],
        compiler_params=pltpu.CompilerParams(collective_id=collective, has_side_effects=True),
        cost_estimate=pl.CostEstimate(flops=0, bytes_accessed=16 * sent, transcendentals=0),
    )(value)
    return out.reshape(16 * rows, columns)


def scatter_kernel(
    p_ref, out_ref, chip, mate_in, up_in, down_in, total,
    core_send, core_recv, mate_send, mate_recv, up_send, up_recv, down_send, down_recv,
):
    me, line, pair, core = grid_place()
    partner, mate = greet_neighbours(me, line, pair, core)
    rows = p_ref.shape[1]
    tile = 16

    def remote(source, target, send, recv, to):
        return pltpu.make_async_remote_copy(
            src_ref=source, dst_ref=target, send_sem=send, recv_sem=recv,
            device_id=at_expert(to), device_id_type=MESH,
        )

    def core_copy(index):
        return remote(
            p_ref.at[2 * index + 1 - core], chip.at[index],
            core_send.at[index], core_recv.at[index], partner,
        )

    def mate_copy(dest):
        return remote(
            total.at[2 * dest + 1 - pair], mate_in.at[dest],
            mate_send.at[dest], mate_recv.at[dest], mate,
        )

    def up_copy(dest):
        return remote(
            total.at[2 * dest + pair], up_in.at[dest], up_send.at[dest], up_recv.at[dest], me + 4
        )

    def down_copy(dest):
        return remote(
            total.at[2 * dest + pair], down_in.at[dest],
            down_send.at[dest], down_recv.at[dest], me - 4,
        )

    def add(target, left, right):
        @pl.loop(0, rows // tile)
        def _(i):
            at = pl.ds(pl.multiple_of(i * tile, tile), tile)
            target[at, :] = (left[at, :].astype(f32) + right[at, :].astype(f32)).astype(
                target.dtype
            )

    def farthest(act):
        for far in (3, 2, 1, 0):
            for step in (-far, far) if far else (0,):

                @pl.when((line + step >= 0) & (line + step <= 3))
                def _():
                    act(line + step, step)

    def send_core(dest, step):
        core_copy(2 * dest + 1 - pair).start()

    def send_core_own(dest, step):
        core_copy(2 * dest + pair).start()

    def chip_sum(index):
        core_copy(index).wait_recv()
        add(total.at[index], p_ref.at[2 * index + core], chip.at[index])

    def to_mate(dest, step):
        chip_sum(2 * dest + 1 - pair)
        mate_copy(dest).start()

    def keep(dest, step):
        chip_sum(2 * dest + pair)

    def along(dest, step):
        mine = total.at[2 * dest + pair]
        mate_copy(dest).wait_recv()
        if step == 0:
            mine, kept = out_ref, mine
            add(mine, kept, mate_in.at[dest])
        else:
            add(mine, mine, mate_in.at[dest])
        if step > 0:

            @pl.when(line > 0)
            def _():
                up_copy(dest).wait_recv()
                add(mine, mine, up_in.at[dest])

            up_copy(dest).start()
        elif step < 0:

            @pl.when(line < 3)
            def _():
                down_copy(dest).wait_recv()
                add(mine, mine, down_in.at[dest])

            down_copy(dest).start()
        else:

            @pl.when(line > 0)
            def _():
                up_copy(dest).wait_recv()
                add(mine, mine, up_in.at[dest])

            @pl.when(line < 3)
            def _():
                down_copy(dest).wait_recv()
                add(mine, mine, down_in.at[dest])

    def finish(dest, step):
        mate_copy(dest).wait_send()
        core_copy(2 * dest + 1 - pair).wait_send()
        core_copy(2 * dest + pair).wait_send()
        if step > 0:
            up_copy(dest).wait_send()
        elif step < 0:
            down_copy(dest).wait_send()

    farthest(send_core)
    farthest(send_core_own)
    farthest(to_mate)
    farthest(keep)
    farthest(along)
    farthest(finish)


def ring_scatter(value, collective):
    rows, columns = value.shape[0] // 16, value.shape[1]
    block = lambda n: pltpu.VMEM((n, rows, columns), bf16)
    sems = lambda n: pltpu.SemaphoreType.DMA((n,))
    sent = 15 * rows * columns * 2
    return pl.pallas_call(
        scatter_kernel,
        out_shape=jax.ShapeDtypeStruct((rows, columns), f32),
        in_specs=[pl.BlockSpec(memory_space=pltpu.VMEM)],
        out_specs=pl.BlockSpec(memory_space=pltpu.VMEM),
        scratch_shapes=[block(8), block(4), block(4), block(4), block(8)]
        + [sems(8), sems(8), sems(4), sems(4), sems(4), sems(4), sems(4), sems(4)],
        compiler_params=pltpu.CompilerParams(collective_id=collective, has_side_effects=True),
        cost_estimate=pl.CostEstimate(flops=0, bytes_accessed=16 * sent, transcendentals=0),
    )(value.reshape(16, rows, columns))


def swap_kernel(source, target, x_ref, out_ref, own_sem, send_sem, recv_sem):
    me = lax.axis_index(EXPERT)
    barrier = pltpu.get_barrier_semaphore()
    for step in range(1, 16):
        pl.semaphore_signal(
            barrier, inc=1, device_id=at_expert((me + step) % 16), device_id_type=MESH
        )
    pl.semaphore_wait(barrier, 15)

    def copy(step):
        to = (me + step) % 16
        return pltpu.make_async_remote_copy(
            src_ref=source(x_ref, to),
            dst_ref=target(out_ref, me),
            send_sem=send_sem.at[step],
            recv_sem=recv_sem.at[step],
            device_id=at_expert(to),
            device_id_type=MESH,
        )

    for step in range(1, 16):
        copy(step).start()
    own = pltpu.make_async_copy(source(x_ref, me), target(out_ref, me), own_sem)
    own.start()
    for step in range(1, 16):
        copy(step).wait()
    own.wait()


def swap_call(source, target, value, shape, collective):
    sent = value.size * 2
    return pl.pallas_call(
        functools.partial(swap_kernel, source, target),
        out_shape=jax.ShapeDtypeStruct(shape, value.dtype),
        in_specs=[pl.BlockSpec(memory_space=pltpu.VMEM)],
        out_specs=pl.BlockSpec(memory_space=pltpu.VMEM),
        scratch_shapes=[
            pltpu.SemaphoreType.DMA,
            pltpu.SemaphoreType.DMA((16,)),
            pltpu.SemaphoreType.DMA((16,)),
        ],
        compiler_params=pltpu.CompilerParams(collective_id=collective, has_side_effects=True),
        cost_estimate=pl.CostEstimate(flops=0, bytes_accessed=64 * sent, transcendentals=0),
    )(value)


def block_rows(span):
    return lambda ref, at: ref.at[:, pl.ds(pl.multiple_of(at * span, span), span), :]


def head_columns(columns):
    return lambda ref, at: ref.at[:, :, pl.ds(pl.multiple_of(at * columns, columns), columns)]


def heads_to_tokens(value, span, collective):
    seqs = value.shape[0]
    return swap_call(
        block_rows(span), head_columns(VD), value, (seqs, span, HEADS * VD), collective
    )


def tokens_to_heads(value, collective):
    seqs, span, _ = value.shape
    return swap_call(
        head_columns(VD), block_rows(span), value, (seqs, span * HEADS, VD), collective
    )


def per_device(
    inputs,
    segments,
    expert_picks,
    priority,
    cotangent,
    query_weight,
    latent_down,
    latent_up,
    output_weight,
    attn_gain,
    latent_gain,
    router_weight,
    shared_gate,
    shared_up,
    shared_down,
    moe_gain,
    expert_gate,
    expert_up,
    expert_down,
):
    groups = lax.axis_size(EXPERT)
    replicas = lax.axis_size(DP)
    place = lax.axis_index(EXPERT)
    seqs, span, width = inputs.shape
    length = span * groups
    own = seqs * span
    tokens = own * groups
    experts = groups
    capacity = (9 * span * TOP + 8 * experts - 1) // (8 * experts)
    scale = 1.0 / math.sqrt(HD + RD)
    rows = query_weight.shape[0]
    part = shared_down.shape[0]
    hidden_own = part * replicas
    QD = HD + RD

    def by_sequence(value):
        return value.reshape(groups, seqs, span, -1).transpose(1, 0, 2, 3).reshape(
            seqs, length, -1
        )

    def by_block(value):
        return value.reshape(seqs, groups, span, -1).transpose(1, 0, 2, 3).reshape(tokens, -1)

    x_low = inputs.reshape(own, width)
    x_all = gather_rows(x_low, EXPERT)
    cot_own = cotangent.reshape(own, width)

    order = priority[:, None, :] < priority[:, :, None]
    hit = jnp.sum(
        (expert_picks[..., None] == jnp.arange(experts, dtype=jnp.int32)).astype(f32), axis=2
    )
    ranks = einsum("stu,sue->ste", order.astype(bf16), hit.astype(bf16))
    codes = jnp.where((hit > 0) & (ranks < capacity), ranks, -1.0).astype(bf16)

    pad = rows - latent_gain.shape[0]
    small = jnp.concatenate(
        [
            latent_down,
            router_weight,
            attn_gain[:, None],
            moe_gain[:, None],
            jnp.pad(latent_gain, (0, pad))[:, None],
            jnp.zeros((rows, 45), bf16),
        ],
        axis=1,
    )
    small_all = dp_gather(small)
    small_all = ring_gather(small_all, 1)
    small_all = (
        small_all.reshape(groups, replicas, rows, -1).transpose(1, 0, 2, 3).reshape(width, -1)
    )
    ldown_all = small_all[:, : RANK + RD]
    router_all = small_all[:, RANK + RD : RANK + RD + experts]
    gains = small_all[:, RANK + RD + experts :].astype(f32)
    gain_attn = gains[:, 0]
    gain_moe = gains[:, 1]
    gain_lat = gains[:, 2].reshape(-1, rows)[:, : latent_gain.shape[0]].reshape(-1)

    query_swap = expert_swap(query_weight.reshape(rows, HEADS, QD).transpose(1, 0, 2))
    lup_rows = latent_up.shape[0]
    code_row = jnp.pad(
        codes.reshape(own, experts).T, ((0, 0), (0, HD + VD - own))
    )[:, None, :]
    lup_swap = expert_swap(
        jnp.concatenate(
            [latent_up.reshape(lup_rows, HEADS, HD + VD).transpose(1, 0, 2), code_row], axis=1
        )
    )
    wq = dp_gather(query_swap.reshape(groups * rows, QD))
    lup = dp_gather(lup_swap[:, :lup_rows].reshape(groups * lup_rows, HD + VD))
    code = lup_swap[:, lup_rows, :own].astype(f32).reshape(tokens)

    def columns_of(weight):
        return (
            weight.reshape(rows, replicas, groups, part)
            .transpose(2, 0, 1, 3)
            .reshape(groups, rows, hidden_own)
        )

    gate_up_swap = expert_swap(
        jnp.concatenate([columns_of(shared_gate), columns_of(shared_up)], axis=2)
    )
    gate_up = dp_gather(gate_up_swap.reshape(groups * rows, 2 * hidden_own))
    gate_up_router = jnp.concatenate([gate_up, router_all], axis=1)
    sdown = dp_gather(shared_down)
    gate_w = dp_gather(expert_gate[0])
    up_w = dp_gather(expert_up[0])
    down_w = dp_gather(expert_down[0])
    out_t = gather_rows(output_weight.T, BOTH)
    cot_all = gather_rows(cot_own, EXPERT)

    at_block = jnp.arange(groups, dtype=jnp.int32)[:, None, None] * span
    positions = jnp.broadcast_to(
        at_block + jnp.arange(span, dtype=jnp.int32), (groups, seqs, span)
    ).reshape(tokens)
    tables = lax.optimization_barrier(angle_tables(positions, RD))
    normed_one, _ = norm_parts(x_all.astype(f32))
    h_one = (normed_one * gain_attn).astype(bf16)
    query_raw = product(h_one, wq)
    query = jnp.concatenate(
        [query_raw[:, :HD], rotate(query_raw[:, HD:], tables)], axis=-1
    ).astype(bf16)
    down = product(h_one, ldown_all)
    normed_lat, factor_lat = norm_parts(down[:, :RANK])
    latent = (normed_lat * gain_lat).astype(bf16)
    key_rope = rotate(down[:, RANK:], tables).astype(bf16)
    expanded = product(latent, lup).astype(bf16)
    query_s = by_sequence(query)
    key_s = by_sequence(jnp.concatenate([expanded[:, :HD], key_rope], axis=-1))
    value_s = by_sequence(expanded[:, HD:])
    at = jnp.arange(length, dtype=jnp.int32)
    mask = (at[None, None, :] <= at[None, :, None]) & (
        segments[:, None, :] == segments[:, :, None]
    )
    scores = jnp.where(mask, einsum("sqd,skd->sqk", query_s, key_s) * scale, masked_score)
    top_score = jnp.max(scores, axis=-1, keepdims=True)
    weights_exp = jnp.exp(scores - top_score)
    probs_attn = (weights_exp / jnp.sum(weights_exp, axis=-1, keepdims=True)).astype(bf16)
    heads_s = einsum("sqk,skd->sqd", probs_attn, value_s).astype(bf16)
    heads_own = heads_to_tokens(heads_s, span, 3).reshape(own, HEADS * VD)

    x_second = x_low.astype(f32) + right_product(heads_own, out_t)
    normed_two, factor_two = norm_parts(x_second)
    h_two = ring_gather((normed_two * gain_moe).astype(bf16), 2)

    chunk = tokens // 2
    blocks = chunk // span
    slots = blocks * capacity
    slot_at = jnp.arange(slots, dtype=jnp.int32)
    token_at = jnp.arange(chunk, dtype=jnp.int32)
    select = (
        (slot_at[:, None] // capacity == token_at[None, :] // span)[None]
        & (
            (slot_at % capacity).astype(f32)[None, :, None]
            == code.reshape(2, chunk)[:, None, :]
        )
    ).astype(bf16)
    select = lax.optimization_barrier(select)

    def to_slots(values):
        return einsum("cst,ctd->csd", select, values.reshape(2, chunk, -1)).astype(bf16).reshape(
            2 * slots, -1
        )

    def to_tokens(values):
        return einsum("cst,csd->ctd", select, values.reshape(2, slots, -1)).reshape(tokens, -1)

    pre = product(h_two, gate_up_router)
    shared_a = pre[:, :hidden_own]
    shared_b = pre[:, hidden_own : 2 * hidden_own]
    gate_probs = jax.nn.softmax(pre[:, 2 * hidden_own :], axis=-1)
    shared_hidden = (jax.nn.silu(shared_a) * shared_b).astype(bf16)
    mine = (jnp.arange(experts, dtype=jnp.int32) == place).astype(f32)
    own_prob = jnp.sum(gate_probs * mine, axis=-1)
    slot_prob = jnp.sum(
        select.astype(f32) * own_prob.reshape(2, 1, chunk), axis=-1
    ).reshape(2 * slots, 1)
    expert_in = to_slots(h_two)
    gate_pre = product(expert_in, gate_w)
    up_pre = product(expert_in, up_w)
    expert_hidden = (jax.nn.silu(gate_pre) * up_pre).astype(bf16)
    expert_out = product(expert_hidden, down_w).astype(bf16).astype(f32)
    partial = product(shared_hidden, sdown) + to_tokens((slot_prob * expert_out).astype(bf16))
    partial, cot_all = lax.optimization_barrier((partial.astype(bf16), cot_all))
    result = x_second + scatter_rows(partial, EXPERT).astype(f32)
    result = result.astype(bf16).reshape(seqs, span, width)

    grad_slots = to_slots(cot_all)
    hidden_grad = right_product(cot_all, sdown)
    sdown_grad = left_product(shared_hidden, cot_all)
    shared_a_grad = (hidden_grad * shared_b * silu_slope(shared_a)).astype(bf16)
    shared_b_grad = (hidden_grad * jax.nn.silu(shared_a)).astype(bf16)
    grad_wide = grad_slots.astype(f32)
    slot_grad = (slot_prob * grad_wide).astype(bf16)
    match = jnp.sum(grad_wide * expert_out, axis=-1).reshape(2, slots, 1)
    prob_grad = jnp.sum(select.astype(f32) * match, axis=1).reshape(tokens, 1)
    logit_grad = (gate_probs * prob_grad * (mine - own_prob[:, None])).astype(bf16)
    pre_grad = jnp.concatenate([shared_a_grad, shared_b_grad, logit_grad], axis=1)
    expert_hidden_grad = right_product(slot_grad, down_w)
    expert_a_grad = (expert_hidden_grad * up_pre * silu_slope(gate_pre)).astype(bf16)
    expert_b_grad = (expert_hidden_grad * jax.nn.silu(gate_pre)).astype(bf16)
    in_grad = (right_product(expert_a_grad, gate_w) + right_product(expert_b_grad, up_w)).astype(
        bf16
    )
    h_two_partial = right_product(pre_grad, gate_up_router) + to_tokens(in_grad)
    routed_down_grad = dp_scatter_product(expert_hidden, slot_grad)
    routed_gate_grad = dp_scatter_product(expert_in, expert_a_grad)
    routed_up_grad = dp_scatter_product(expert_in, expert_b_grad)
    h_two_grad = ring_scatter(h_two_partial.astype(bf16), 4)
    pre_weight_grad = left_product(h_two, pre_grad)
    sdown_owned = dp_scatter(sdown_grad)
    gate_up_owned = dp_scatter(pre_weight_grad[:, : 2 * hidden_own]).astype(bf16)
    gate_up_owned = expert_swap(
        gate_up_owned.reshape(groups, rows, 2 * hidden_own)
    ).astype(f32)

    def owned_columns(value):
        return (
            value.reshape(groups, rows, replicas, part)
            .transpose(1, 2, 0, 3)
            .reshape(rows, replicas * groups * part)
        )

    sgate_owned = owned_columns(gate_up_owned[:, :, :hidden_own])
    sup_owned = owned_columns(gate_up_owned[:, :, hidden_own:])
    router_grad = pre_weight_grad[:, 2 * hidden_own :]

    gmoe_grad = jnp.sum(h_two_grad * normed_two, axis=0)
    x_second_grad = cot_own.astype(f32) + norm_back(h_two_grad * gain_moe, normed_two, factor_two)
    attn_low = x_second_grad.astype(bf16)
    heads_grad = product(attn_low, out_t).astype(bf16)
    grad_s = tokens_to_heads(heads_grad.reshape(seqs, span, HEADS * VD), 5)
    out_owned = (
        scatter_rows(left_product(attn_low, heads_own).astype(bf16), BOTH).astype(f32).T
    )
    probs_grad = einsum("sqd,skd->sqk", grad_s, value_s)
    spread = jnp.sum(grad_s.astype(f32) * heads_s.astype(f32), axis=-1, keepdims=True)
    score_grad = (probs_attn.astype(f32) * (probs_grad - spread) * scale).astype(bf16)
    value_grad = einsum("sqk,sqd->skd", probs_attn, grad_s)
    key_grad = einsum("sqk,sqd->skd", score_grad, query_s)
    query_grad = by_block(einsum("sqk,skd->sqd", score_grad, key_s))
    expanded_grad = by_block(
        jnp.concatenate([key_grad[..., :HD], value_grad], axis=-1).astype(bf16)
    )
    rope_grad = by_block(key_grad[..., HD:])
    lup_grad = left_product(latent, expanded_grad)
    latent_grad = right_product(expanded_grad, lup)
    glat_grad = jnp.sum(latent_grad * normed_lat, axis=0)
    joint_grad = jnp.concatenate(
        [
            query_grad[:, :HD],
            unrotate(query_grad[:, HD:], tables),
            norm_back(latent_grad * gain_lat, normed_lat, factor_lat),
            unrotate(rope_grad, tables),
        ],
        axis=-1,
    ).astype(bf16)
    joint_weight = jnp.concatenate([wq, ldown_all], axis=1)
    h_one_partial = right_product(joint_grad, joint_weight)
    gattn_grad = jnp.sum(h_one_partial * normed_one, axis=0)
    h_one_grad = ring_scatter(h_one_partial.astype(bf16), 6)
    normed_own, factor_own = norm_parts(x_low.astype(f32))
    input_grad = x_second_grad + norm_back(h_one_grad * gain_attn, normed_own, factor_own)
    input_grad = input_grad.astype(bf16).reshape(seqs, span, width)
    joint_weight_grad = left_product(h_one, joint_grad)
    q_owned = expert_swap(
        dp_scatter(joint_weight_grad[:, :QD]).astype(bf16).reshape(groups, rows, QD)
    ).astype(f32)
    q_owned = q_owned.transpose(1, 0, 2).reshape(rows, HEADS * QD)
    lup_owned = expert_swap(
        dp_scatter(lup_grad).astype(bf16).reshape(groups, lup_rows, HD + VD)
    ).astype(f32)
    lup_owned = lup_owned.transpose(1, 0, 2).reshape(lup_rows, HEADS * (HD + VD))
    glat_column = jnp.pad(
        glat_grad.reshape(-1, latent_gain.shape[0]), ((0, 0), (0, pad))
    ).reshape(-1, 1)
    small_grad = jnp.concatenate(
        [
            joint_weight_grad[:, QD:],
            router_grad,
            gattn_grad[:, None],
            gmoe_grad[:, None],
            glat_column,
            jnp.zeros((width, 45), f32),
        ],
        axis=1,
    )
    small_grad = (
        small_grad.astype(bf16)
        .reshape(replicas, groups, rows, -1)
        .transpose(1, 0, 2, 3)
        .reshape(width, -1)
    )
    small_owned = ring_scatter(small_grad, 7)
    small_owned = dp_scatter(small_owned)
    ldown_owned = small_owned[:, : RANK + RD]
    router_owned = small_owned[:, RANK + RD : RANK + RD + experts]
    gain_owned = small_owned[:, RANK + RD + experts :]
    return (
        result,
        input_grad,
        q_owned,
        ldown_owned,
        lup_owned,
        out_owned,
        gain_owned[:, 0],
        gain_owned[: latent_gain.shape[0], 2],
        router_owned,
        sgate_owned,
        sup_owned,
        sdown_owned,
        gain_owned[:, 1],
        routed_gate_grad[None],
        routed_up_grad[None],
        routed_down_grad[None],
    )


def solution(mesh):
    return jax.shard_map(
        per_device,
        mesh=mesh,
        in_specs=(
            TOKENS, P(DP, None), TOKENS, P(DP, EXPERT), TOKENS,
            ROWS, ROWS, ROWS, P(None, BOTH), P(BOTH), P(BOTH),
            ROWS, ROWS, ROWS, ROWS, P(BOTH), ROUTED, ROUTED, ROUTED,
        ),
        out_specs=(
            TOKENS, TOKENS, ROWS, ROWS, ROWS, P(None, BOTH), P(BOTH), P(BOTH),
            ROWS, ROWS, ROWS, ROWS, P(BOTH), ROUTED, ROUTED, ROUTED,
        ),
        check_vma=False,
    )
```

```python
import functools
import math

import jax
import jax.numpy as jnp
from jax import lax
from jax.experimental import pallas as pl
from jax.experimental.pallas import tpu as pltpu
from jax.sharding import PartitionSpec as P

HEADS = 16
HD = 128
RD = 64
VD = 128
RANK = 512
TOP = 6

epsilon = 1e-06
masked_score = -1e30
DP = "dp"
EXPERT = "expert"
BOTH = (DP, EXPERT)
TOKENS = P(DP, EXPERT, None)
ROWS = P(BOTH, None)
ROUTED = P(EXPERT, DP, None)
f32 = jnp.float32
bf16 = jnp.bfloat16


def product(left, right):
    return jnp.dot(left, right, preferred_element_type=f32)


def left_product(left, right):
    return lax.dot_general(left, right, (((0,), (0,)), ((), ())), preferred_element_type=f32)


def right_product(left, right):
    return lax.dot_general(left, right, (((1,), (1,)), ((), ())), preferred_element_type=f32)


def einsum(spec, left, right):
    return jnp.einsum(spec, left, right, preferred_element_type=f32)


def norm_parts(values):
    factor = lax.rsqrt(jnp.mean(values * values, axis=-1, keepdims=True) + epsilon)
    return (values * factor, factor)


def norm_back(grad_normed, normed, factor):
    return factor * (grad_normed - normed * jnp.mean(grad_normed * normed, axis=-1, keepdims=True))


def angle_tables(positions, width):
    half = width // 2
    freqs = jnp.power(10000.0, -2.0 * jnp.arange(half, dtype=f32) / width)
    angles = positions.astype(f32)[:, None] * freqs[None, :]
    return (jnp.cos(angles), jnp.sin(angles))


def rotate(values, tables):
    half = values.shape[-1] // 2
    cosine, sine = tables
    first = values[..., :half]
    second = values[..., half:]
    return jnp.concatenate(
        [first * cosine - second * sine, second * cosine + first * sine], axis=-1
    )


def unrotate(grads, tables):
    half = grads.shape[-1] // 2
    cosine, sine = tables
    first = grads[..., :half]
    second = grads[..., half:]
    return jnp.concatenate(
        [first * cosine + second * sine, second * cosine - first * sine], axis=-1
    )


def silu_slope(pre):
    sigma = jax.nn.sigmoid(pre)
    return sigma * (1.0 + pre * (1.0 - sigma))


def dp_swap(value):
    return lax.ppermute(value, DP, [(0, 1), (1, 0)])


def dp_gather(value):
    if lax.axis_size(DP) == 2:
        other = dp_swap(value)
        first = lax.axis_index(DP) == 0
        return jnp.concatenate(
            [jnp.where(first, value, other), jnp.where(first, other, value)], axis=0
        )
    return lax.all_gather(value, DP, axis=0, tiled=True)


def dp_scatter_product(left, right):
    if lax.axis_size(DP) == 2:
        first = lax.axis_index(DP) == 0
        half = left.shape[1] // 2
        low, high = left[:, :half], left[:, half:]
        sent = left_product(jnp.where(first, high, low), right).astype(bf16)
        other = dp_swap(sent)
        return left_product(jnp.where(first, low, high), right) + other.astype(f32)
    return dp_scatter(left_product(left, right))


def dp_scatter(value):
    if lax.axis_size(DP) == 2:
        rows = value.shape[0] // 2
        at = lax.axis_index(DP)
        sent = lax.dynamic_slice_in_dim(value, (1 - at) * rows, rows, 0)
        kept = lax.dynamic_slice_in_dim(value, at * rows, rows, 0)
        return kept + dp_swap(sent.astype(bf16)).astype(f32)
    return lax.psum_scatter(
        value.astype(bf16), DP, scatter_dimension=0, tiled=True
    ).astype(f32)


def expert_swap(value):
    return lax.all_to_all(value, EXPERT, split_axis=0, concat_axis=0, tiled=True)


def gather_rows(value, axes):
    return lax.all_gather(value, axes, axis=0, tiled=True)


def scatter_rows(value, axes):
    return lax.psum_scatter(value, axes, scatter_dimension=0, tiled=True)


MESH = pl.DeviceIdType.MESH


def at_expert(index):
    return {EXPERT: index}


def grid_place():
    me = lax.axis_index(EXPERT)
    return me, me // 4, (me // 2) % 2, me % 2


def greet_neighbours(me, line, pair, core):
    partner = me + 1 - 2 * core
    mate = me + 2 - 4 * pair
    barrier = pltpu.get_barrier_semaphore()
    for other in (partner, mate):
        pl.semaphore_signal(barrier, inc=1, device_id=at_expert(other), device_id_type=MESH)

    @pl.when(line < 3)
    def _():
        pl.semaphore_signal(barrier, inc=1, device_id=at_expert(me + 4), device_id_type=MESH)

    @pl.when(line > 0)
    def _():
        pl.semaphore_signal(barrier, inc=1, device_id=at_expert(me - 4), device_id_type=MESH)

    pl.semaphore_wait(barrier, 3 + jnp.where((line > 0) & (line < 3), 1, 0))
    return partner, mate


def greet_all(me):
    barrier = pltpu.get_barrier_semaphore()
    for step in range(1, 16):
        pl.semaphore_signal(
            barrier, inc=1, device_id=at_expert((me + step) % 16), device_id_type=MESH
        )
    pl.semaphore_wait(barrier, 15)


def gather_kernel(n, m, *refs):
    x_refs, swap_refs = refs[:n], refs[n : n + m]
    outs, swap_outs = refs[n + m : 2 * n + m], refs[2 * n + m : 2 * (n + m)]
    own_sem, send_sem, recv_sem, swap_send, swap_recv = refs[2 * (n + m) :]
    me, line, pair, core = grid_place()
    if m:
        greet_all(me)
        partner, mate = me + 1 - 2 * core, me + 2 - 4 * pair
    else:
        partner, mate = greet_neighbours(me, line, pair, core)

    def own_copy(i):
        if i < n:
            return pltpu.make_async_copy(x_refs[i], outs[i].at[me], own_sem.at[i])
        i -= n
        return pltpu.make_async_copy(
            swap_refs[i].at[me], swap_outs[i].at[me], own_sem.at[n + i]
        )

    def copy(i, source, origin, way, to):
        return pltpu.make_async_remote_copy(
            src_ref=source,
            dst_ref=outs[i].at[origin],
            send_sem=send_sem.at[i, origin, way],
            recv_sem=recv_sem.at[i, origin],
            device_id=at_expert(to),
            device_id_type=MESH,
        )

    def swap_copy(i, step):
        to = (me + step) % 16
        return pltpu.make_async_remote_copy(
            src_ref=swap_refs[i].at[to],
            dst_ref=swap_outs[i].at[me],
            send_sem=swap_send.at[i, step],
            recv_sem=swap_recv.at[i, step],
            device_id=at_expert(to),
            device_id_type=MESH,
        )

    def arrived(i, origin):
        copy(i, outs[i].at[origin], origin, 0, partner).wait_recv()

    def along(i, origin, source, upward, downward, act):
        if upward:

            @pl.when(line < 3)
            def _():
                act(copy(i, source, origin, 0, me + 4))

        if downward:

            @pl.when(line > 0)
            def _():
                act(copy(i, source, origin, 1, me - 4))

        act(copy(i, source, origin, 2, mate))
        act(copy(i, source, origin, 3, partner))

    def walk(act, wait):
        for far in range(1, 5):
            if far < 4:

                @pl.when(line >= far)
                def _():
                    origin = me - 4 * far
                    for i in range(n):
                        wait(i, origin)
                        along(i, origin, outs[i].at[origin], True, False, act)

                @pl.when(line + far <= 3)
                def _():
                    origin = me + 4 * far
                    for i in range(n):
                        wait(i, origin)
                        along(i, origin, outs[i].at[origin], False, True, act)

            for sign in (-1, 1) if far > 1 else (1,):
                step = sign * (far - 1)

                @pl.when((line + step >= 0) & (line + step <= 3))
                def _():
                    origin = mate + 4 * step
                    for i in range(n):
                        wait(i, origin)
                        act(copy(i, outs[i].at[origin], origin, 3, partner))

    def start(c):
        c.start()

    def sent(c):
        c.wait_send()

    for i in range(n):
        along(i, me, x_refs[i], True, True, start)
    for i in range(m):
        for step in range(1, 16):
            swap_copy(i, step).start()
    for i in range(n + m):
        own_copy(i).start()
    walk(start, arrived)
    for i in range(n):
        for index in range(8):
            arrived(i, 2 * index + 1 - core)
    for i in range(n):
        along(i, me, x_refs[i], True, True, sent)
    walk(sent, lambda i, origin: None)
    for i in range(m):
        for step in range(1, 16):
            swap_copy(i, step).wait()
    for i in range(n + m):
        own_copy(i).wait()


def ring_gather(values, swaps, collective):
    n, m = len(values), len(swaps)
    sent = 2 * (15 * sum(v.size for v in values) + sum(v.size for v in swaps))
    sems = pltpu.SemaphoreType.DMA
    anywhere = pl.BlockSpec(memory_space=pl.ANY)
    outs = pl.pallas_call(
        functools.partial(gather_kernel, n, m),
        out_shape=[jax.ShapeDtypeStruct((16,) + v.shape, v.dtype) for v in values]
        + [jax.ShapeDtypeStruct(v.shape, v.dtype) for v in swaps],
        in_specs=[pl.BlockSpec(memory_space=pltpu.VMEM)] * (n + m),
        out_specs=[anywhere] * (n + m),
        scratch_shapes=[
            sems((n + m,)),
            sems((n, 16, 4)),
            sems((n, 16)),
            sems((max(m, 1), 16)),
            sems((max(m, 1), 16)),
        ],
        compiler_params=pltpu.CompilerParams(collective_id=collective, has_side_effects=True),
        cost_estimate=pl.CostEstimate(flops=0, bytes_accessed=16 * sent, transcendentals=0),
    )(*values, *swaps)
    return [o.reshape(-1, o.shape[-1]) for o in outs[:n]] + list(outs[n:])


def scatter_kernel(n, *refs):
    parts = [(refs[i], refs[n + i]) + refs[2 * n + 5 * i : 2 * n + 5 * i + 5] for i in range(n)]
    (
        core_send, core_recv, mate_send, mate_recv, up_send, up_recv, down_send, down_recv,
    ) = refs[7 * n :]
    me, line, pair, core = grid_place()
    partner, mate = greet_neighbours(me, line, pair, core)

    def remote(source, target, send, recv, to):
        return pltpu.make_async_remote_copy(
            src_ref=source, dst_ref=target, send_sem=send, recv_sem=recv,
            device_id=at_expert(to), device_id_type=MESH,
        )

    def core_copy(i, index):
        return remote(
            parts[i][0].at[2 * index + 1 - core], parts[i][2].at[index],
            core_send.at[i, index], core_recv.at[i, index], partner,
        )

    def mate_copy(i, dest):
        return remote(
            parts[i][6].at[2 * dest + 1 - pair], parts[i][3].at[dest],
            mate_send.at[i, dest], mate_recv.at[i, dest], mate,
        )

    def up_copy(i, dest):
        return remote(
            parts[i][6].at[2 * dest + pair], parts[i][4].at[dest],
            up_send.at[i, dest], up_recv.at[i, dest], me + 4,
        )

    def down_copy(i, dest):
        return remote(
            parts[i][6].at[2 * dest + pair], parts[i][5].at[dest],
            down_send.at[i, dest], down_recv.at[i, dest], me - 4,
        )

    def add(target, left, right):
        tile = 16

        @pl.loop(0, left.shape[0] // tile)
        def _(i):
            at = pl.ds(pl.multiple_of(i * tile, tile), tile)
            target[at, :] = (left[at, :].astype(f32) + right[at, :].astype(f32)).astype(
                target.dtype
            )

    def farthest(act):
        for far in (3, 2, 1, 0):
            for step in (-far, far) if far else (0,):

                @pl.when((line + step >= 0) & (line + step <= 3))
                def _():
                    for i in range(n):
                        act(i, line + step, step)

    def send_core(i, dest, step):
        core_copy(i, 2 * dest + 1 - pair).start()

    def send_core_own(i, dest, step):
        core_copy(i, 2 * dest + pair).start()

    def chip_sum(i, index):
        core_copy(i, index).wait_recv()
        add(parts[i][6].at[index], parts[i][0].at[2 * index + core], parts[i][2].at[index])

    def to_mate(i, dest, step):
        chip_sum(i, 2 * dest + 1 - pair)
        mate_copy(i, dest).start()

    def keep(i, dest, step):
        chip_sum(i, 2 * dest + pair)

    def along(i, dest, step):
        out, up_in, down_in, total = parts[i][1], parts[i][4], parts[i][5], parts[i][6]
        mine = total.at[2 * dest + pair]
        mate_copy(i, dest).wait_recv()
        if step == 0:
            add(out, mine, parts[i][3].at[dest])
            mine = out
        else:
            add(mine, mine, parts[i][3].at[dest])
        if step >= 0:

            @pl.when(line > 0)
            def _():
                up_copy(i, dest).wait_recv()
                add(mine, mine, up_in.at[dest])

        if step <= 0:

            @pl.when(line < 3)
            def _():
                down_copy(i, dest).wait_recv()
                add(mine, mine, down_in.at[dest])

        if step > 0:
            up_copy(i, dest).start()
        elif step < 0:
            down_copy(i, dest).start()

    def finish(i, dest, step):
        mate_copy(i, dest).wait_send()
        core_copy(i, 2 * dest + 1 - pair).wait_send()
        core_copy(i, 2 * dest + pair).wait_send()
        if step > 0:
            up_copy(i, dest).wait_send()
        elif step < 0:
            down_copy(i, dest).wait_send()

    for act in (send_core, send_core_own, to_mate, keep, along, finish):
        farthest(act)


def ring_scatter(values, collective):
    n = len(values)
    shapes = [(v.shape[0] // 16, v.shape[1]) for v in values]
    buffers = [pltpu.VMEM((k,) + s, bf16) for s in shapes for k in (8, 4, 4, 4, 8)]
    sent = 30 * sum(a * b for a, b in shapes)
    vmem = pl.BlockSpec(memory_space=pltpu.VMEM)
    return pl.pallas_call(
        functools.partial(scatter_kernel, n),
        out_shape=[jax.ShapeDtypeStruct(s, f32) for s in shapes],
        in_specs=[vmem] * n,
        out_specs=[vmem] * n,
        scratch_shapes=buffers
        + [pltpu.SemaphoreType.DMA((n, k)) for k in (8, 8, 4, 4, 4, 4, 4, 4)],
        compiler_params=pltpu.CompilerParams(collective_id=collective, has_side_effects=True),
        cost_estimate=pl.CostEstimate(flops=0, bytes_accessed=16 * sent, transcendentals=0),
    )(*[v.reshape((16,) + s) for v, s in zip(values, shapes)])


def swap_kernel(source, target, x_ref, out_ref, own_sem, send_sem, recv_sem):
    me = lax.axis_index(EXPERT)
    greet_all(me)

    def copy(step):
        to = (me + step) % 16
        return pltpu.make_async_remote_copy(
            src_ref=source(x_ref, to),
            dst_ref=target(out_ref, me),
            send_sem=send_sem.at[step],
            recv_sem=recv_sem.at[step],
            device_id=at_expert(to),
            device_id_type=MESH,
        )

    for step in range(1, 16):
        copy(step).start()
    own = pltpu.make_async_copy(source(x_ref, me), target(out_ref, me), own_sem)
    own.start()
    for step in range(1, 16):
        copy(step).wait()
    own.wait()


def swap_call(source, target, value, shape, collective):
    sent = value.size * 2
    return pl.pallas_call(
        functools.partial(swap_kernel, source, target),
        out_shape=jax.ShapeDtypeStruct(shape, value.dtype),
        in_specs=[pl.BlockSpec(memory_space=pltpu.VMEM)],
        out_specs=pl.BlockSpec(memory_space=pltpu.VMEM),
        scratch_shapes=[
            pltpu.SemaphoreType.DMA,
            pltpu.SemaphoreType.DMA((16,)),
            pltpu.SemaphoreType.DMA((16,)),
        ],
        compiler_params=pltpu.CompilerParams(collective_id=collective, has_side_effects=True),
        cost_estimate=pl.CostEstimate(flops=0, bytes_accessed=64 * sent, transcendentals=0),
    )(value)


def block_rows(span):
    return lambda ref, at: ref.at[:, pl.ds(pl.multiple_of(at * span, span), span), :]


def head_columns(columns):
    return lambda ref, at: ref.at[:, :, pl.ds(pl.multiple_of(at * columns, columns), columns)]


def heads_to_tokens(value, span, collective):
    seqs = value.shape[0]
    return swap_call(
        block_rows(span), head_columns(VD), value, (seqs, span, HEADS * VD), collective
    )


def tokens_to_heads(value, collective):
    seqs, span, _ = value.shape
    return swap_call(
        head_columns(VD), block_rows(span), value, (seqs, span * HEADS, VD), collective
    )


def per_device(
    inputs,
    segments,
    expert_picks,
    priority,
    cotangent,
    query_weight,
    latent_down,
    latent_up,
    output_weight,
    attn_gain,
    latent_gain,
    router_weight,
    shared_gate,
    shared_up,
    shared_down,
    moe_gain,
    expert_gate,
    expert_up,
    expert_down,
):
    groups = lax.axis_size(EXPERT)
    replicas = lax.axis_size(DP)
    place = lax.axis_index(EXPERT)
    seqs, span, width = inputs.shape
    length = span * groups
    own = seqs * span
    tokens = own * groups
    experts = groups
    capacity = (9 * span * TOP + 8 * experts - 1) // (8 * experts)
    scale = 1.0 / math.sqrt(HD + RD)
    rows = query_weight.shape[0]
    part = shared_down.shape[0]
    hidden_own = part * replicas
    QD = HD + RD

    def by_sequence(value):
        return value.reshape(groups, seqs, span, -1).transpose(1, 0, 2, 3).reshape(
            seqs, length, -1
        )

    def by_block(value):
        return value.reshape(seqs, groups, span, -1).transpose(1, 0, 2, 3).reshape(tokens, -1)

    x_low = inputs.reshape(own, width)
    cot_own = cotangent.reshape(own, width)

    order = priority[:, None, :] < priority[:, :, None]
    hit = jnp.sum(
        (expert_picks[..., None] == jnp.arange(experts, dtype=jnp.int32)).astype(f32), axis=2
    )
    ranks = einsum("stu,sue->ste", order.astype(bf16), hit.astype(bf16))
    codes = jnp.where((hit > 0) & (ranks < capacity), ranks, -1.0).astype(bf16)

    pad = rows - latent_gain.shape[0]
    small = jnp.concatenate(
        [
            latent_down,
            router_weight,
            attn_gain[:, None],
            moe_gain[:, None],
            jnp.pad(latent_gain, (0, pad))[:, None],
            jnp.zeros((rows, 45), bf16),
        ],
        axis=1,
    )
    small = dp_gather(small)
    query_parts = query_weight.reshape(rows, HEADS, QD).transpose(1, 0, 2)
    lup_rows = latent_up.shape[0]
    code_rows = -(lup_rows + 1) % 16 + 1
    code_part = jnp.pad(
        codes.reshape(own, 1, experts).T, ((0, 0), (0, code_rows - 1), (0, HD + VD - own))
    )
    lup_parts = jnp.concatenate(
        [latent_up.reshape(lup_rows, HEADS, HD + VD).transpose(1, 0, 2), code_part], axis=1
    )
    small_all, x_all, query_swap, lup_swap = ring_gather(
        [small, x_low], [query_parts, lup_parts], 1
    )
    small_all = (
        small_all.reshape(groups, replicas, rows, -1).transpose(1, 0, 2, 3).reshape(width, -1)
    )
    ldown_all = small_all[:, : RANK + RD]
    router_all = small_all[:, RANK + RD : RANK + RD + experts]
    gains = small_all[:, RANK + RD + experts :].astype(f32)
    gain_attn = gains[:, 0]
    gain_moe = gains[:, 1]
    gain_lat = gains[:, 2].reshape(-1, rows)[:, : latent_gain.shape[0]].reshape(-1)

    wq = dp_gather(query_swap.reshape(groups * rows, QD))
    lup = dp_gather(lup_swap[:, :lup_rows].reshape(groups * lup_rows, HD + VD))
    code = lup_swap[:, lup_rows, :own].astype(f32).reshape(tokens)

    def columns_of(weight):
        return (
            weight.reshape(rows, replicas, groups, part)
            .transpose(2, 0, 1, 3)
            .reshape(groups, rows, hidden_own)
        )

    gate_up_parts, query_swap = lax.optimization_barrier(
        (jnp.concatenate([columns_of(shared_gate), columns_of(shared_up)], axis=2), query_swap)
    )
    gate_up_swap = expert_swap(gate_up_parts)
    gate_up = dp_gather(gate_up_swap.reshape(groups * rows, 2 * hidden_own))
    gate_up_router = jnp.concatenate([gate_up, router_all], axis=1)
    sdown = dp_gather(shared_down)
    gate_w = dp_gather(expert_gate[0])
    up_w = dp_gather(expert_up[0])
    down_w = dp_gather(expert_down[0])
    out_t = gather_rows(output_weight.T, BOTH)
    cot_all = gather_rows(cot_own, EXPERT)

    at_block = jnp.arange(groups, dtype=jnp.int32)[:, None, None] * span
    positions = jnp.broadcast_to(
        at_block + jnp.arange(span, dtype=jnp.int32), (groups, seqs, span)
    ).reshape(tokens)
    tables = lax.optimization_barrier(angle_tables(positions, RD))
    normed_one, _ = norm_parts(x_all.astype(f32))
    h_one = (normed_one * gain_attn).astype(bf16)
    query_raw = product(h_one, wq)
    query = jnp.concatenate(
        [query_raw[:, :HD], rotate(query_raw[:, HD:], tables)], axis=-1
    ).astype(bf16)
    down = product(h_one, ldown_all)
    normed_lat, factor_lat = norm_parts(down[:, :RANK])
    latent = (normed_lat * gain_lat).astype(bf16)
    key_rope = rotate(down[:, RANK:], tables).astype(bf16)
    expanded = product(latent, lup).astype(bf16)
    query_s = by_sequence(query)
    key_s = by_sequence(jnp.concatenate([expanded[:, :HD], key_rope], axis=-1))
    value_s = by_sequence(expanded[:, HD:])
    at = jnp.arange(length, dtype=jnp.int32)
    mask = (at[None, None, :] <= at[None, :, None]) & (
        segments[:, None, :] == segments[:, :, None]
    )
    scores = jnp.where(mask, einsum("sqd,skd->sqk", query_s, key_s) * scale, masked_score)
    top_score = jnp.max(scores, axis=-1, keepdims=True)
    weights_exp = jnp.exp(scores - top_score)
    probs_attn = (weights_exp / jnp.sum(weights_exp, axis=-1, keepdims=True)).astype(bf16)
    heads_s = einsum("sqk,skd->sqd", probs_attn, value_s).astype(bf16)
    heads_own = heads_to_tokens(heads_s, span, 3).reshape(own, HEADS * VD)

    x_second = x_low.astype(f32) + right_product(heads_own, out_t)
    normed_two, factor_two = norm_parts(x_second)
    (h_two,) = ring_gather([(normed_two * gain_moe).astype(bf16)], [], 2)

    chunk = tokens // 2
    blocks = chunk // span
    slots = blocks * capacity
    slot_at = jnp.arange(slots, dtype=jnp.int32)
    token_at = jnp.arange(chunk, dtype=jnp.int32)
    select = (
        (slot_at[:, None] // capacity == token_at[None, :] // span)[None]
        & (
            (slot_at % capacity).astype(f32)[None, :, None]
            == code.reshape(2, chunk)[:, None, :]
        )
    ).astype(bf16)
    select = lax.optimization_barrier(select)

    def to_slots(values):
        return einsum("cst,ctd->csd", select, values.reshape(2, chunk, -1)).astype(bf16).reshape(
            2 * slots, -1
        )

    def to_tokens(values):
        return einsum("cst,csd->ctd", select, values.reshape(2, slots, -1)).reshape(tokens, -1)

    pre = product(h_two, gate_up_router)
    shared_a = pre[:, :hidden_own]
    shared_b = pre[:, hidden_own : 2 * hidden_own]
    gate_probs = jax.nn.softmax(pre[:, 2 * hidden_own :], axis=-1)
    shared_hidden = (jax.nn.silu(shared_a) * shared_b).astype(bf16)
    mine = (jnp.arange(experts, dtype=jnp.int32) == place).astype(f32)
    own_prob = jnp.sum(gate_probs * mine, axis=-1)
    slot_prob = jnp.sum(
        select.astype(f32) * own_prob.reshape(2, 1, chunk), axis=-1
    ).reshape(2 * slots, 1)
    expert_in = to_slots(h_two)
    gate_pre = product(expert_in, gate_w)
    up_pre = product(expert_in, up_w)
    expert_hidden = (jax.nn.silu(gate_pre) * up_pre).astype(bf16)
    expert_out = product(expert_hidden, down_w).astype(bf16).astype(f32)
    partial = product(shared_hidden, sdown) + to_tokens((slot_prob * expert_out).astype(bf16))
    partial, cot_all = lax.optimization_barrier((partial.astype(bf16), cot_all))
    result = x_second + scatter_rows(partial, EXPERT).astype(f32)
    result = result.astype(bf16).reshape(seqs, span, width)

    grad_slots = to_slots(cot_all)
    hidden_grad = right_product(cot_all, sdown)
    sdown_grad = left_product(shared_hidden, cot_all)
    shared_a_grad = (hidden_grad * shared_b * silu_slope(shared_a)).astype(bf16)
    shared_b_grad = (hidden_grad * jax.nn.silu(shared_a)).astype(bf16)
    grad_wide = grad_slots.astype(f32)
    slot_grad = (slot_prob * grad_wide).astype(bf16)
    match = jnp.sum(grad_wide * expert_out, axis=-1).reshape(2, slots, 1)
    prob_grad = jnp.sum(select.astype(f32) * match, axis=1).reshape(tokens, 1)
    logit_grad = (gate_probs * prob_grad * (mine - own_prob[:, None])).astype(bf16)
    pre_grad = jnp.concatenate([shared_a_grad, shared_b_grad, logit_grad], axis=1)
    expert_hidden_grad = right_product(slot_grad, down_w)
    expert_a_grad = (expert_hidden_grad * up_pre * silu_slope(gate_pre)).astype(bf16)
    expert_b_grad = (expert_hidden_grad * jax.nn.silu(gate_pre)).astype(bf16)
    in_grad = (right_product(expert_a_grad, gate_w) + right_product(expert_b_grad, up_w)).astype(
        bf16
    )
    h_two_partial = right_product(pre_grad, gate_up_router) + to_tokens(in_grad)
    routed_down_grad = dp_scatter_product(expert_hidden, slot_grad)
    routed_gate_grad = dp_scatter_product(expert_in, expert_a_grad)
    routed_up_grad = dp_scatter_product(expert_in, expert_b_grad)
    (h_two_grad,) = ring_scatter([h_two_partial.astype(bf16)], 4)
    pre_weight_grad = left_product(h_two, pre_grad)
    sdown_owned = dp_scatter(sdown_grad)
    gate_up_owned = dp_scatter(pre_weight_grad[:, : 2 * hidden_own]).astype(bf16)
    router_grad = pre_weight_grad[:, 2 * hidden_own :]

    gmoe_grad = jnp.sum(h_two_grad * normed_two, axis=0)
    x_second_grad = cot_own.astype(f32) + norm_back(h_two_grad * gain_moe, normed_two, factor_two)
    attn_low = x_second_grad.astype(bf16)
    heads_grad = product(attn_low, out_t).astype(bf16)
    grad_s = tokens_to_heads(heads_grad.reshape(seqs, span, HEADS * VD), 5)
    attn_low, gate_up_owned, grad_s = lax.optimization_barrier((attn_low, gate_up_owned, grad_s))
    out_owned = (
        scatter_rows(left_product(attn_low, heads_own).astype(bf16), BOTH).astype(f32).T
    )
    gate_up_owned = expert_swap(
        gate_up_owned.reshape(groups, rows, 2 * hidden_own)
    ).astype(f32)

    def owned_columns(value):
        return (
            value.reshape(groups, rows, replicas, part)
            .transpose(1, 2, 0, 3)
            .reshape(rows, replicas * groups * part)
        )

    sgate_owned = owned_columns(gate_up_owned[:, :, :hidden_own])
    sup_owned = owned_columns(gate_up_owned[:, :, hidden_own:])
    probs_grad = einsum("sqd,skd->sqk", grad_s, value_s)
    spread = jnp.sum(grad_s.astype(f32) * heads_s.astype(f32), axis=-1, keepdims=True)
    score_grad = (probs_attn.astype(f32) * (probs_grad - spread) * scale).astype(bf16)
    value_grad = einsum("sqk,sqd->skd", probs_attn, grad_s)
    key_grad = einsum("sqk,sqd->skd", score_grad, query_s)
    query_grad = by_block(einsum("sqk,skd->sqd", score_grad, key_s))
    expanded_grad = by_block(
        jnp.concatenate([key_grad[..., :HD], value_grad], axis=-1).astype(bf16)
    )
    rope_grad = by_block(key_grad[..., HD:])
    lup_grad = left_product(latent, expanded_grad)
    latent_grad = right_product(expanded_grad, lup)
    glat_grad = jnp.sum(latent_grad * normed_lat, axis=0)
    joint_grad = jnp.concatenate(
        [
            query_grad[:, :HD],
            unrotate(query_grad[:, HD:], tables),
            norm_back(latent_grad * gain_lat, normed_lat, factor_lat),
            unrotate(rope_grad, tables),
        ],
        axis=-1,
    ).astype(bf16)
    joint_weight = jnp.concatenate([wq, ldown_all], axis=1)
    h_one_partial = right_product(joint_grad, joint_weight)
    gattn_grad = jnp.sum(h_one_partial * normed_one, axis=0)
    joint_weight_grad = left_product(h_one, joint_grad)
    back_grad = jnp.concatenate([joint_weight_grad[:, :QD], lup_grad.reshape(width, -1)], axis=1)
    back_grad = dp_scatter(back_grad).astype(bf16)
    back_owned = expert_swap(back_grad.reshape(groups, rows, -1)).astype(f32)
    q_owned = back_owned[:, :, :QD].transpose(1, 0, 2).reshape(rows, HEADS * QD)
    lup_owned = back_owned[:, :, QD:].reshape(groups, lup_rows, HD + VD)
    lup_owned = lup_owned.transpose(1, 0, 2).reshape(lup_rows, HEADS * (HD + VD))
    glat_column = jnp.pad(
        glat_grad.reshape(-1, latent_gain.shape[0]), ((0, 0), (0, pad))
    ).reshape(-1, 1)
    small_grad = jnp.concatenate(
        [
            joint_weight_grad[:, QD:],
            router_grad,
            gattn_grad[:, None],
            gmoe_grad[:, None],
            glat_column,
            jnp.zeros((width, 45), f32),
        ],
        axis=1,
    )
    small_grad = (
        small_grad.astype(bf16)
        .reshape(replicas, groups, rows, -1)
        .transpose(1, 0, 2, 3)
        .reshape(width, -1)
    )
    small_owned, h_one_grad = ring_scatter([small_grad, h_one_partial.astype(bf16)], 6)
    normed_own, factor_own = norm_parts(x_low.astype(f32))
    input_grad = x_second_grad + norm_back(h_one_grad * gain_attn, normed_own, factor_own)
    input_grad = input_grad.astype(bf16).reshape(seqs, span, width)
    small_owned = dp_scatter(small_owned)
    ldown_owned = small_owned[:, : RANK + RD]
    router_owned = small_owned[:, RANK + RD : RANK + RD + experts]
    gain_owned = small_owned[:, RANK + RD + experts :]
    return (
        result,
        input_grad,
        q_owned,
        ldown_owned,
        lup_owned,
        out_owned,
        gain_owned[:, 0],
        gain_owned[: latent_gain.shape[0], 2],
        router_owned,
        sgate_owned,
        sup_owned,
        sdown_owned,
        gain_owned[:, 1],
        routed_gate_grad[None],
        routed_up_grad[None],
        routed_down_grad[None],
    )


def solution(mesh):
    return jax.shard_map(
        per_device,
        mesh=mesh,
        in_specs=(
            TOKENS, P(DP, None), TOKENS, P(DP, EXPERT), TOKENS,
            ROWS, ROWS, ROWS, P(None, BOTH), P(BOTH), P(BOTH),
            ROWS, ROWS, ROWS, ROWS, P(BOTH), ROUTED, ROUTED, ROUTED,
        ),
        out_specs=(
            TOKENS, TOKENS, ROWS, ROWS, ROWS, P(None, BOTH), P(BOTH), P(BOTH),
            ROWS, ROWS, ROWS, ROWS, P(BOTH), ROUTED, ROUTED, ROUTED,
        ),
        check_vma=False,
    )
```

```python
import functools
import math

import jax
import jax.numpy as jnp
from jax import lax
from jax.experimental import pallas as pl
from jax.experimental.pallas import tpu as pltpu
from jax.sharding import PartitionSpec as P

HEADS = 16
HD = 128
RD = 64
VD = 128
RANK = 512
TOP = 6

epsilon = 1e-06
masked_score = -1e30
DP = "dp"
EXPERT = "expert"
BOTH = (DP, EXPERT)
TOKENS = P(DP, EXPERT, None)
ROWS = P(BOTH, None)
ROUTED = P(EXPERT, DP, None)
f32 = jnp.float32
bf16 = jnp.bfloat16


def product(left, right):
    return jnp.dot(left, right, preferred_element_type=f32)


def left_product(left, right):
    return lax.dot_general(left, right, (((0,), (0,)), ((), ())), preferred_element_type=f32)


def right_product(left, right):
    return lax.dot_general(left, right, (((1,), (1,)), ((), ())), preferred_element_type=f32)


def einsum(spec, left, right):
    return jnp.einsum(spec, left, right, preferred_element_type=f32)


def norm_parts(values):
    factor = lax.rsqrt(jnp.mean(values * values, axis=-1, keepdims=True) + epsilon)
    return (values * factor, factor)


def norm_back(grad_normed, normed, factor):
    return factor * (grad_normed - normed * jnp.mean(grad_normed * normed, axis=-1, keepdims=True))


def angle_tables(positions, width):
    half = width // 2
    freqs = jnp.power(10000.0, -2.0 * jnp.arange(half, dtype=f32) / width)
    angles = positions.astype(f32)[:, None] * freqs[None, :]
    return (jnp.cos(angles), jnp.sin(angles))


def rotate(values, tables):
    half = values.shape[-1] // 2
    cosine, sine = tables
    first = values[..., :half]
    second = values[..., half:]
    return jnp.concatenate(
        [first * cosine - second * sine, second * cosine + first * sine], axis=-1
    )


def unrotate(grads, tables):
    half = grads.shape[-1] // 2
    cosine, sine = tables
    first = grads[..., :half]
    second = grads[..., half:]
    return jnp.concatenate(
        [first * cosine + second * sine, second * cosine - first * sine], axis=-1
    )


def silu_slope(pre):
    sigma = jax.nn.sigmoid(pre)
    return sigma * (1.0 + pre * (1.0 - sigma))


def dp_swap(value):
    return lax.ppermute(value, DP, [(0, 1), (1, 0)])


def dp_gather(value):
    if lax.axis_size(DP) == 2:
        other = dp_swap(value)
        first = lax.axis_index(DP) == 0
        return jnp.concatenate(
            [jnp.where(first, value, other), jnp.where(first, other, value)], axis=0
        )
    return lax.all_gather(value, DP, axis=0, tiled=True)


def dp_scatter_product(left, right):
    if lax.axis_size(DP) == 2:
        first = lax.axis_index(DP) == 0
        half = left.shape[1] // 2
        low, high = left[:, :half], left[:, half:]
        sent = left_product(jnp.where(first, high, low), right).astype(bf16)
        other = dp_swap(sent)
        return left_product(jnp.where(first, low, high), right) + other.astype(f32)
    return dp_scatter(left_product(left, right))


def dp_scatter(value):
    if lax.axis_size(DP) == 2:
        rows = value.shape[0] // 2
        at = lax.axis_index(DP)
        sent = lax.dynamic_slice_in_dim(value, (1 - at) * rows, rows, 0)
        kept = lax.dynamic_slice_in_dim(value, at * rows, rows, 0)
        return kept + dp_swap(sent.astype(bf16)).astype(f32)
    return lax.psum_scatter(
        value.astype(bf16), DP, scatter_dimension=0, tiled=True
    ).astype(f32)


def expert_swap(value):
    return lax.all_to_all(value, EXPERT, split_axis=0, concat_axis=0, tiled=True)


def gather_rows(value, axes):
    return lax.all_gather(value, axes, axis=0, tiled=True)


def scatter_rows(value, axes):
    return lax.psum_scatter(value, axes, scatter_dimension=0, tiled=True)


MESH = pl.DeviceIdType.MESH


def at_expert(index):
    return {EXPERT: index}


def grid_place():
    me = lax.axis_index(EXPERT)
    return me, me // 4, (me // 2) % 2, me % 2


def greet_neighbours(me, line, pair, core):
    partner = me + 1 - 2 * core
    mate = me + 2 - 4 * pair
    barrier = pltpu.get_barrier_semaphore()
    for other in (partner, mate):
        pl.semaphore_signal(barrier, inc=1, device_id=at_expert(other), device_id_type=MESH)

    @pl.when(line < 3)
    def _():
        pl.semaphore_signal(barrier, inc=1, device_id=at_expert(me + 4), device_id_type=MESH)

    @pl.when(line > 0)
    def _():
        pl.semaphore_signal(barrier, inc=1, device_id=at_expert(me - 4), device_id_type=MESH)

    pl.semaphore_wait(barrier, 3 + jnp.where((line > 0) & (line < 3), 1, 0))
    return partner, mate


def greet_all(me):
    barrier = pltpu.get_barrier_semaphore()
    for step in range(1, 16):
        pl.semaphore_signal(
            barrier, inc=1, device_id=at_expert((me + step) % 16), device_id_type=MESH
        )
    pl.semaphore_wait(barrier, 15)


def gather_kernel(n, m, *refs):
    x_refs, swap_refs = refs[:n], refs[n : n + m]
    outs, swap_outs = refs[n + m : 2 * n + m], refs[2 * n + m : 2 * (n + m)]
    own_sem, send_sem, recv_sem, swap_send, swap_recv = refs[2 * (n + m) :]
    me, line, pair, core = grid_place()
    if m:
        greet_all(me)
        partner, mate = me + 1 - 2 * core, me + 2 - 4 * pair
    else:
        partner, mate = greet_neighbours(me, line, pair, core)

    def own_copy(i):
        if i < n:
            return pltpu.make_async_copy(x_refs[i], outs[i].at[me], own_sem.at[i])
        i -= n
        return pltpu.make_async_copy(
            swap_refs[i].at[me], swap_outs[i].at[me], own_sem.at[n + i]
        )

    def copy(i, source, origin, way, to):
        return pltpu.make_async_remote_copy(
            src_ref=source,
            dst_ref=outs[i].at[origin],
            send_sem=send_sem.at[i, origin, way],
            recv_sem=recv_sem.at[i, origin],
            device_id=at_expert(to),
            device_id_type=MESH,
        )

    def swap_copy(i, step):
        to = (me + step) % 16
        return pltpu.make_async_remote_copy(
            src_ref=swap_refs[i].at[to],
            dst_ref=swap_outs[i].at[me],
            send_sem=swap_send.at[i, step],
            recv_sem=swap_recv.at[i, step],
            device_id=at_expert(to),
            device_id_type=MESH,
        )

    def arrived(i, origin):
        copy(i, outs[i].at[origin], origin, 0, partner).wait_recv()

    def along(i, origin, source, upward, downward, act):
        if upward:

            @pl.when(line < 3)
            def _():
                act(copy(i, source, origin, 0, me + 4))

        if downward:

            @pl.when(line > 0)
            def _():
                act(copy(i, source, origin, 1, me - 4))

        act(copy(i, source, origin, 2, mate))
        act(copy(i, source, origin, 3, partner))

    def walk(act, wait):
        for far in range(1, 5):
            if far < 4:

                @pl.when(line >= far)
                def _():
                    origin = me - 4 * far
                    for i in range(n):
                        wait(i, origin)
                        along(i, origin, outs[i].at[origin], True, False, act)

                @pl.when(line + far <= 3)
                def _():
                    origin = me + 4 * far
                    for i in range(n):
                        wait(i, origin)
                        along(i, origin, outs[i].at[origin], False, True, act)

            for sign in (-1, 1) if far > 1 else (1,):
                step = sign * (far - 1)

                @pl.when((line + step >= 0) & (line + step <= 3))
                def _():
                    origin = mate + 4 * step
                    for i in range(n):
                        wait(i, origin)
                        act(copy(i, outs[i].at[origin], origin, 3, partner))

    def start(c):
        c.start()

    def sent(c):
        c.wait_send()

    for i in range(n):
        along(i, me, x_refs[i], True, True, start)
    for i in range(m):
        for step in range(1, 16):
            swap_copy(i, step).start()
    for i in range(n + m):
        own_copy(i).start()
    walk(start, arrived)
    for i in range(n):
        for index in range(8):
            arrived(i, 2 * index + 1 - core)
    for i in range(n):
        along(i, me, x_refs[i], True, True, sent)
    walk(sent, lambda i, origin: None)
    for i in range(m):
        for step in range(1, 16):
            swap_copy(i, step).wait()
    for i in range(n + m):
        own_copy(i).wait()


def ring_gather(values, swaps, collective):
    n, m = len(values), len(swaps)
    sent = 2 * (15 * sum(v.size for v in values) + sum(v.size for v in swaps))
    sems = pltpu.SemaphoreType.DMA
    anywhere = pl.BlockSpec(memory_space=pl.ANY)
    outs = pl.pallas_call(
        functools.partial(gather_kernel, n, m),
        out_shape=[jax.ShapeDtypeStruct((16,) + v.shape, v.dtype) for v in values]
        + [jax.ShapeDtypeStruct(v.shape, v.dtype) for v in swaps],
        in_specs=[pl.BlockSpec(memory_space=pltpu.VMEM)] * (n + m),
        out_specs=[anywhere] * (n + m),
        scratch_shapes=[
            sems((n + m,)),
            sems((n, 16, 4)),
            sems((n, 16)),
            sems((max(m, 1), 16)),
            sems((max(m, 1), 16)),
        ],
        compiler_params=pltpu.CompilerParams(collective_id=collective, has_side_effects=True),
        cost_estimate=pl.CostEstimate(flops=0, bytes_accessed=16 * sent, transcendentals=0),
    )(*values, *swaps)
    return [o.reshape(-1, o.shape[-1]) for o in outs[:n]] + list(outs[n:])


def scatter_kernel(n, *refs):
    parts = [(refs[i], refs[n + i]) + refs[2 * n + 5 * i : 2 * n + 5 * i + 5] for i in range(n)]
    (
        core_send, core_recv, mate_send, mate_recv, up_send, up_recv, down_send, down_recv,
    ) = refs[7 * n :]
    me, line, pair, core = grid_place()
    partner, mate = greet_neighbours(me, line, pair, core)

    def block(i, dest):
        ref = parts[i][0]
        return ref.at[dest] if len(ref.shape) == 3 else ref.at[:, dest]

    def remote(source, target, send, recv, to):
        return pltpu.make_async_remote_copy(
            src_ref=source, dst_ref=target, send_sem=send, recv_sem=recv,
            device_id=at_expert(to), device_id_type=MESH,
        )

    def core_copy(i, index):
        return remote(
            block(i, 2 * index + 1 - core), parts[i][2].at[index],
            core_send.at[i, index], core_recv.at[i, index], partner,
        )

    def mate_copy(i, dest):
        return remote(
            parts[i][6].at[2 * dest + 1 - pair], parts[i][3].at[dest],
            mate_send.at[i, dest], mate_recv.at[i, dest], mate,
        )

    def up_copy(i, dest):
        return remote(
            parts[i][6].at[2 * dest + pair], parts[i][4].at[dest],
            up_send.at[i, dest], up_recv.at[i, dest], me + 4,
        )

    def down_copy(i, dest):
        return remote(
            parts[i][6].at[2 * dest + pair], parts[i][5].at[dest],
            down_send.at[i, dest], down_recv.at[i, dest], me - 4,
        )

    def add(target, left, right):
        if len(left.shape) == 3:
            for i in range(left.shape[0]):
                add(target.at[i], left.at[i], right.at[i])
            return
        tile = min(16, left.shape[0])

        @pl.loop(0, left.shape[0] // tile)
        def _(i):
            at = pl.ds(pl.multiple_of(i * tile, tile), tile)
            target[at, :] = (left[at, :].astype(f32) + right[at, :].astype(f32)).astype(
                target.dtype
            )

    def farthest(act):
        for far in (3, 2, 1, 0):
            for step in (-far, far) if far else (0,):

                @pl.when((line + step >= 0) & (line + step <= 3))
                def _():
                    for i in range(n):
                        act(i, line + step, step)

    def send_core(i, dest, step):
        core_copy(i, 2 * dest + 1 - pair).start()

    def send_core_own(i, dest, step):
        core_copy(i, 2 * dest + pair).start()

    def chip_sum(i, index):
        core_copy(i, index).wait_recv()
        add(parts[i][6].at[index], block(i, 2 * index + core), parts[i][2].at[index])

    def to_mate(i, dest, step):
        chip_sum(i, 2 * dest + 1 - pair)
        mate_copy(i, dest).start()

    def keep(i, dest, step):
        chip_sum(i, 2 * dest + pair)

    def along(i, dest, step):
        out, up_in, down_in, total = parts[i][1], parts[i][4], parts[i][5], parts[i][6]
        mine = total.at[2 * dest + pair]
        mate_copy(i, dest).wait_recv()
        if step == 0:
            add(out, mine, parts[i][3].at[dest])
            mine = out
        else:
            add(mine, mine, parts[i][3].at[dest])
        if step >= 0:

            @pl.when(line > 0)
            def _():
                up_copy(i, dest).wait_recv()
                add(mine, mine, up_in.at[dest])

        if step <= 0:

            @pl.when(line < 3)
            def _():
                down_copy(i, dest).wait_recv()
                add(mine, mine, down_in.at[dest])

        if step > 0:
            up_copy(i, dest).start()
        elif step < 0:
            down_copy(i, dest).start()

    def finish(i, dest, step):
        mate_copy(i, dest).wait_send()
        core_copy(i, 2 * dest + 1 - pair).wait_send()
        core_copy(i, 2 * dest + pair).wait_send()
        if step > 0:
            up_copy(i, dest).wait_send()
        elif step < 0:
            down_copy(i, dest).wait_send()

    for act in (send_core, send_core_own, to_mate, keep, along, finish):
        farthest(act)


def ring_scatter(values, collective):
    n = len(values)
    shapes = [v.shape[1:] if len(v.shape) == 3 else v.shape[:1] + v.shape[2:] for v in values]
    buffers = [pltpu.VMEM((k,) + s, bf16) for s in shapes for k in (8, 4, 4, 4, 8)]
    sent = 30 * sum(math.prod(s) for s in shapes)
    vmem = pl.BlockSpec(memory_space=pltpu.VMEM)
    return pl.pallas_call(
        functools.partial(scatter_kernel, n),
        out_shape=[jax.ShapeDtypeStruct(s, f32) for s in shapes],
        in_specs=[vmem] * n,
        out_specs=[vmem] * n,
        scratch_shapes=buffers
        + [pltpu.SemaphoreType.DMA((n, k)) for k in (8, 8, 4, 4, 4, 4, 4, 4)],
        compiler_params=pltpu.CompilerParams(collective_id=collective, has_side_effects=True),
        cost_estimate=pl.CostEstimate(flops=0, bytes_accessed=16 * sent, transcendentals=0),
    )(*values)


def swap_kernel(source, target, x_ref, out_ref, own_sem, send_sem, recv_sem):
    me = lax.axis_index(EXPERT)
    greet_all(me)

    def copy(step):
        to = (me + step) % 16
        return pltpu.make_async_remote_copy(
            src_ref=source(x_ref, to),
            dst_ref=target(out_ref, me),
            send_sem=send_sem.at[step],
            recv_sem=recv_sem.at[step],
            device_id=at_expert(to),
            device_id_type=MESH,
        )

    for step in range(1, 16):
        copy(step).start()
    own = pltpu.make_async_copy(source(x_ref, me), target(out_ref, me), own_sem)
    own.start()
    for step in range(1, 16):
        copy(step).wait()
    own.wait()


def swap_call(source, target, value, shape, collective):
    sent = value.size * 2
    return pl.pallas_call(
        functools.partial(swap_kernel, source, target),
        out_shape=jax.ShapeDtypeStruct(shape, value.dtype),
        in_specs=[pl.BlockSpec(memory_space=pltpu.VMEM)],
        out_specs=pl.BlockSpec(memory_space=pltpu.VMEM),
        scratch_shapes=[
            pltpu.SemaphoreType.DMA,
            pltpu.SemaphoreType.DMA((16,)),
            pltpu.SemaphoreType.DMA((16,)),
        ],
        compiler_params=pltpu.CompilerParams(collective_id=collective, has_side_effects=True),
        cost_estimate=pl.CostEstimate(flops=0, bytes_accessed=64 * sent, transcendentals=0),
    )(value)


def block_rows(span):
    return lambda ref, at: ref.at[:, pl.ds(pl.multiple_of(at * span, span), span), :]


def head_columns(columns):
    return lambda ref, at: ref.at[:, :, pl.ds(pl.multiple_of(at * columns, columns), columns)]


def heads_to_tokens(value, span, collective):
    seqs = value.shape[0]
    return swap_call(
        block_rows(span), head_columns(VD), value, (seqs, span, HEADS * VD), collective
    )


def tokens_to_heads(value, collective):
    seqs, span, _ = value.shape
    return swap_call(
        head_columns(VD), block_rows(span), value, (seqs, span * HEADS, VD), collective
    )


def per_device(
    inputs,
    segments,
    expert_picks,
    priority,
    cotangent,
    query_weight,
    latent_down,
    latent_up,
    output_weight,
    attn_gain,
    latent_gain,
    router_weight,
    shared_gate,
    shared_up,
    shared_down,
    moe_gain,
    expert_gate,
    expert_up,
    expert_down,
):
    groups = lax.axis_size(EXPERT)
    replicas = lax.axis_size(DP)
    place = lax.axis_index(EXPERT)
    seqs, span, width = inputs.shape
    length = span * groups
    own = seqs * span
    tokens = own * groups
    experts = groups
    capacity = (9 * span * TOP + 8 * experts - 1) // (8 * experts)
    scale = 1.0 / math.sqrt(HD + RD)
    rows = query_weight.shape[0]
    part = shared_down.shape[0]
    hidden_own = part * replicas
    QD = HD + RD

    def by_sequence(value):
        return value.reshape(groups, seqs, span, -1).transpose(1, 0, 2, 3).reshape(
            seqs, length, -1
        )

    def by_owner(value):
        return value.astype(bf16).reshape(groups, own, -1)

    def by_block(value):
        return value.reshape(seqs, groups, span, -1).transpose(1, 0, 2, 3).reshape(tokens, -1)

    x_low = inputs.reshape(own, width)
    cot_own = cotangent.reshape(own, width)

    order = priority[:, None, :] < priority[:, :, None]
    hit = jnp.sum(
        (expert_picks[..., None] == jnp.arange(experts, dtype=jnp.int32)).astype(f32), axis=2
    )
    ranks = einsum("stu,sue->ste", order.astype(bf16), hit.astype(bf16))
    codes = jnp.where((hit > 0) & (ranks < capacity), ranks, -1.0).astype(bf16)

    pad = rows - latent_gain.shape[0]
    small = jnp.concatenate(
        [
            latent_down,
            router_weight,
            attn_gain[:, None],
            moe_gain[:, None],
            jnp.pad(latent_gain, (0, pad))[:, None],
            jnp.zeros((rows, 45), bf16),
        ],
        axis=1,
    )
    small = dp_gather(small)
    query_parts = query_weight.reshape(rows, HEADS, QD).transpose(1, 0, 2)
    lup_rows = latent_up.shape[0]
    code_rows = -(lup_rows + 1) % 16 + 1
    code_part = jnp.pad(
        codes.reshape(own, 1, experts).T, ((0, 0), (0, code_rows - 1), (0, HD + VD - own))
    )
    lup_parts = jnp.concatenate(
        [latent_up.reshape(lup_rows, HEADS, HD + VD).transpose(1, 0, 2), code_part], axis=1
    )
    small_all, x_all, query_swap, lup_swap = ring_gather(
        [small, x_low], [query_parts, lup_parts], 1
    )
    small_all = (
        small_all.reshape(groups, replicas, rows, -1).transpose(1, 0, 2, 3).reshape(width, -1)
    )
    ldown_all = small_all[:, : RANK + RD]
    router_all = small_all[:, RANK + RD : RANK + RD + experts]
    gains = small_all[:, RANK + RD + experts :].astype(f32)
    gain_attn = gains[:, 0]
    gain_moe = gains[:, 1]
    gain_lat = gains[:, 2].reshape(-1, rows)[:, : latent_gain.shape[0]].reshape(-1)

    wq = dp_gather(query_swap.reshape(groups * rows, QD))
    lup = dp_gather(lup_swap[:, :lup_rows].reshape(groups * lup_rows, HD + VD))
    code = lup_swap[:, lup_rows, :own].astype(f32).reshape(tokens)

    def columns_of(weight):
        return (
            weight.reshape(rows, replicas, groups, part)
            .transpose(2, 0, 1, 3)
            .reshape(groups, rows, hidden_own)
        )

    gate_up_parts = jnp.concatenate([columns_of(shared_gate), columns_of(shared_up)], axis=2)
    gate_up_swap = expert_swap(gate_up_parts)
    gate_up = dp_gather(gate_up_swap.reshape(groups * rows, 2 * hidden_own))
    gate_up_router = jnp.concatenate([gate_up, router_all], axis=1)
    sdown = dp_gather(shared_down)
    gate_w = dp_gather(expert_gate[0])
    up_w = dp_gather(expert_up[0])
    down_w = dp_gather(expert_down[0])
    out_t = gather_rows(output_weight.T, BOTH)

    at_block = jnp.arange(groups, dtype=jnp.int32)[:, None, None] * span
    positions = jnp.broadcast_to(
        at_block + jnp.arange(span, dtype=jnp.int32), (groups, seqs, span)
    ).reshape(tokens)
    tables = lax.optimization_barrier(angle_tables(positions, RD))
    normed_one, _ = norm_parts(x_all.astype(f32))
    h_one = (normed_one * gain_attn).astype(bf16)
    query_raw = product(h_one, wq)
    query = jnp.concatenate(
        [query_raw[:, :HD], rotate(query_raw[:, HD:], tables)], axis=-1
    ).astype(bf16)
    down = product(h_one, ldown_all)
    normed_lat, factor_lat = norm_parts(down[:, :RANK])
    latent = (normed_lat * gain_lat).astype(bf16)
    key_rope = rotate(down[:, RANK:], tables).astype(bf16)
    expanded = product(latent, lup).astype(bf16)
    query_s = by_sequence(query)
    key_s = by_sequence(jnp.concatenate([expanded[:, :HD], key_rope], axis=-1))
    value_s = by_sequence(expanded[:, HD:])
    at = jnp.arange(length, dtype=jnp.int32)
    mask = (at[None, None, :] <= at[None, :, None]) & (
        segments[:, None, :] == segments[:, :, None]
    )
    scores = jnp.where(mask, einsum("sqd,skd->sqk", query_s, key_s) * scale, masked_score)
    top_score = jnp.max(scores, axis=-1, keepdims=True)
    weights_exp = jnp.exp(scores - top_score)
    probs_attn = (weights_exp / jnp.sum(weights_exp, axis=-1, keepdims=True)).astype(bf16)
    heads_s = einsum("sqk,skd->sqd", probs_attn, value_s).astype(bf16)
    heads_own = heads_to_tokens(heads_s, span, 3).reshape(own, HEADS * VD)

    x_second = x_low.astype(f32) + right_product(heads_own, out_t)
    normed_two, factor_two = norm_parts(x_second)
    (h_two,) = ring_gather([(normed_two * gain_moe).astype(bf16)], [], 2)

    cot_all = gather_rows(cot_own, EXPERT)

    chunks = 4
    chunk = tokens // chunks
    blocks = chunk // span
    slots = blocks * capacity
    slot_at = jnp.arange(slots, dtype=jnp.int32)
    token_at = jnp.arange(chunk, dtype=jnp.int32)
    select = (
        (slot_at[:, None] // capacity == token_at[None, :] // span)[None]
        & (
            (slot_at % capacity).astype(f32)[None, :, None]
            == code.reshape(chunks, chunk)[:, None, :]
        )
    ).astype(bf16)
    select = lax.optimization_barrier(select)

    def to_slots(values):
        return einsum("cst,ctd->csd", select, values.reshape(chunks, chunk, -1)).astype(bf16).reshape(
            chunks * slots, -1
        )

    def to_tokens(values):
        return einsum("cst,csd->ctd", select, values.reshape(chunks, slots, -1)).reshape(tokens, -1)

    pre = product(h_two, gate_up_router)
    shared_a = pre[:, :hidden_own]
    shared_b = pre[:, hidden_own : 2 * hidden_own]
    gate_probs = jax.nn.softmax(pre[:, 2 * hidden_own :], axis=-1)
    shared_hidden = (jax.nn.silu(shared_a) * shared_b).astype(bf16)
    mine = (jnp.arange(experts, dtype=jnp.int32) == place).astype(f32)
    own_prob = jnp.sum(gate_probs * mine, axis=-1)
    slot_prob = jnp.sum(
        select.astype(f32) * own_prob.reshape(chunks, 1, chunk), axis=-1
    ).reshape(chunks * slots, 1)
    expert_in = to_slots(h_two)
    gate_pre = product(expert_in, gate_w)
    up_pre = product(expert_in, up_w)
    expert_hidden = (jax.nn.silu(gate_pre) * up_pre).astype(bf16)
    expert_out = product(expert_hidden, down_w).astype(bf16).astype(f32)
    partial = product(shared_hidden, sdown) + to_tokens((slot_prob * expert_out).astype(bf16))
    partial = partial.astype(bf16)
    result = x_second + scatter_rows(partial, EXPERT).astype(f32)
    result = result.astype(bf16).reshape(seqs, span, width)

    grad_slots = to_slots(cot_all)
    hidden_grad = right_product(cot_all, sdown)
    sdown_grad = left_product(shared_hidden, cot_all)
    shared_a_grad = (hidden_grad * shared_b * silu_slope(shared_a)).astype(bf16)
    shared_b_grad = (hidden_grad * jax.nn.silu(shared_a)).astype(bf16)
    grad_wide = grad_slots.astype(f32)
    slot_grad = (slot_prob * grad_wide).astype(bf16)
    match = jnp.sum(grad_wide * expert_out, axis=-1).reshape(chunks, slots, 1)
    prob_grad = jnp.sum(select.astype(f32) * match, axis=1).reshape(tokens, 1)
    logit_grad = (gate_probs * prob_grad * (mine - own_prob[:, None])).astype(bf16)
    pre_grad = jnp.concatenate([shared_a_grad, shared_b_grad, logit_grad], axis=1)
    expert_hidden_grad = right_product(slot_grad, down_w)
    expert_a_grad = (expert_hidden_grad * up_pre * silu_slope(gate_pre)).astype(bf16)
    expert_b_grad = (expert_hidden_grad * jax.nn.silu(gate_pre)).astype(bf16)
    in_grad = right_product(expert_a_grad, gate_w) + right_product(expert_b_grad, up_w)
    in_grad = in_grad.astype(bf16)
    h_two_partial = right_product(pre_grad, gate_up_router) + to_tokens(in_grad)
    routed_down_grad = dp_scatter_product(expert_hidden, slot_grad)
    routed_gate_grad = dp_scatter_product(expert_in, expert_a_grad)
    routed_up_grad = dp_scatter_product(expert_in, expert_b_grad)
    (h_two_grad,) = ring_scatter([by_owner(h_two_partial)], 4)
    pre_weight_grad = left_product(h_two, pre_grad)
    sdown_owned = dp_scatter(sdown_grad)
    gate_up_owned = dp_scatter(pre_weight_grad[:, : 2 * hidden_own]).astype(bf16)
    router_grad = pre_weight_grad[:, 2 * hidden_own :]

    gmoe_grad = jnp.sum(h_two_grad * normed_two, axis=0)
    x_second_grad = cot_own.astype(f32) + norm_back(h_two_grad * gain_moe, normed_two, factor_two)
    attn_low = x_second_grad.astype(bf16)
    heads_grad = product(attn_low, out_t).astype(bf16)
    grad_s = tokens_to_heads(heads_grad.reshape(seqs, span, HEADS * VD), 5)
    low_all = gather_rows(attn_low, EXPERT)
    gate_up_owned = expert_swap(
        gate_up_owned.reshape(groups, rows, 2 * hidden_own)
    ).astype(f32)

    def owned_columns(value):
        return (
            value.reshape(groups, rows, replicas, part)
            .transpose(1, 2, 0, 3)
            .reshape(rows, replicas * groups * part)
        )

    sgate_owned = owned_columns(gate_up_owned[:, :, :hidden_own])
    sup_owned = owned_columns(gate_up_owned[:, :, hidden_own:])
    probs_grad = einsum("sqd,skd->sqk", grad_s, value_s)
    spread = jnp.sum(grad_s.astype(f32) * heads_s.astype(f32), axis=-1, keepdims=True)
    score_grad = (probs_attn.astype(f32) * (probs_grad - spread) * scale).astype(bf16)
    value_grad = einsum("sqk,sqd->skd", probs_attn, grad_s)
    key_grad = einsum("sqk,sqd->skd", score_grad, query_s)
    query_grad = by_block(einsum("sqk,skd->sqd", score_grad, key_s))
    expanded_grad = by_block(
        jnp.concatenate([key_grad[..., :HD], value_grad], axis=-1).astype(bf16)
    )
    rope_grad = by_block(key_grad[..., HD:])
    lup_grad = left_product(latent, expanded_grad)
    latent_grad = right_product(expanded_grad, lup)
    glat_grad = jnp.sum(latent_grad * normed_lat, axis=0)
    joint_grad = jnp.concatenate(
        [
            norm_back(latent_grad * gain_lat, normed_lat, factor_lat),
            unrotate(rope_grad, tables),
            unrotate(query_grad[:, HD:], tables),
            query_grad[:, :HD],
        ],
        axis=-1,
    ).astype(bf16)
    joint_weight = jnp.concatenate([ldown_all, wq[:, HD:], wq[:, :HD]], axis=1)
    h_one_partial = right_product(joint_grad, joint_weight)
    joint_weight_grad = left_product(h_one, joint_grad)
    gattn_grad = jnp.sum(joint_weight_grad * joint_weight.astype(f32), axis=1) / gain_attn
    out_grad = left_product(low_all, by_block(heads_s))
    down_at = RANK + RD
    back_grad = jnp.concatenate(
        [
            joint_weight_grad[:, down_at + RD :],
            out_grad,
            joint_weight_grad[:, down_at : down_at + RD],
            lup_grad.reshape(width, -1),
        ],
        axis=1,
    )
    back_grad = dp_scatter(back_grad).astype(bf16)
    back_owned = expert_swap(back_grad.reshape(groups, rows, -1)).astype(f32)
    q_owned = jnp.concatenate(
        [back_owned[:, :, :HD], back_owned[:, :, HD + VD : HD + VD + RD]], axis=2
    )
    q_owned = q_owned.transpose(1, 0, 2).reshape(rows, HEADS * QD)
    out_owned = back_owned[:, :, HD : HD + VD].transpose(0, 2, 1).reshape(HEADS * VD, rows)
    lup_owned = back_owned[:, :, HD + VD + RD :].reshape(groups, lup_rows, HD + VD)
    lup_owned = lup_owned.transpose(1, 0, 2).reshape(lup_rows, HEADS * (HD + VD))
    glat_column = jnp.pad(
        glat_grad.reshape(-1, latent_gain.shape[0]), ((0, 0), (0, pad))
    ).reshape(-1)
    lane = jnp.arange(128, dtype=jnp.int32)
    small_grad = jnp.pad(router_grad, ((0, 0), (0, 128 - experts)))
    for at_lane, column in enumerate((gattn_grad, gmoe_grad, glat_column)):
        small_grad = jnp.where(lane == experts + at_lane, column[:, None], small_grad)

    def by_row_owner(value):
        return value.astype(bf16).reshape(replicas, groups, rows, -1)

    ldown_owned, small_owned, h_one_grad = ring_scatter(
        [
            by_row_owner(joint_weight_grad[:, :down_at]),
            by_row_owner(small_grad),
            by_owner(h_one_partial),
        ],
        6,
    )
    normed_own, factor_own = norm_parts(x_low.astype(f32))
    input_grad = x_second_grad + norm_back(h_one_grad * gain_attn, normed_own, factor_own)
    input_grad = input_grad.astype(bf16).reshape(seqs, span, width)
    small_owned = dp_scatter(
        jnp.concatenate([ldown_owned, small_owned], axis=2).reshape(replicas * rows, -1)
    )
    ldown_owned = small_owned[:, :down_at]
    router_owned = small_owned[:, down_at : down_at + experts]
    gain_owned = small_owned[:, down_at + experts :]
    return (
        result,
        input_grad,
        q_owned,
        ldown_owned,
        lup_owned,
        out_owned,
        gain_owned[:, 0],
        gain_owned[: latent_gain.shape[0], 2],
        router_owned,
        sgate_owned,
        sup_owned,
        sdown_owned,
        gain_owned[:, 1],
        routed_gate_grad[None],
        routed_up_grad[None],
        routed_down_grad[None],
    )


def solution(mesh):
    return jax.shard_map(
        per_device,
        mesh=mesh,
        in_specs=(
            TOKENS, P(DP, None), TOKENS, P(DP, EXPERT), TOKENS,
            ROWS, ROWS, ROWS, P(None, BOTH), P(BOTH), P(BOTH),
            ROWS, ROWS, ROWS, ROWS, P(BOTH), ROUTED, ROUTED, ROUTED,
        ),
        out_specs=(
            TOKENS, TOKENS, ROWS, ROWS, ROWS, P(None, BOTH), P(BOTH), P(BOTH),
            ROWS, ROWS, ROWS, ROWS, P(BOTH), ROUTED, ROUTED, ROUTED,
        ),
        check_vma=False,
    )
```

```python
import functools
import math

import jax
import jax.numpy as jnp
from jax import lax
from jax.experimental import pallas as pl
from jax.experimental.pallas import tpu as pltpu
from jax.sharding import PartitionSpec as P

HEADS = 16
HD = 128
RD = 64
VD = 128
RANK = 512
TOP = 6

epsilon = 1e-06
masked_score = -1e30
DP = "dp"
EXPERT = "expert"
BOTH = (DP, EXPERT)
TOKENS = P(DP, EXPERT, None)
ROWS = P(BOTH, None)
ROUTED = P(EXPERT, DP, None)
f32 = jnp.float32
bf16 = jnp.bfloat16


def product(left, right):
    return jnp.dot(left, right, preferred_element_type=f32)


def left_product(left, right):
    return lax.dot_general(left, right, (((0,), (0,)), ((), ())), preferred_element_type=f32)


def right_product(left, right):
    return lax.dot_general(left, right, (((1,), (1,)), ((), ())), preferred_element_type=f32)


def einsum(spec, left, right):
    return jnp.einsum(spec, left, right, preferred_element_type=f32)


def norm_parts(values):
    factor = lax.rsqrt(jnp.mean(values * values, axis=-1, keepdims=True) + epsilon)
    return (values * factor, factor)


def norm_back(grad_normed, normed, factor):
    return factor * (grad_normed - normed * jnp.mean(grad_normed * normed, axis=-1, keepdims=True))


def angle_tables(positions, width):
    half = width // 2
    freqs = jnp.power(10000.0, -2.0 * jnp.arange(half, dtype=f32) / width)
    angles = positions.astype(f32)[:, None] * freqs[None, :]
    return (jnp.cos(angles), jnp.sin(angles))


def silu_slope(pre):
    sigma = jax.nn.sigmoid(pre)
    return sigma * (1.0 + pre * (1.0 - sigma))


def dp_swap(value):
    return lax.ppermute(value, DP, [(0, 1), (1, 0)])


def dp_gather(value):
    if lax.axis_size(DP) == 2:
        other = dp_swap(value)
        first = lax.axis_index(DP) == 0
        return jnp.concatenate(
            [jnp.where(first, value, other), jnp.where(first, other, value)], axis=0
        )
    return lax.all_gather(value, DP, axis=0, tiled=True)


def dp_scatter_product(left, right):
    if lax.axis_size(DP) == 2:
        first = lax.axis_index(DP) == 0
        half = left.shape[1] // 2
        low, high = left[:, :half], left[:, half:]
        sent = left_product(jnp.where(first, high, low), right).astype(bf16)
        other = dp_swap(sent)
        return left_product(jnp.where(first, low, high), right) + other.astype(f32)
    return dp_scatter(left_product(left, right))


def dp_scatter(value):
    if lax.axis_size(DP) == 2:
        rows = value.shape[0] // 2
        at = lax.axis_index(DP)
        sent = lax.dynamic_slice_in_dim(value, (1 - at) * rows, rows, 0)
        kept = lax.dynamic_slice_in_dim(value, at * rows, rows, 0)
        return kept + dp_swap(sent.astype(bf16)).astype(f32)
    return lax.psum_scatter(
        value.astype(bf16), DP, scatter_dimension=0, tiled=True
    ).astype(f32)


def expert_swap(value):
    return lax.all_to_all(value, EXPERT, split_axis=0, concat_axis=0, tiled=True)


def gather_rows(value, axes):
    return lax.all_gather(value, axes, axis=0, tiled=True)


def scatter_rows(value, axes):
    return lax.psum_scatter(value, axes, scatter_dimension=0, tiled=True)


MESH = pl.DeviceIdType.MESH


def at_expert(index):
    return {EXPERT: index}


def grid_place():
    me = lax.axis_index(EXPERT)
    return me, me // 4, (me // 2) % 2, me % 2


def greet_neighbours(me, line, pair, core):
    partner = me + 1 - 2 * core
    mate = me + 2 - 4 * pair
    barrier = pltpu.get_barrier_semaphore()
    for other in (partner, mate):
        pl.semaphore_signal(barrier, inc=1, device_id=at_expert(other), device_id_type=MESH)

    @pl.when(line < 3)
    def _():
        pl.semaphore_signal(barrier, inc=1, device_id=at_expert(me + 4), device_id_type=MESH)

    @pl.when(line > 0)
    def _():
        pl.semaphore_signal(barrier, inc=1, device_id=at_expert(me - 4), device_id_type=MESH)

    pl.semaphore_wait(barrier, 3 + jnp.where((line > 0) & (line < 3), 1, 0))
    return partner, mate


def greet_all(me):
    barrier = pltpu.get_barrier_semaphore()
    for step in range(1, 16):
        pl.semaphore_signal(
            barrier, inc=1, device_id=at_expert((me + step) % 16), device_id_type=MESH
        )
    pl.semaphore_wait(barrier, 15)


def gather_kernel(n, m, *refs):
    x_refs, swap_refs = refs[:n], refs[n : n + m]
    outs, swap_outs = refs[n + m : 2 * n + m], refs[2 * n + m : 2 * (n + m)]
    own_sem, send_sem, recv_sem, swap_send, swap_recv = refs[2 * (n + m) :]
    me, line, pair, core = grid_place()
    if m:
        greet_all(me)
        partner, mate = me + 1 - 2 * core, me + 2 - 4 * pair
    else:
        partner, mate = greet_neighbours(me, line, pair, core)

    def own_copy(i):
        if i < n:
            return pltpu.make_async_copy(x_refs[i], outs[i].at[me], own_sem.at[i])
        i -= n
        return pltpu.make_async_copy(
            swap_refs[i].at[me], swap_outs[i].at[me], own_sem.at[n + i]
        )

    def copy(i, source, origin, way, to):
        return pltpu.make_async_remote_copy(
            src_ref=source,
            dst_ref=outs[i].at[origin],
            send_sem=send_sem.at[i, origin, way],
            recv_sem=recv_sem.at[i, origin],
            device_id=at_expert(to),
            device_id_type=MESH,
        )

    def swap_copy(i, step):
        to = (me + step) % 16
        return pltpu.make_async_remote_copy(
            src_ref=swap_refs[i].at[to],
            dst_ref=swap_outs[i].at[me],
            send_sem=swap_send.at[i, step],
            recv_sem=swap_recv.at[i, step],
            device_id=at_expert(to),
            device_id_type=MESH,
        )

    def arrived(i, origin):
        copy(i, outs[i].at[origin], origin, 0, partner).wait_recv()

    def along(i, origin, source, upward, downward, act):
        if upward:

            @pl.when(line < 3)
            def _():
                act(copy(i, source, origin, 0, me + 4))

        if downward:

            @pl.when(line > 0)
            def _():
                act(copy(i, source, origin, 1, me - 4))

        act(copy(i, source, origin, 2, mate))
        act(copy(i, source, origin, 3, partner))

    def walk(act, wait):
        for far in range(1, 5):
            if far < 4:

                @pl.when(line >= far)
                def _():
                    origin = me - 4 * far
                    for i in range(n):
                        wait(i, origin)
                        along(i, origin, outs[i].at[origin], True, False, act)

                @pl.when(line + far <= 3)
                def _():
                    origin = me + 4 * far
                    for i in range(n):
                        wait(i, origin)
                        along(i, origin, outs[i].at[origin], False, True, act)

            for sign in (-1, 1) if far > 1 else (1,):
                step = sign * (far - 1)

                @pl.when((line + step >= 0) & (line + step <= 3))
                def _():
                    origin = mate + 4 * step
                    for i in range(n):
                        wait(i, origin)
                        act(copy(i, outs[i].at[origin], origin, 3, partner))

    def start(c):
        c.start()

    def sent(c):
        c.wait_send()

    for i in range(n):
        along(i, me, x_refs[i], True, True, start)
    for i in range(m):
        for step in range(1, 16):
            swap_copy(i, step).start()
    for i in range(n + m):
        own_copy(i).start()
    walk(start, arrived)
    for i in range(n):
        for index in range(8):
            arrived(i, 2 * index + 1 - core)
    for i in range(n):
        along(i, me, x_refs[i], True, True, sent)
    walk(sent, lambda i, origin: None)
    for i in range(m):
        for step in range(1, 16):
            swap_copy(i, step).wait()
    for i in range(n + m):
        own_copy(i).wait()


def ring_gather(values, swaps, collective):
    n, m = len(values), len(swaps)
    sent = 2 * (15 * sum(v.size for v in values) + sum(v.size for v in swaps))
    sems = pltpu.SemaphoreType.DMA
    anywhere = pl.BlockSpec(memory_space=pl.ANY)
    outs = pl.pallas_call(
        functools.partial(gather_kernel, n, m),
        out_shape=[jax.ShapeDtypeStruct((16,) + v.shape, v.dtype) for v in values]
        + [jax.ShapeDtypeStruct(v.shape, v.dtype) for v in swaps],
        in_specs=[pl.BlockSpec(memory_space=pltpu.VMEM)] * (n + m),
        out_specs=[anywhere] * (n + m),
        scratch_shapes=[
            sems((n + m,)),
            sems((n, 16, 4)),
            sems((n, 16)),
            sems((max(m, 1), 16)),
            sems((max(m, 1), 16)),
        ],
        compiler_params=pltpu.CompilerParams(collective_id=collective, has_side_effects=True),
        cost_estimate=pl.CostEstimate(flops=0, bytes_accessed=16 * sent, transcendentals=0),
    )(*values, *swaps)
    return [o.reshape(-1, o.shape[-1]) for o in outs[:n]] + list(outs[n:])


def scatter_kernel(n, *refs):
    parts = [(refs[i], refs[n + i]) + refs[2 * n + 5 * i : 2 * n + 5 * i + 5] for i in range(n)]
    (
        core_send, core_recv, mate_send, mate_recv, up_send, up_recv, down_send, down_recv,
    ) = refs[7 * n :]
    me, line, pair, core = grid_place()
    partner, mate = greet_neighbours(me, line, pair, core)

    def block(i, dest):
        ref = parts[i][0]
        return ref.at[dest] if len(ref.shape) == 3 else ref.at[:, dest]

    def remote(source, target, send, recv, to):
        return pltpu.make_async_remote_copy(
            src_ref=source, dst_ref=target, send_sem=send, recv_sem=recv,
            device_id=at_expert(to), device_id_type=MESH,
        )

    def core_copy(i, index):
        return remote(
            block(i, 2 * index + 1 - core), parts[i][2].at[index],
            core_send.at[i, index], core_recv.at[i, index], partner,
        )

    def mate_copy(i, dest):
        return remote(
            parts[i][6].at[2 * dest + 1 - pair], parts[i][3].at[dest],
            mate_send.at[i, dest], mate_recv.at[i, dest], mate,
        )

    def up_copy(i, dest):
        return remote(
            parts[i][6].at[2 * dest + pair], parts[i][4].at[dest],
            up_send.at[i, dest], up_recv.at[i, dest], me + 4,
        )

    def down_copy(i, dest):
        return remote(
            parts[i][6].at[2 * dest + pair], parts[i][5].at[dest],
            down_send.at[i, dest], down_recv.at[i, dest], me - 4,
        )

    def add(target, left, right):
        if len(left.shape) == 3:
            for i in range(left.shape[0]):
                add(target.at[i], left.at[i], right.at[i])
            return
        tile = min(16, left.shape[0])

        @pl.loop(0, left.shape[0] // tile)
        def _(i):
            at = pl.ds(pl.multiple_of(i * tile, tile), tile)
            target[at, :] = (left[at, :].astype(f32) + right[at, :].astype(f32)).astype(
                target.dtype
            )

    def farthest(act):
        for far in (3, 2, 1, 0):
            for step in (-far, far) if far else (0,):

                @pl.when((line + step >= 0) & (line + step <= 3))
                def _():
                    for i in range(n):
                        act(i, line + step, step)

    def send_core(i, dest, step):
        core_copy(i, 2 * dest + 1 - pair).start()

    def send_core_own(i, dest, step):
        core_copy(i, 2 * dest + pair).start()

    def chip_sum(i, index):
        core_copy(i, index).wait_recv()
        add(parts[i][6].at[index], block(i, 2 * index + core), parts[i][2].at[index])

    def to_mate(i, dest, step):
        chip_sum(i, 2 * dest + 1 - pair)
        mate_copy(i, dest).start()

    def keep(i, dest, step):
        chip_sum(i, 2 * dest + pair)

    def along(i, dest, step):
        out, up_in, down_in, total = parts[i][1], parts[i][4], parts[i][5], parts[i][6]
        mine = total.at[2 * dest + pair]
        mate_copy(i, dest).wait_recv()
        if step == 0:
            add(out, mine, parts[i][3].at[dest])
            mine = out
        else:
            add(mine, mine, parts[i][3].at[dest])
        if step >= 0:

            @pl.when(line > 0)
            def _():
                up_copy(i, dest).wait_recv()
                add(mine, mine, up_in.at[dest])

        if step <= 0:

            @pl.when(line < 3)
            def _():
                down_copy(i, dest).wait_recv()
                add(mine, mine, down_in.at[dest])

        if step > 0:
            up_copy(i, dest).start()
        elif step < 0:
            down_copy(i, dest).start()

    def finish(i, dest, step):
        mate_copy(i, dest).wait_send()
        core_copy(i, 2 * dest + 1 - pair).wait_send()
        core_copy(i, 2 * dest + pair).wait_send()
        if step > 0:
            up_copy(i, dest).wait_send()
        elif step < 0:
            down_copy(i, dest).wait_send()

    for act in (send_core, send_core_own, to_mate, keep, along, finish):
        farthest(act)


def ring_scatter(values, collective):
    n = len(values)
    shapes = [v.shape[1:] if len(v.shape) == 3 else v.shape[:1] + v.shape[2:] for v in values]
    buffers = [pltpu.VMEM((k,) + s, bf16) for s in shapes for k in (8, 4, 4, 4, 8)]
    sent = 30 * sum(math.prod(s) for s in shapes)
    vmem = pl.BlockSpec(memory_space=pltpu.VMEM)
    return pl.pallas_call(
        functools.partial(scatter_kernel, n),
        out_shape=[jax.ShapeDtypeStruct(s, f32) for s in shapes],
        in_specs=[vmem] * n,
        out_specs=[vmem] * n,
        scratch_shapes=buffers
        + [pltpu.SemaphoreType.DMA((n, k)) for k in (8, 8, 4, 4, 4, 4, 4, 4)],
        compiler_params=pltpu.CompilerParams(collective_id=collective, has_side_effects=True),
        cost_estimate=pl.CostEstimate(flops=0, bytes_accessed=16 * sent, transcendentals=0),
    )(*values)


def swap_kernel(source, target, x_ref, out_ref, own_sem, send_sem, recv_sem):
    me = lax.axis_index(EXPERT)
    greet_all(me)

    def copy(step):
        to = (me + step) % 16
        return pltpu.make_async_remote_copy(
            src_ref=source(x_ref, to),
            dst_ref=target(out_ref, me),
            send_sem=send_sem.at[step],
            recv_sem=recv_sem.at[step],
            device_id=at_expert(to),
            device_id_type=MESH,
        )

    for step in range(1, 16):
        copy(step).start()
    own = pltpu.make_async_copy(source(x_ref, me), target(out_ref, me), own_sem)
    own.start()
    for step in range(1, 16):
        copy(step).wait()
    own.wait()


def swap_call(source, target, value, shape, collective):
    sent = value.size * 2
    return pl.pallas_call(
        functools.partial(swap_kernel, source, target),
        out_shape=jax.ShapeDtypeStruct(shape, value.dtype),
        in_specs=[pl.BlockSpec(memory_space=pltpu.VMEM)],
        out_specs=pl.BlockSpec(memory_space=pltpu.VMEM),
        scratch_shapes=[
            pltpu.SemaphoreType.DMA,
            pltpu.SemaphoreType.DMA((16,)),
            pltpu.SemaphoreType.DMA((16,)),
        ],
        compiler_params=pltpu.CompilerParams(collective_id=collective, has_side_effects=True),
        cost_estimate=pl.CostEstimate(flops=0, bytes_accessed=64 * sent, transcendentals=0),
    )(value)


def block_rows(span):
    return lambda ref, at: ref.at[:, pl.ds(pl.multiple_of(at * span, span), span), :]


def head_columns(columns):
    return lambda ref, at: ref.at[:, :, pl.ds(pl.multiple_of(at * columns, columns), columns)]


def heads_to_tokens(value, span, collective):
    seqs = value.shape[0]
    return swap_call(
        block_rows(span), head_columns(VD), value, (seqs, span, HEADS * VD), collective
    )


def tokens_to_heads(value, collective):
    seqs, span, _ = value.shape
    return swap_call(
        head_columns(VD), block_rows(span), value, (seqs, span * HEADS, VD), collective
    )


def matmul(left, right, dims):
    return lax.dot_general(left, right, (dims, ((), ())), preferred_element_type=f32)


ROWS_ROWS = ((0,), (0,))
COLS_COLS = ((1,), (1,))
COLS_ROWS = ((1,), (0,))


def full(shape):
    return pl.BlockSpec(shape, lambda *_: (0,) * len(shape), pipeline_mode=pl.Buffered(1))


def tiled(rows, columns):
    return pl.BlockSpec((rows, columns), lambda i: (i, 0))


def estimate(flops, nbytes):
    return pl.CostEstimate(
        flops=int(flops), bytes_accessed=int(nbytes), transcendentals=0
    )


def combine_kernel(dims, select_ref, slot_ref, left_ref, right_ref, out_ref):
    routed = matmul(select_ref[0], slot_ref[0], ROWS_ROWS)
    out_ref[...] = (routed + matmul(left_ref[...], right_ref[...], dims)).astype(bf16)


def combine(select, slot_rows, left, right, dims):
    chunks, slots, chunk = select.shape
    width = slot_rows.shape[-1]
    tile = 256
    per = chunk // tile
    inner = left.shape[1]
    return pl.pallas_call(
        functools.partial(combine_kernel, dims),
        grid=(chunks, per),
        in_specs=[
            pl.BlockSpec((1, slots, tile), lambda c, t: (c, 0, t)),
            pl.BlockSpec((1, slots, width), lambda c, t: (c, 0, 0)),
            pl.BlockSpec((tile, inner), lambda c, t: (c * per + t, 0)),
            full(right.shape),
        ],
        out_specs=pl.BlockSpec((tile, width), lambda c, t: (c * per + t, 0)),
        out_shape=jax.ShapeDtypeStruct((chunks * chunk, width), bf16),
        cost_estimate=estimate(
            2 * chunks * chunk * width * (slots + inner), 4 * chunks * chunk * width
        ),
    )(select, slot_rows.reshape(chunks, slots, width), left, right)


def turn(values, cosine, sine):
    lane = lax.broadcasted_iota(jnp.int32, values.shape, 1)
    other = jnp.where(lane % 64 < 32, pltpu.roll(values, 96, 1), pltpu.roll(values, 32, 1))
    return values * cosine + other * sine


def project_kernel(
    x_ref, weight_ref, lup_ref, gain_ref, gain_lat_ref, cos_ref, sin_ref,
    h_ref, query_ref, key_ref, value_ref, latent_ref, normed_ref, factor_ref,
):
    x = x_ref[...].astype(f32)
    factor = lax.rsqrt(jnp.mean(x * x, axis=-1, keepdims=True) + epsilon)
    h = (x * factor * gain_ref[...]).astype(bf16)
    h_ref[...] = h
    raw = matmul(h, weight_ref[...], COLS_ROWS)
    low = raw[:, :RANK]
    factor = lax.rsqrt(jnp.mean(low * low, axis=-1, keepdims=True) + epsilon)
    normed = low * factor
    normed_ref[...] = normed
    factor_ref[...] = factor
    latent = (normed * gain_lat_ref[...]).astype(bf16)
    latent_ref[...] = latent
    expanded = matmul(latent, lup_ref[...], COLS_ROWS)
    rope = turn(raw[:, RANK : RANK + 128], cos_ref[...], sin_ref[...])
    lane = lax.broadcasted_iota(jnp.int32, rope.shape, 1)
    query_ref[:, :HD] = raw[:, RANK + 128 :].astype(bf16)
    query_ref[:, HD:] = jnp.where(lane < RD, pltpu.roll(rope, 64, 1), 0.0).astype(bf16)
    key_ref[:, :HD] = expanded[:, :HD].astype(bf16)
    key_ref[:, HD:] = jnp.where(lane < RD, rope, 0.0).astype(bf16)
    value_ref[...] = expanded[:, HD:].astype(bf16)


def project(x_all, weight, lup, gain, gain_lat, cosine, sine):
    tokens, width = x_all.shape
    tile = 256
    outs = [
        ((tokens, width), bf16),
        ((tokens, HD + 128), bf16),
        ((tokens, HD + 128), bf16),
        ((tokens, VD), bf16),
        ((tokens, RANK), bf16),
        ((tokens, RANK), f32),
        ((tokens, 1), f32),
    ]
    return pl.pallas_call(
        project_kernel,
        name="project",
        grid=(tokens // tile,),
        in_specs=[
            tiled(tile, width),
            full(weight.shape),
            full(lup.shape),
            full((1, width)),
            full((1, RANK)),
            tiled(tile, 128),
            tiled(tile, 128),
        ],
        out_specs=[tiled(tile, s[1]) for s, _ in outs],
        out_shape=[jax.ShapeDtypeStruct(s, d) for s, d in outs],
        cost_estimate=estimate(2 * tokens * width * (weight.shape[1] + 64), 5 * tokens * width),
    )(x_all, weight, lup, gain[None], gain_lat[None], cosine, sine)


def attend_kernel(scale, query_ref, key_ref, value_ref, row_ref, col_ref, probs_ref, out_ref):
    length = probs_ref.shape[1]
    tile = 256
    query = query_ref[...].reshape(length, -1)
    key = key_ref[...].reshape(length, -1)
    value = value_ref[...].reshape(length, -1)
    for at in range(0, length, tile):
        seen = at + tile
        scores = matmul(query[at:seen], key[:seen], COLS_COLS) * scale
        row = at + lax.broadcasted_iota(jnp.int32, scores.shape, 0)
        col = lax.broadcasted_iota(jnp.int32, scores.shape, 1)
        keep = (col <= row) & (row_ref[0, :, :seen] == col_ref[0, at:seen, :])
        scores = jnp.where(keep, scores, masked_score)
        weights = jnp.exp(scores - jnp.max(scores, axis=-1, keepdims=True))
        probs = (weights / jnp.sum(weights, axis=-1, keepdims=True)).astype(bf16)
        probs_ref[0, at:seen, :seen] = probs
        if seen < length:
            probs_ref[0, at:seen, seen:] = jnp.zeros((tile, length - seen), bf16)
        out_ref[0, at:seen, :] = matmul(probs, value[:seen], COLS_ROWS).astype(bf16)


def of_sequence(groups, span, columns):
    return pl.BlockSpec((groups, 1, span, columns), lambda s: (0, s, 0, 0))


def attend(query, key, value, segments, scale, groups, seqs, span):
    length = groups * span
    view = lambda v: v.reshape(groups, seqs, span, -1)
    return pl.pallas_call(
        functools.partial(attend_kernel, scale),
        name="attend",
        grid=(seqs,),
        in_specs=[
            of_sequence(groups, span, HD + 128),
            of_sequence(groups, span, HD + 128),
            of_sequence(groups, span, VD),
            pl.BlockSpec((1, 1, length), lambda s: (s, 0, 0)),
            pl.BlockSpec((1, length, 1), lambda s: (s, 0, 0)),
        ],
        out_specs=[
            pl.BlockSpec((1, length, length), lambda s: (s, 0, 0)),
            pl.BlockSpec((1, length, VD), lambda s: (s, 0, 0)),
        ],
        out_shape=[
            jax.ShapeDtypeStruct((seqs, length, length), bf16),
            jax.ShapeDtypeStruct((seqs, length, VD), bf16),
        ],
        cost_estimate=estimate(seqs * length * length * 500, seqs * length * length * 4),
    )(view(query), view(key), view(value), segments[:, None, :], segments[:, :, None])


def attend_back_kernel(
    scale, probs_ref, grad_ref, out_ref, query_ref, key_ref, value_ref, dq_ref, dkv_ref, acc_ref
):
    length = probs_ref.shape[1]
    tile = 256
    _, _, span, _ = query_ref.shape
    per = tile // span
    query = query_ref[...].reshape(length, -1)
    key = key_ref[...].reshape(length, -1)
    value = value_ref[...].reshape(length, -1)
    wide = query.shape[1]
    for at in reversed(range(0, length, tile)):
        seen = at + tile
        grad = grad_ref[0, at:seen, :]
        spread = jnp.sum(
            grad.astype(f32) * out_ref[0, at:seen, :].astype(f32), axis=-1, keepdims=True
        )
        probs = probs_ref[0, at:seen, :seen]
        back = matmul(grad, value[:seen], COLS_COLS) - spread
        score_grad = (probs.astype(f32) * back * scale).astype(bf16)
        dq = matmul(score_grad, key[:seen], COLS_ROWS)
        dq_ref[at // span : seen // span, 0] = dq.reshape(per, span, wide)
        dk = matmul(score_grad, query[at:seen], ROWS_ROWS)
        dv = matmul(probs, grad, ROWS_ROWS)
        if seen == length:
            acc_ref[:, :wide] = dk
            acc_ref[:, wide:] = dv
        else:
            acc_ref[:seen, :wide] += dk
            acc_ref[:seen, wide:] += dv
    dkv_ref[...] = acc_ref[...].reshape(dkv_ref.shape)


def attend_back(probs, grad, out, query, key, value, scale, groups, span):
    seqs, length, _ = probs.shape
    wide = HD + 128
    view = lambda v: v.reshape(groups, seqs, span, -1)
    by_seq = lambda n: pl.BlockSpec((1, length, n), lambda s: (s, 0, 0))
    dq, dkv = pl.pallas_call(
        functools.partial(attend_back_kernel, scale),
        name="attend_back",
        grid=(seqs,),
        in_specs=[
            by_seq(length),
            by_seq(VD),
            by_seq(VD),
            of_sequence(groups, span, wide),
            of_sequence(groups, span, wide),
            of_sequence(groups, span, VD),
        ],
        out_specs=[of_sequence(groups, span, wide), of_sequence(groups, span, wide + VD)],
        out_shape=[
            jax.ShapeDtypeStruct((groups, seqs, span, wide), f32),
            jax.ShapeDtypeStruct((groups, seqs, span, wide + VD), f32),
        ],
        scratch_shapes=[pltpu.VMEM((length, wide + VD), f32)],
        cost_estimate=estimate(seqs * length * length * 1000, seqs * length * length * 4),
    )(probs, grad, out, view(query), view(key), view(value))
    return dq.reshape(-1, wide), dkv.reshape(-1, wide + VD)


def project_back_kernel(
    dq_ref, dkv_ref, weight_ref, lup_ref, gain_lat_ref, cos_ref, sin_ref,
    latent_ref, normed_ref, factor_ref, joint_ref, h_ref, lup_grad_ref, gain_grad_ref,
):
    dq = dq_ref[...]
    dkv = dkv_ref[...]
    lane = lax.broadcasted_iota(jnp.int32, (dq.shape[0], 128), 1)
    rope = jnp.where(lane < RD, dkv[:, HD : HD + 128], pltpu.roll(dq[:, HD:], 64, 1))
    rope = turn(rope, cos_ref[...], -sin_ref[...])
    expanded = jnp.concatenate([dkv[:, :HD], dkv[:, HD + 128 :]], axis=1).astype(bf16)
    latent_grad = matmul(expanded, lup_ref[...], COLS_COLS)
    normed = normed_ref[...]

    @pl.when(pl.program_id(0) == 0)
    def _():
        lup_grad_ref[...] = jnp.zeros_like(lup_grad_ref)
        gain_grad_ref[...] = jnp.zeros_like(gain_grad_ref)

    lup_grad_ref[...] += matmul(latent_ref[...], expanded, ROWS_ROWS)
    gain_grad_ref[...] += jnp.sum(latent_grad * normed, axis=0, keepdims=True)
    scaled = latent_grad * gain_lat_ref[...]
    down = factor_ref[...] * (
        scaled - normed * jnp.mean(scaled * normed, axis=-1, keepdims=True)
    )
    joint = jnp.concatenate([down, rope, dq[:, :HD]], axis=1).astype(bf16)
    joint_ref[...] = joint
    h_ref[...] = matmul(joint, weight_ref[...], COLS_COLS).astype(bf16)


def project_back(dq, dkv, weight, lup, gain_lat, cosine, sine, latent, normed, factor):
    tokens = dq.shape[0]
    width, joint = weight.shape
    tile = 256
    return pl.pallas_call(
        project_back_kernel,
        name="project_back",
        grid=(tokens // tile,),
        in_specs=[
            tiled(tile, dq.shape[1]),
            tiled(tile, dkv.shape[1]),
            full(weight.shape),
            full(lup.shape),
            full((1, RANK)),
            tiled(tile, 128),
            tiled(tile, 128),
            tiled(tile, RANK),
            tiled(tile, RANK),
            tiled(tile, 1),
        ],
        out_specs=[
            tiled(tile, joint),
            tiled(tile, width),
            pl.BlockSpec(lup.shape, lambda i: (0, 0)),
            pl.BlockSpec((1, RANK), lambda i: (0, 0)),
        ],
        out_shape=[
            jax.ShapeDtypeStruct((tokens, joint), bf16),
            jax.ShapeDtypeStruct((tokens, width), bf16),
            jax.ShapeDtypeStruct(lup.shape, f32),
            jax.ShapeDtypeStruct((1, RANK), f32),
        ],
        cost_estimate=estimate(2 * tokens * width * joint * 1.2, 6 * tokens * width),
    )(dq, dkv, weight, lup, gain_lat[None], cosine, sine, latent, normed, factor)


def per_device(
    inputs,
    segments,
    expert_picks,
    priority,
    cotangent,
    query_weight,
    latent_down,
    latent_up,
    output_weight,
    attn_gain,
    latent_gain,
    router_weight,
    shared_gate,
    shared_up,
    shared_down,
    moe_gain,
    expert_gate,
    expert_up,
    expert_down,
):
    groups = lax.axis_size(EXPERT)
    replicas = lax.axis_size(DP)
    place = lax.axis_index(EXPERT)
    seqs, span, width = inputs.shape
    own = seqs * span
    tokens = own * groups
    experts = groups
    capacity = (9 * span * TOP + 8 * experts - 1) // (8 * experts)
    scale = 1.0 / math.sqrt(HD + RD)
    rows = query_weight.shape[0]
    part = shared_down.shape[0]
    hidden_own = part * replicas
    QD = HD + RD

    def by_owner(value):
        return value.astype(bf16).reshape(groups, own, -1)

    def by_block(value):
        return value.reshape(seqs, groups, span, -1).transpose(1, 0, 2, 3).reshape(tokens, -1)

    x_low = inputs.reshape(own, width)
    cot_own = cotangent.reshape(own, width)

    order = priority[:, None, :] < priority[:, :, None]
    hit = jnp.sum(
        (expert_picks[..., None] == jnp.arange(experts, dtype=jnp.int32)).astype(f32), axis=2
    )
    ranks = einsum("stu,sue->ste", order.astype(bf16), hit.astype(bf16))
    codes = jnp.where((hit > 0) & (ranks < capacity), ranks, -1.0).astype(bf16)

    pad = rows - latent_gain.shape[0]
    small = jnp.concatenate(
        [
            latent_down,
            router_weight,
            attn_gain[:, None],
            moe_gain[:, None],
            jnp.pad(latent_gain, (0, pad))[:, None],
            jnp.zeros((rows, 45), bf16),
        ],
        axis=1,
    )
    small = dp_gather(small)
    query_parts = query_weight.reshape(rows, HEADS, QD).transpose(1, 0, 2)
    lup_rows = latent_up.shape[0]
    code_rows = -(lup_rows + 1) % 16 + 1
    code_part = jnp.pad(
        codes.reshape(own, 1, experts).T, ((0, 0), (0, code_rows - 1), (0, HD + VD - own))
    )
    lup_parts = jnp.concatenate(
        [latent_up.reshape(lup_rows, HEADS, HD + VD).transpose(1, 0, 2), code_part], axis=1
    )
    small_all, x_all, query_swap, lup_swap = ring_gather(
        [small, x_low], [query_parts, lup_parts], 1
    )
    small_all = (
        small_all.reshape(groups, replicas, rows, -1).transpose(1, 0, 2, 3).reshape(width, -1)
    )
    ldown_all = small_all[:, : RANK + RD]
    router_all = small_all[:, RANK + RD : RANK + RD + experts]
    gains = small_all[:, RANK + RD + experts :].astype(f32)
    gain_attn = gains[:, 0]
    gain_moe = gains[:, 1]
    gain_lat = gains[:, 2].reshape(-1, rows)[:, : latent_gain.shape[0]].reshape(-1)

    wq = dp_gather(query_swap.reshape(groups * rows, QD))
    lup = dp_gather(lup_swap[:, :lup_rows].reshape(groups * lup_rows, HD + VD))
    code = lup_swap[:, lup_rows, :own].astype(f32).reshape(tokens)

    def columns_of(weight):
        return (
            weight.reshape(rows, replicas, groups, part)
            .transpose(2, 0, 1, 3)
            .reshape(groups, rows, hidden_own)
        )

    gate_up_parts = jnp.concatenate([columns_of(shared_gate), columns_of(shared_up)], axis=2)
    gate_up_swap = expert_swap(gate_up_parts)
    gate_up = dp_gather(gate_up_swap.reshape(groups * rows, 2 * hidden_own))
    gate_up_router = jnp.concatenate([gate_up, router_all], axis=1)
    sdown = dp_gather(shared_down)
    gate_w = dp_gather(expert_gate[0])
    up_w = dp_gather(expert_up[0])
    down_w = dp_gather(expert_down[0])
    out_t = gather_rows(output_weight.T, BOTH)

    at_block = jnp.arange(groups, dtype=jnp.int32)[:, None, None] * span
    positions = jnp.broadcast_to(
        at_block + jnp.arange(span, dtype=jnp.int32), (groups, seqs, span)
    ).reshape(tokens)
    cosine, sine = angle_tables(positions, RD)
    cosine = jnp.concatenate([cosine] * 4, axis=1)
    sine = jnp.concatenate([-sine, sine] * 2, axis=1)
    joint_weight = jnp.concatenate([ldown_all, wq[:, HD:], wq[:, :HD]], axis=1)
    h_one, query, key, value, latent, normed_lat, factor_lat = project(
        x_all, joint_weight, lup, gain_attn, gain_lat, cosine, sine
    )
    probs_attn, heads_s = attend(query, key, value, segments, scale, groups, seqs, span)
    heads_own = heads_to_tokens(heads_s, span, 3).reshape(own, HEADS * VD)

    x_second = x_low.astype(f32) + right_product(heads_own, out_t)
    normed_two, factor_two = norm_parts(x_second)
    (h_two,) = ring_gather([(normed_two * gain_moe).astype(bf16)], [], 2)

    cot_all = gather_rows(cot_own, EXPERT)

    chunks = 4
    chunk = tokens // chunks
    blocks = chunk // span
    slots = blocks * capacity
    slot_at = jnp.arange(slots, dtype=jnp.int32)
    token_at = jnp.arange(chunk, dtype=jnp.int32)
    select = (
        (slot_at[:, None] // capacity == token_at[None, :] // span)[None]
        & (
            (slot_at % capacity).astype(f32)[None, :, None]
            == code.reshape(chunks, chunk)[:, None, :]
        )
    ).astype(bf16)
    select = lax.optimization_barrier(select)

    def to_slots(values):
        return einsum("cst,ctd->csd", select, values.reshape(chunks, chunk, -1)).astype(bf16).reshape(
            chunks * slots, -1
        )

    pre = product(h_two, gate_up_router)
    shared_a = pre[:, :hidden_own]
    shared_b = pre[:, hidden_own : 2 * hidden_own]
    gate_probs = jax.nn.softmax(pre[:, 2 * hidden_own :], axis=-1)
    shared_hidden = (jax.nn.silu(shared_a) * shared_b).astype(bf16)
    mine = (jnp.arange(experts, dtype=jnp.int32) == place).astype(f32)
    own_prob = jnp.sum(gate_probs * mine, axis=-1)
    slot_prob = jnp.sum(
        select.astype(f32) * own_prob.reshape(chunks, 1, chunk), axis=-1
    ).reshape(chunks * slots, 1)
    expert_in = to_slots(h_two)
    gate_pre = product(expert_in, gate_w)
    up_pre = product(expert_in, up_w)
    expert_hidden = (jax.nn.silu(gate_pre) * up_pre).astype(bf16)
    expert_out = product(expert_hidden, down_w).astype(bf16).astype(f32)
    partial = combine(
        select, (slot_prob * expert_out).astype(bf16), shared_hidden, sdown, COLS_ROWS
    )
    result = x_second + scatter_rows(partial, EXPERT).astype(f32)
    result = result.astype(bf16).reshape(seqs, span, width)

    grad_slots = to_slots(cot_all)
    hidden_grad = right_product(cot_all, sdown)
    sdown_grad = left_product(shared_hidden, cot_all)
    shared_a_grad = (hidden_grad * shared_b * silu_slope(shared_a)).astype(bf16)
    shared_b_grad = (hidden_grad * jax.nn.silu(shared_a)).astype(bf16)
    grad_wide = grad_slots.astype(f32)
    slot_grad = (slot_prob * grad_wide).astype(bf16)
    match = jnp.sum(grad_wide * expert_out, axis=-1).reshape(chunks, slots, 1)
    prob_grad = jnp.sum(select.astype(f32) * match, axis=1).reshape(tokens, 1)
    logit_grad = (gate_probs * prob_grad * (mine - own_prob[:, None])).astype(bf16)
    pre_grad = jnp.concatenate([shared_a_grad, shared_b_grad, logit_grad], axis=1)
    expert_hidden_grad = right_product(slot_grad, down_w)
    expert_a_grad = (expert_hidden_grad * up_pre * silu_slope(gate_pre)).astype(bf16)
    expert_b_grad = (expert_hidden_grad * jax.nn.silu(gate_pre)).astype(bf16)
    in_grad = right_product(expert_a_grad, gate_w) + right_product(expert_b_grad, up_w)
    in_grad = in_grad.astype(bf16)
    h_two_partial = combine(select, in_grad, pre_grad, gate_up_router, COLS_COLS)
    routed_down_grad = dp_scatter_product(expert_hidden, slot_grad)
    routed_gate_grad = dp_scatter_product(expert_in, expert_a_grad)
    routed_up_grad = dp_scatter_product(expert_in, expert_b_grad)
    (h_two_grad,) = ring_scatter([by_owner(h_two_partial)], 4)
    pre_weight_grad = left_product(h_two, pre_grad)
    sdown_owned = dp_scatter(sdown_grad)
    gate_up_owned = dp_scatter(pre_weight_grad[:, : 2 * hidden_own]).astype(bf16)
    router_grad = pre_weight_grad[:, 2 * hidden_own :]

    gmoe_grad = jnp.sum(h_two_grad * normed_two, axis=0)
    x_second_grad = cot_own.astype(f32) + norm_back(h_two_grad * gain_moe, normed_two, factor_two)
    attn_low = x_second_grad.astype(bf16)
    heads_grad = product(attn_low, out_t).astype(bf16)
    grad_s = tokens_to_heads(heads_grad.reshape(seqs, span, HEADS * VD), 5)
    low_all = gather_rows(attn_low, EXPERT)
    gate_up_owned = expert_swap(
        gate_up_owned.reshape(groups, rows, 2 * hidden_own)
    ).astype(f32)

    def owned_columns(value):
        return (
            value.reshape(groups, rows, replicas, part)
            .transpose(1, 2, 0, 3)
            .reshape(rows, replicas * groups * part)
        )

    sgate_owned = owned_columns(gate_up_owned[:, :, :hidden_own])
    sup_owned = owned_columns(gate_up_owned[:, :, hidden_own:])
    query_grad, pair_grad = attend_back(
        probs_attn, grad_s, heads_s, query, key, value, scale, groups, span
    )
    joint_grad, h_one_partial, lup_grad, glat_grad = project_back(
        query_grad, pair_grad, joint_weight, lup, gain_lat, cosine, sine,
        latent, normed_lat, factor_lat,
    )
    joint_weight_grad = left_product(h_one, joint_grad)
    gattn_grad = jnp.sum(joint_weight_grad * joint_weight.astype(f32), axis=1) / gain_attn
    out_grad = left_product(low_all, by_block(heads_s))
    down_at = RANK + RD
    back_grad = jnp.concatenate(
        [
            joint_weight_grad[:, down_at + RD :],
            out_grad,
            joint_weight_grad[:, down_at : down_at + RD],
            lup_grad.reshape(width, -1),
        ],
        axis=1,
    )
    back_grad = dp_scatter(back_grad).astype(bf16)
    back_owned = expert_swap(back_grad.reshape(groups, rows, -1)).astype(f32)
    q_owned = jnp.concatenate(
        [back_owned[:, :, :HD], back_owned[:, :, HD + VD : HD + VD + RD]], axis=2
    )
    q_owned = q_owned.transpose(1, 0, 2).reshape(rows, HEADS * QD)
    out_owned = back_owned[:, :, HD : HD + VD].transpose(0, 2, 1).reshape(HEADS * VD, rows)
    lup_owned = back_owned[:, :, HD + VD + RD :].reshape(groups, lup_rows, HD + VD)
    lup_owned = lup_owned.transpose(1, 0, 2).reshape(lup_rows, HEADS * (HD + VD))
    glat_column = jnp.pad(
        glat_grad.reshape(-1, latent_gain.shape[0]), ((0, 0), (0, pad))
    ).reshape(-1)
    lane = jnp.arange(128, dtype=jnp.int32)
    small_grad = jnp.pad(router_grad, ((0, 0), (0, 128 - experts)))
    for at_lane, column in enumerate((gattn_grad, gmoe_grad, glat_column)):
        small_grad = jnp.where(lane == experts + at_lane, column[:, None], small_grad)

    def by_row_owner(value):
        return value.astype(bf16).reshape(replicas, groups, rows, -1)

    ldown_owned, small_owned, h_one_grad = ring_scatter(
        [
            by_row_owner(joint_weight_grad[:, :down_at]),
            by_row_owner(small_grad),
            by_owner(h_one_partial),
        ],
        6,
    )
    normed_own, factor_own = norm_parts(x_low.astype(f32))
    input_grad = x_second_grad + norm_back(h_one_grad * gain_attn, normed_own, factor_own)
    input_grad = input_grad.astype(bf16).reshape(seqs, span, width)
    small_owned = dp_scatter(
        jnp.concatenate([ldown_owned, small_owned], axis=2).reshape(replicas * rows, -1)
    )
    ldown_owned = small_owned[:, :down_at]
    router_owned = small_owned[:, down_at : down_at + experts]
    gain_owned = small_owned[:, down_at + experts :]
    return (
        result,
        input_grad,
        q_owned,
        ldown_owned,
        lup_owned,
        out_owned,
        gain_owned[:, 0],
        gain_owned[: latent_gain.shape[0], 2],
        router_owned,
        sgate_owned,
        sup_owned,
        sdown_owned,
        gain_owned[:, 1],
        routed_gate_grad[None],
        routed_up_grad[None],
        routed_down_grad[None],
    )


def solution(mesh):
    return jax.shard_map(
        per_device,
        mesh=mesh,
        in_specs=(
            TOKENS, P(DP, None), TOKENS, P(DP, EXPERT), TOKENS,
            ROWS, ROWS, ROWS, P(None, BOTH), P(BOTH), P(BOTH),
            ROWS, ROWS, ROWS, ROWS, P(BOTH), ROUTED, ROUTED, ROUTED,
        ),
        out_specs=(
            TOKENS, TOKENS, ROWS, ROWS, ROWS, P(None, BOTH), P(BOTH), P(BOTH),
            ROWS, ROWS, ROWS, ROWS, P(BOTH), ROUTED, ROUTED, ROUTED,
        ),
        check_vma=False,
    )
```

```python
import functools
import math

import jax
import jax.numpy as jnp
from jax import lax
from jax.experimental import pallas as pl
from jax.experimental.pallas import tpu as pltpu
from jax.sharding import PartitionSpec as P

HEADS = 16
HD = 128
RD = 64
VD = 128
RANK = 512
TOP = 6

epsilon = 1e-06
masked_score = -1e30
DP = "dp"
EXPERT = "expert"
BOTH = (DP, EXPERT)
TOKENS = P(DP, EXPERT, None)
ROWS = P(BOTH, None)
ROUTED = P(EXPERT, DP, None)
f32 = jnp.float32
bf16 = jnp.bfloat16


def product(left, right):
    return jnp.dot(left, right, preferred_element_type=f32)


def left_product(left, right):
    return lax.dot_general(left, right, (((0,), (0,)), ((), ())), preferred_element_type=f32)


def right_product(left, right):
    return lax.dot_general(left, right, (((1,), (1,)), ((), ())), preferred_element_type=f32)


def einsum(spec, left, right):
    return jnp.einsum(spec, left, right, preferred_element_type=f32)


def norm_parts(values):
    factor = lax.rsqrt(jnp.mean(values * values, axis=-1, keepdims=True) + epsilon)
    return (values * factor, factor)


def norm_back(grad_normed, normed, factor):
    return factor * (grad_normed - normed * jnp.mean(grad_normed * normed, axis=-1, keepdims=True))


def angle_tables(positions, width):
    half = width // 2
    freqs = jnp.power(10000.0, -2.0 * jnp.arange(half, dtype=f32) / width)
    angles = positions.astype(f32)[:, None] * freqs[None, :]
    return (jnp.cos(angles), jnp.sin(angles))


def silu_slope(pre):
    sigma = jax.nn.sigmoid(pre)
    return sigma * (1.0 + pre * (1.0 - sigma))


def dp_swap(value):
    return lax.ppermute(value, DP, [(0, 1), (1, 0)])


def ordered(value, other):
    first = lax.axis_index(DP) == 0
    return jnp.concatenate(
        [jnp.where(first, value, other), jnp.where(first, other, value)], axis=0
    )


def dp_gather(value):
    if lax.axis_size(DP) == 2:
        return ordered(value, dp_swap(value))
    return lax.all_gather(value, DP, axis=0, tiled=True)


def dp_scatter_product(left, right):
    if lax.axis_size(DP) == 2:
        first = lax.axis_index(DP) == 0
        half = left.shape[1] // 2
        low, high = left[:, :half], left[:, half:]
        sent = left_product(jnp.where(first, high, low), right).astype(bf16)
        other = dp_swap(sent)
        return left_product(jnp.where(first, low, high), right) + other.astype(f32)
    return dp_scatter(left_product(left, right))


def dp_scatter(value):
    if lax.axis_size(DP) == 2:
        rows = value.shape[0] // 2
        at = lax.axis_index(DP)
        sent = lax.dynamic_slice_in_dim(value, (1 - at) * rows, rows, 0)
        kept = lax.dynamic_slice_in_dim(value, at * rows, rows, 0)
        return kept + dp_swap(sent.astype(bf16)).astype(f32)
    return lax.psum_scatter(
        value.astype(bf16), DP, scatter_dimension=0, tiled=True
    ).astype(f32)


def expert_swap(value):
    return lax.all_to_all(value, EXPERT, split_axis=0, concat_axis=0, tiled=True)


def gather_rows(value, axes):
    return lax.all_gather(value, axes, axis=0, tiled=True)


def scatter_rows(value, axes):
    return lax.psum_scatter(value, axes, scatter_dimension=0, tiled=True)


MESH = pl.DeviceIdType.MESH


def at_expert(index):
    return {EXPERT: index}


def grid_place():
    me = lax.axis_index(EXPERT)
    return me, me // 4, (me // 2) % 2, me % 2


def greet_neighbours(me, line, pair, core):
    partner = me + 1 - 2 * core
    mate = me + 2 - 4 * pair
    barrier = pltpu.get_barrier_semaphore()
    for other in (partner, mate):
        pl.semaphore_signal(barrier, inc=1, device_id=at_expert(other), device_id_type=MESH)

    @pl.when(line < 3)
    def _():
        pl.semaphore_signal(barrier, inc=1, device_id=at_expert(me + 4), device_id_type=MESH)

    @pl.when(line > 0)
    def _():
        pl.semaphore_signal(barrier, inc=1, device_id=at_expert(me - 4), device_id_type=MESH)

    pl.semaphore_wait(barrier, 3 + jnp.where((line > 0) & (line < 3), 1, 0))
    return partner, mate


def greet_all(me, mirrored=False):
    barrier = pltpu.get_barrier_semaphore()
    if mirrored:
        other = 1 - lax.axis_index(DP)
        pl.semaphore_signal(barrier, inc=1, device_id={DP: other}, device_id_type=MESH)
    for step in range(1, 16):
        pl.semaphore_signal(
            barrier, inc=1, device_id=at_expert((me + step) % 16), device_id_type=MESH
        )
    pl.semaphore_wait(barrier, 15 + mirrored)


def halves(rows):
    return (pl.ds(0, rows // 2), pl.ds(rows // 2, rows // 2)) if rows % 32 == 0 else (pl.ds(0, rows),)


def gather_kernel(k, m, mirrored, *refs):
    x_refs, swap_refs = refs[:k], refs[k : k + m]
    outs, swap_outs = refs[k + m : 2 * k + m], refs[2 * k + m : 2 * (k + m)]
    mirrors = refs[2 * (k + m) : 2 * (k + m) + m * mirrored]
    own_sem, send_sem, recv_sem, swap_send, swap_recv, mirror_sem = refs[
        2 * (k + m) + m * mirrored :
    ]
    pieces = [
        (a, at)
        for a in range(k)
        for at in (halves(x_refs[a].shape[0]) if len(x_refs[a].shape) == 2 else (None,))
    ]
    n = len(pieces)
    me, line, pair, core = grid_place()
    if m:
        greet_all(me, mirrored)
        partner, mate = me + 1 - 2 * core, me + 2 - 4 * pair
    else:
        partner, mate = greet_neighbours(me, line, pair, core)

    def held(i):
        a, at = pieces[i]
        return x_refs[a] if at is None else x_refs[a].at[at, :]

    def slot(i, origin):
        a, at = pieces[i]
        return outs[a].at[:, origin] if at is None else outs[a].at[origin, at, :]

    def own_copy(i):
        if i < n:
            return pltpu.make_async_copy(held(i), slot(i, me), own_sem.at[i])
        i -= n
        return pltpu.make_async_copy(
            swap_refs[i].at[me], swap_outs[i].at[me], own_sem.at[n + i]
        )

    def copy(i, source, origin, way, to):
        return pltpu.make_async_remote_copy(
            src_ref=source,
            dst_ref=slot(i, origin),
            send_sem=send_sem.at[i, origin, way],
            recv_sem=recv_sem.at[i, origin],
            device_id=at_expert(to),
            device_id_type=MESH,
        )

    def swap_copy(i, step):
        to = (me + step) % 16
        return pltpu.make_async_remote_copy(
            src_ref=swap_refs[i].at[to],
            dst_ref=swap_outs[i].at[me],
            send_sem=swap_send.at[i, step],
            recv_sem=swap_recv.at[i, step],
            device_id=at_expert(to),
            device_id_type=MESH,
        )

    def arrived(i, origin):
        copy(i, slot(i, origin), origin, 0, partner).wait_recv()

    def mirror_copy(i):
        return pltpu.make_async_remote_copy(
            src_ref=swap_outs[i],
            dst_ref=mirrors[i],
            send_sem=mirror_sem.at[i, 0],
            recv_sem=mirror_sem.at[i, 1],
            device_id={DP: 1 - lax.axis_index(DP)},
            device_id_type=MESH,
        )

    def swaps_done():
        for i in range(m):
            for step in range(1, 16):
                swap_copy(i, step).wait_recv()
            own_copy(n + i).wait()
            if mirrored:
                mirror_copy(i).start()

    def along(i, origin, source, upward, downward, act):
        if upward:

            @pl.when(line < 3)
            def _():
                act(copy(i, source, origin, 0, me + 4))

        if downward:

            @pl.when(line > 0)
            def _():
                act(copy(i, source, origin, 1, me - 4))

        act(copy(i, source, origin, 2, mate))
        act(copy(i, source, origin, 3, partner))

    def walk(act, wait, between):
        for far in range(1, 5):
            if far == 3:
                between()
            if far < 4:

                @pl.when(line >= far)
                def _():
                    origin = me - 4 * far
                    for i in range(n):
                        wait(i, origin)
                        along(i, origin, slot(i, origin), True, False, act)

                @pl.when(line + far <= 3)
                def _():
                    origin = me + 4 * far
                    for i in range(n):
                        wait(i, origin)
                        along(i, origin, slot(i, origin), False, True, act)

            for sign in (-1, 1) if far > 1 else (1,):
                step = sign * (far - 1)

                @pl.when((line + step >= 0) & (line + step <= 3))
                def _():
                    origin = mate + 4 * step
                    for i in range(n):
                        wait(i, origin)
                        act(copy(i, slot(i, origin), origin, 3, partner))

    def start(c):
        c.start()

    def sent(c):
        c.wait_send()

    for i in range(n):
        along(i, me, held(i), True, True, start)
    for i in range(m):
        for step in range(1, 16):
            swap_copy(i, step).start()
    for i in range(n + m):
        own_copy(i).start()
    walk(start, arrived, swaps_done)
    for i in range(n):
        for index in range(8):
            arrived(i, 2 * index + 1 - core)
    for i in range(n):
        along(i, me, held(i), True, True, sent)
    walk(sent, lambda i, origin: None, lambda: None)
    for i in range(m):
        for step in range(1, 16):
            swap_copy(i, step).wait_send()
        if mirrored:
            mirror_copy(i).wait()
    for i in range(n):
        own_copy(i).wait()


def ring_gather(values, swaps, collective, mirrored=False):
    k, m = len(values), len(swaps)
    n = sum(len(halves(v.shape[0])) if v.ndim == 2 else 1 for v in values)
    sent = 2 * (15 * sum(v.size for v in values) + sum(v.size for v in swaps))
    sems = pltpu.SemaphoreType.DMA
    anywhere = pl.BlockSpec(memory_space=pl.ANY)
    shapes = [(16,) + v.shape if v.ndim == 2 else v.shape[:1] + (16,) + v.shape[1:] for v in values]
    shapes += [v.shape for v in swaps] * (1 + mirrored)
    outs = pl.pallas_call(
        functools.partial(gather_kernel, k, m, mirrored),
        out_shape=[jax.ShapeDtypeStruct(shape, bf16) for shape in shapes],
        in_specs=[pl.BlockSpec(memory_space=pltpu.VMEM)] * (k + m),
        out_specs=[anywhere] * len(shapes),
        scratch_shapes=[
            sems((n + m,)),
            sems((n, 16, 4)),
            sems((n, 16)),
            sems((max(m, 1), 16)),
            sems((max(m, 1), 16)),
            sems((max(m, 1), 2)),
        ],
        compiler_params=pltpu.CompilerParams(collective_id=collective, has_side_effects=True),
        cost_estimate=pl.CostEstimate(flops=0, bytes_accessed=16 * sent, transcendentals=0),
    )(*values, *swaps)
    return [o.reshape(-1, o.shape[-1]) for o in outs[:k]] + list(outs[k:])


def scatter_pieces(shapes):
    return [
        (a, at)
        for a, shape in enumerate(shapes)
        for at in (halves(shape[0]) if len(shape) == 2 else (None,))
    ]


def scatter_kernel(k, *refs):
    pieces = scatter_pieces([ref.shape for ref in refs[k : 2 * k]])
    n = len(pieces)
    parts = [
        (refs[a], refs[k + a] if at is None else refs[k + a].at[at, :])
        + refs[2 * k + 5 * i : 2 * k + 5 * i + 5]
        for i, (a, at) in enumerate(pieces)
    ]
    (
        core_send, core_recv, mate_send, mate_recv, up_send, up_recv, down_send, down_recv,
    ) = refs[2 * k + 5 * n :]
    me, line, pair, core = grid_place()
    partner, mate = greet_neighbours(me, line, pair, core)

    def block(i, dest):
        ref, at = parts[i][0], pieces[i][1]
        return ref.at[:, dest] if at is None else ref.at[dest, at, :]

    def remote(source, target, send, recv, to):
        return pltpu.make_async_remote_copy(
            src_ref=source, dst_ref=target, send_sem=send, recv_sem=recv,
            device_id=at_expert(to), device_id_type=MESH,
        )

    def core_copy(i, index):
        return remote(
            block(i, 2 * index + 1 - core), parts[i][2].at[index],
            core_send.at[i, index], core_recv.at[i, index], partner,
        )

    def mate_copy(i, dest):
        return remote(
            parts[i][6].at[2 * dest + 1 - pair], parts[i][3].at[dest],
            mate_send.at[i, dest], mate_recv.at[i, dest], mate,
        )

    def up_copy(i, dest):
        return remote(
            parts[i][6].at[2 * dest + pair], parts[i][4].at[dest],
            up_send.at[i, dest], up_recv.at[i, dest], me + 4,
        )

    def down_copy(i, dest):
        return remote(
            parts[i][6].at[2 * dest + pair], parts[i][5].at[dest],
            down_send.at[i, dest], down_recv.at[i, dest], me - 4,
        )

    def add(target, left, right):
        if len(left.shape) == 3:
            for i in range(left.shape[0]):
                add(target.at[i], left.at[i], right.at[i])
            return
        tile = min(16, left.shape[0])

        @pl.loop(0, left.shape[0] // tile)
        def _(i):
            at = pl.ds(pl.multiple_of(i * tile, tile), tile)
            target[at, :] = (left[at, :].astype(f32) + right[at, :].astype(f32)).astype(
                target.dtype
            )

    def farthest(act):
        for far in (3, 2, 1, 0):
            for step in (-far, far) if far else (0,):

                @pl.when((line + step >= 0) & (line + step <= 3))
                def _():
                    for i in range(n):
                        act(i, line + step, step)

    def send_core(i, dest, step):
        core_copy(i, 2 * dest + 1 - pair).start()

    def send_core_own(i, dest, step):
        core_copy(i, 2 * dest + pair).start()

    def chip_sum(i, index):
        core_copy(i, index).wait_recv()
        add(parts[i][6].at[index], block(i, 2 * index + core), parts[i][2].at[index])

    def to_mate(i, dest, step):
        chip_sum(i, 2 * dest + 1 - pair)
        mate_copy(i, dest).start()

    def keep(i, dest, step):
        chip_sum(i, 2 * dest + pair)

    def along(i, dest, step):
        out, up_in, down_in, total = parts[i][1], parts[i][4], parts[i][5], parts[i][6]
        mine = total.at[2 * dest + pair]
        mate_copy(i, dest).wait_recv()
        if step == 0:
            add(out, mine, parts[i][3].at[dest])
            mine = out
        else:
            add(mine, mine, parts[i][3].at[dest])
        if step >= 0:

            @pl.when(line > 0)
            def _():
                up_copy(i, dest).wait_recv()
                add(mine, mine, up_in.at[dest])

        if step <= 0:

            @pl.when(line < 3)
            def _():
                down_copy(i, dest).wait_recv()
                add(mine, mine, down_in.at[dest])

        if step > 0:
            up_copy(i, dest).start()
        elif step < 0:
            down_copy(i, dest).start()

    def finish(i, dest, step):
        mate_copy(i, dest).wait_send()
        core_copy(i, 2 * dest + 1 - pair).wait_send()
        core_copy(i, 2 * dest + pair).wait_send()
        if step > 0:
            up_copy(i, dest).wait_send()
        elif step < 0:
            down_copy(i, dest).wait_send()

    for act in (send_core, send_core_own, to_mate, keep, along, finish):
        farthest(act)


def ring_scatter(values, collective):
    count = len(values)
    shapes = [v.shape[1:] if len(v.shape) == 3 else v.shape[:1] + v.shape[2:] for v in values]
    pieces = scatter_pieces(shapes)
    n = len(pieces)
    parts = [
        shapes[a] if at is None else (at.size,) + shapes[a][1:] for a, at in pieces
    ]
    buffers = [pltpu.VMEM((k,) + s, bf16) for s in parts for k in (8, 4, 4, 4, 8)]
    sent = 30 * sum(math.prod(s) for s in shapes)
    vmem = pl.BlockSpec(memory_space=pltpu.VMEM)
    return pl.pallas_call(
        functools.partial(scatter_kernel, count),
        out_shape=[jax.ShapeDtypeStruct(s, f32) for s in shapes],
        in_specs=[vmem] * count,
        out_specs=[vmem] * count,
        scratch_shapes=buffers
        + [pltpu.SemaphoreType.DMA((n, k)) for k in (8, 8, 4, 4, 4, 4, 4, 4)],
        compiler_params=pltpu.CompilerParams(collective_id=collective, has_side_effects=True),
        cost_estimate=pl.CostEstimate(flops=0, bytes_accessed=16 * sent, transcendentals=0),
    )(*values)


def swap_kernel(source, target, x_ref, out_ref, own_sem, send_sem, recv_sem):
    me = lax.axis_index(EXPERT)
    greet_all(me)

    def copy(step):
        to = (me + step) % 16
        return pltpu.make_async_remote_copy(
            src_ref=source(x_ref, to),
            dst_ref=target(out_ref, me),
            send_sem=send_sem.at[step],
            recv_sem=recv_sem.at[step],
            device_id=at_expert(to),
            device_id_type=MESH,
        )

    for step in range(1, 16):
        copy(step).start()
    own = pltpu.make_async_copy(source(x_ref, me), target(out_ref, me), own_sem)
    own.start()
    for step in range(1, 16):
        copy(step).wait()
    own.wait()


def swap_call(source, target, value, shape, collective):
    sent = value.size * 2
    return pl.pallas_call(
        functools.partial(swap_kernel, source, target),
        out_shape=jax.ShapeDtypeStruct(shape, value.dtype),
        in_specs=[pl.BlockSpec(memory_space=pltpu.VMEM)],
        out_specs=pl.BlockSpec(memory_space=pltpu.VMEM),
        scratch_shapes=[
            pltpu.SemaphoreType.DMA,
            pltpu.SemaphoreType.DMA((16,)),
            pltpu.SemaphoreType.DMA((16,)),
        ],
        compiler_params=pltpu.CompilerParams(collective_id=collective, has_side_effects=True),
        cost_estimate=pl.CostEstimate(flops=0, bytes_accessed=64 * sent, transcendentals=0),
    )(value)


def block_rows(span):
    return lambda ref, at: ref.at[:, pl.ds(pl.multiple_of(at * span, span), span), :]


def head_columns(columns):
    return lambda ref, at: ref.at[:, :, pl.ds(pl.multiple_of(at * columns, columns), columns)]


def heads_to_tokens(value, span, collective):
    seqs = value.shape[0]
    return swap_call(
        block_rows(span), head_columns(VD), value, (seqs, span, HEADS * VD), collective
    )


def tokens_to_heads(value, collective):
    seqs, span, _ = value.shape
    return swap_call(
        head_columns(VD), block_rows(span), value, (seqs, span * HEADS, VD), collective
    )


def matmul(left, right, dims):
    return lax.dot_general(left, right, (dims, ((), ())), preferred_element_type=f32)


ROWS_ROWS = ((0,), (0,))
COLS_COLS = ((1,), (1,))
COLS_ROWS = ((1,), (0,))


def full(shape):
    return pl.BlockSpec(shape, lambda *_: (0,) * len(shape), pipeline_mode=pl.Buffered(1))


def tiled(rows, columns):
    return pl.BlockSpec((rows, columns), lambda i: (i, 0))


def estimate(flops, nbytes):
    return pl.CostEstimate(
        flops=int(flops), bytes_accessed=int(nbytes), transcendentals=0
    )


def combine_kernel(dims, select_ref, slot_ref, left_ref, right_ref, out_ref):
    routed = matmul(select_ref[0], slot_ref[0], ROWS_ROWS)
    out_ref[...] = (routed + matmul(left_ref[...], right_ref[...], dims)).astype(bf16)


def combine(select, slot_rows, left, right, dims):
    chunks, slots, chunk = select.shape
    width = slot_rows.shape[-1]
    tile = 256
    per = chunk // tile
    inner = left.shape[1]
    return pl.pallas_call(
        functools.partial(combine_kernel, dims),
        grid=(chunks, per),
        in_specs=[
            pl.BlockSpec((1, slots, tile), lambda c, t: (c, 0, t)),
            pl.BlockSpec((1, slots, width), lambda c, t: (c, 0, 0)),
            pl.BlockSpec((tile, inner), lambda c, t: (c * per + t, 0)),
            full(right.shape),
        ],
        out_specs=pl.BlockSpec((tile, width), lambda c, t: (c * per + t, 0)),
        out_shape=jax.ShapeDtypeStruct((chunks * chunk, width), bf16),
        cost_estimate=estimate(
            2 * chunks * chunk * width * (slots + inner), 4 * chunks * chunk * width
        ),
    )(select, slot_rows.reshape(chunks, slots, width), left, right)


def turn(values, cosine, sine):
    lane = lax.broadcasted_iota(jnp.int32, values.shape, 1)
    other = jnp.where(lane % 64 < 32, pltpu.roll(values, 96, 1), pltpu.roll(values, 32, 1))
    return values * cosine + other * sine


def project_kernel(
    x_ref, weight_ref, lup_ref, gain_ref, gain_lat_ref, cos_ref, sin_ref,
    h_ref, query_ref, key_ref, value_ref, latent_ref, normed_ref, factor_ref,
):
    x = x_ref[...].astype(f32)
    factor = lax.rsqrt(jnp.mean(x * x, axis=-1, keepdims=True) + epsilon)
    h = (x * factor * gain_ref[...]).astype(bf16)
    h_ref[...] = h
    raw = matmul(h, weight_ref[...], COLS_ROWS)
    low = raw[:, :RANK]
    factor = lax.rsqrt(jnp.mean(low * low, axis=-1, keepdims=True) + epsilon)
    normed = low * factor
    normed_ref[...] = normed
    factor_ref[...] = factor
    latent = (normed * gain_lat_ref[...]).astype(bf16)
    latent_ref[...] = latent
    expanded = matmul(latent, lup_ref[...], COLS_ROWS)
    rope = turn(raw[:, RANK : RANK + 128], cos_ref[...], sin_ref[...])
    lane = lax.broadcasted_iota(jnp.int32, rope.shape, 1)
    query_ref[:, :HD] = raw[:, RANK + 128 :].astype(bf16)
    query_ref[:, HD:] = jnp.where(lane < RD, pltpu.roll(rope, 64, 1), 0.0).astype(bf16)
    key_ref[:, :HD] = expanded[:, :HD].astype(bf16)
    key_ref[:, HD:] = jnp.where(lane < RD, rope, 0.0).astype(bf16)
    value_ref[...] = expanded[:, HD:].astype(bf16)


def project(x_all, weight, lup, gain, gain_lat, cosine, sine):
    tokens, width = x_all.shape
    tile = 256
    outs = [
        ((tokens, width), bf16),
        ((tokens, HD + 128), bf16),
        ((tokens, HD + 128), bf16),
        ((tokens, VD), bf16),
        ((tokens, RANK), bf16),
        ((tokens, RANK), f32),
        ((tokens, 1), f32),
    ]
    return pl.pallas_call(
        project_kernel,
        name="project",
        grid=(tokens // tile,),
        in_specs=[
            tiled(tile, width),
            full(weight.shape),
            full(lup.shape),
            full((1, width)),
            full((1, RANK)),
            tiled(tile, 128),
            tiled(tile, 128),
        ],
        out_specs=[tiled(tile, s[1]) for s, _ in outs],
        out_shape=[jax.ShapeDtypeStruct(s, d) for s, d in outs],
        cost_estimate=estimate(2 * tokens * width * (weight.shape[1] + 64), 5 * tokens * width),
    )(x_all, weight, lup, gain[None], gain_lat[None], cosine, sine)


def attend_kernel(scale, query_ref, key_ref, value_ref, row_ref, col_ref, probs_ref, out_ref):
    length = probs_ref.shape[1]
    tile = 256
    query = query_ref[...].reshape(length, -1)
    key = key_ref[...].reshape(length, -1)
    value = value_ref[...].reshape(length, -1)
    for at in range(0, length, tile):
        seen = at + tile
        scores = matmul(query[at:seen], key[:seen], COLS_COLS) * scale
        row = at + lax.broadcasted_iota(jnp.int32, scores.shape, 0)
        col = lax.broadcasted_iota(jnp.int32, scores.shape, 1)
        keep = (col <= row) & (row_ref[0, :, :seen] == col_ref[0, at:seen, :])
        scores = jnp.where(keep, scores, masked_score)
        weights = jnp.exp(scores - jnp.max(scores, axis=-1, keepdims=True))
        probs = (weights / jnp.sum(weights, axis=-1, keepdims=True)).astype(bf16)
        probs_ref[0, at:seen, :seen] = probs
        if seen < length:
            probs_ref[0, at:seen, seen:] = jnp.zeros((tile, length - seen), bf16)
        out_ref[0, at:seen, :] = matmul(probs, value[:seen], COLS_ROWS).astype(bf16)


def of_sequence(groups, span, columns):
    return pl.BlockSpec((groups, 1, span, columns), lambda s: (0, s, 0, 0))


def attend(query, key, value, segments, scale, groups, seqs, span):
    length = groups * span
    view = lambda v: v.reshape(groups, seqs, span, -1)
    return pl.pallas_call(
        functools.partial(attend_kernel, scale),
        name="attend",
        grid=(seqs,),
        in_specs=[
            of_sequence(groups, span, HD + 128),
            of_sequence(groups, span, HD + 128),
            of_sequence(groups, span, VD),
            pl.BlockSpec((1, 1, length), lambda s: (s, 0, 0)),
            pl.BlockSpec((1, length, 1), lambda s: (s, 0, 0)),
        ],
        out_specs=[
            pl.BlockSpec((1, length, length), lambda s: (s, 0, 0)),
            pl.BlockSpec((1, length, VD), lambda s: (s, 0, 0)),
        ],
        out_shape=[
            jax.ShapeDtypeStruct((seqs, length, length), bf16),
            jax.ShapeDtypeStruct((seqs, length, VD), bf16),
        ],
        cost_estimate=estimate(seqs * length * length * 500, seqs * length * length * 4),
    )(view(query), view(key), view(value), segments[:, None, :], segments[:, :, None])


def attend_back_kernel(
    scale, probs_ref, grad_ref, out_ref, query_ref, key_ref, value_ref, dq_ref, dkv_ref, acc_ref
):
    length = probs_ref.shape[1]
    tile = 256
    _, _, span, _ = query_ref.shape
    per = tile // span
    query = query_ref[...].reshape(length, -1)
    key = key_ref[...].reshape(length, -1)
    value = value_ref[...].reshape(length, -1)
    wide = query.shape[1]
    for at in reversed(range(0, length, tile)):
        seen = at + tile
        grad = grad_ref[0, at:seen, :]
        spread = jnp.sum(
            grad.astype(f32) * out_ref[0, at:seen, :].astype(f32), axis=-1, keepdims=True
        )
        probs = probs_ref[0, at:seen, :seen]
        back = matmul(grad, value[:seen], COLS_COLS) - spread
        score_grad = (probs.astype(f32) * back * scale).astype(bf16)
        dq = matmul(score_grad, key[:seen], COLS_ROWS)
        dq_ref[at // span : seen // span, 0] = dq.reshape(per, span, wide)
        dk = matmul(score_grad, query[at:seen], ROWS_ROWS)
        dv = matmul(probs, grad, ROWS_ROWS)
        if seen == length:
            acc_ref[:, :wide] = dk
            acc_ref[:, wide:] = dv
        else:
            acc_ref[:seen, :wide] += dk
            acc_ref[:seen, wide:] += dv
    dkv_ref[...] = acc_ref[...].reshape(dkv_ref.shape)


def attend_back(probs, grad, out, query, key, value, scale, groups, span):
    seqs, length, _ = probs.shape
    wide = HD + 128
    view = lambda v: v.reshape(groups, seqs, span, -1)
    by_seq = lambda n: pl.BlockSpec((1, length, n), lambda s: (s, 0, 0))
    dq, dkv = pl.pallas_call(
        functools.partial(attend_back_kernel, scale),
        name="attend_back",
        grid=(seqs,),
        in_specs=[
            by_seq(length),
            by_seq(VD),
            by_seq(VD),
            of_sequence(groups, span, wide),
            of_sequence(groups, span, wide),
            of_sequence(groups, span, VD),
        ],
        out_specs=[of_sequence(groups, span, wide), of_sequence(groups, span, wide + VD)],
        out_shape=[
            jax.ShapeDtypeStruct((groups, seqs, span, wide), f32),
            jax.ShapeDtypeStruct((groups, seqs, span, wide + VD), f32),
        ],
        scratch_shapes=[pltpu.VMEM((length, wide + VD), f32)],
        cost_estimate=estimate(seqs * length * length * 1000, seqs * length * length * 4),
    )(probs, grad, out, view(query), view(key), view(value))
    return dq.reshape(-1, wide), dkv.reshape(-1, wide + VD)


def project_back_kernel(
    dq_ref, dkv_ref, weight_ref, lup_ref, gain_lat_ref, cos_ref, sin_ref,
    latent_ref, normed_ref, factor_ref, joint_ref, h_ref, lup_grad_ref, gain_grad_ref,
):
    dq = dq_ref[...]
    dkv = dkv_ref[...]
    lane = lax.broadcasted_iota(jnp.int32, (dq.shape[0], 128), 1)
    rope = jnp.where(lane < RD, dkv[:, HD : HD + 128], pltpu.roll(dq[:, HD:], 64, 1))
    rope = turn(rope, cos_ref[...], -sin_ref[...])
    expanded = jnp.concatenate([dkv[:, :HD], dkv[:, HD + 128 :]], axis=1).astype(bf16)
    latent_grad = matmul(expanded, lup_ref[...], COLS_COLS)
    normed = normed_ref[...]

    @pl.when(pl.program_id(0) == 0)
    def _():
        lup_grad_ref[...] = jnp.zeros_like(lup_grad_ref)
        gain_grad_ref[...] = jnp.zeros_like(gain_grad_ref)

    lup_grad_ref[...] += matmul(latent_ref[...], expanded, ROWS_ROWS)
    gain_grad_ref[...] += jnp.sum(latent_grad * normed, axis=0, keepdims=True)
    scaled = latent_grad * gain_lat_ref[...]
    down = factor_ref[...] * (
        scaled - normed * jnp.mean(scaled * normed, axis=-1, keepdims=True)
    )
    joint = jnp.concatenate([down, rope, dq[:, :HD]], axis=1).astype(bf16)
    joint_ref[...] = joint
    h_ref[...] = matmul(joint, weight_ref[...], COLS_COLS).astype(bf16)


def project_back(dq, dkv, weight, lup, gain_lat, cosine, sine, latent, normed, factor):
    tokens = dq.shape[0]
    width, joint = weight.shape
    tile = 256
    return pl.pallas_call(
        project_back_kernel,
        name="project_back",
        grid=(tokens // tile,),
        in_specs=[
            tiled(tile, dq.shape[1]),
            tiled(tile, dkv.shape[1]),
            full(weight.shape),
            full(lup.shape),
            full((1, RANK)),
            tiled(tile, 128),
            tiled(tile, 128),
            tiled(tile, RANK),
            tiled(tile, RANK),
            tiled(tile, 1),
        ],
        out_specs=[
            tiled(tile, joint),
            tiled(tile, width),
            pl.BlockSpec(lup.shape, lambda i: (0, 0)),
            pl.BlockSpec((1, RANK), lambda i: (0, 0)),
        ],
        out_shape=[
            jax.ShapeDtypeStruct((tokens, joint), bf16),
            jax.ShapeDtypeStruct((tokens, width), bf16),
            jax.ShapeDtypeStruct(lup.shape, f32),
            jax.ShapeDtypeStruct((1, RANK), f32),
        ],
        cost_estimate=estimate(2 * tokens * width * joint * 1.2, 6 * tokens * width),
    )(dq, dkv, weight, lup, gain_lat[None], cosine, sine, latent, normed, factor)


def per_device(
    inputs,
    segments,
    expert_picks,
    priority,
    cotangent,
    query_weight,
    latent_down,
    latent_up,
    output_weight,
    attn_gain,
    latent_gain,
    router_weight,
    shared_gate,
    shared_up,
    shared_down,
    moe_gain,
    expert_gate,
    expert_up,
    expert_down,
):
    groups = lax.axis_size(EXPERT)
    replicas = lax.axis_size(DP)
    place = lax.axis_index(EXPERT)
    seqs, span, width = inputs.shape
    own = seqs * span
    tokens = own * groups
    experts = groups
    capacity = (9 * span * TOP + 8 * experts - 1) // (8 * experts)
    scale = 1.0 / math.sqrt(HD + RD)
    rows = query_weight.shape[0]
    part = shared_down.shape[0]
    hidden_own = part * replicas
    QD = HD + RD

    def by_owner(value):
        return value.astype(bf16).reshape(groups, own, -1)

    def by_block(value):
        return value.reshape(seqs, groups, span, -1).transpose(1, 0, 2, 3).reshape(tokens, -1)

    x_low = inputs.reshape(own, width)
    cot_own = cotangent.reshape(own, width)

    order = priority[:, None, :] < priority[:, :, None]
    hit = jnp.sum(
        (expert_picks[..., None] == jnp.arange(experts, dtype=jnp.int32)).astype(f32), axis=2
    )
    ranks = einsum("stu,sue->ste", order.astype(bf16), hit.astype(bf16))
    codes = jnp.where((hit > 0) & (ranks < capacity), ranks, -1.0).astype(bf16)

    pad = rows - latent_gain.shape[0]
    small = jnp.concatenate(
        [
            latent_down,
            router_weight,
            attn_gain[:, None],
            moe_gain[:, None],
            jnp.pad(latent_gain, (0, pad))[:, None],
            jnp.zeros((rows, 45), bf16),
        ],
        axis=1,
    )
    small = dp_gather(small).reshape(replicas, rows, -1)
    query_parts = query_weight.reshape(rows, HEADS, QD).transpose(1, 0, 2)
    lup_rows = latent_up.shape[0]
    code_rows = -(lup_rows + 1) % 16 + 1
    code_part = jnp.pad(
        codes.reshape(own, 1, experts).T, ((0, 0), (0, code_rows - 1), (0, HD + VD - own))
    )
    lup_parts = jnp.concatenate(
        [latent_up.reshape(lup_rows, HEADS, HD + VD).transpose(1, 0, 2), code_part], axis=1
    )
    small_all, x_all, *swapped = ring_gather(
        [small, x_low], [query_parts, lup_parts], 1, replicas == 2
    )
    ldown_all = small_all[:, : RANK + RD]
    router_all = small_all[:, RANK + RD : RANK + RD + experts]
    gains = small_all[:, RANK + RD + experts :].astype(f32)
    gain_attn = gains[:, 0]
    gain_moe = gains[:, 1]
    gain_lat = gains[:, 2].reshape(-1, rows)[:, : latent_gain.shape[0]].reshape(-1)

    def all_rows(at, cut):
        value = swapped[at][:, :cut].reshape(groups * cut, -1)
        if replicas != 2:
            return dp_gather(value)
        return ordered(value, swapped[at + 2][:, :cut].reshape(groups * cut, -1))

    wq = all_rows(0, rows)
    lup = all_rows(1, lup_rows)
    code = swapped[1][:, lup_rows, :own].astype(f32).reshape(tokens)

    def columns_of(weight):
        return (
            weight.reshape(rows, replicas, groups, part)
            .transpose(2, 0, 1, 3)
            .reshape(groups, rows, hidden_own)
        )

    gate_up_parts = jnp.concatenate([columns_of(shared_gate), columns_of(shared_up)], axis=2)
    gate_up_swap = expert_swap(gate_up_parts)
    gate_up = dp_gather(gate_up_swap.reshape(groups * rows, 2 * hidden_own))
    gate_up_router = jnp.concatenate([gate_up, router_all], axis=1)
    sdown = dp_gather(shared_down)
    gate_w = dp_gather(expert_gate[0])
    up_w = dp_gather(expert_up[0])
    down_w = dp_gather(expert_down[0])
    out_t = gather_rows(output_weight.T, BOTH)

    at_block = jnp.arange(groups, dtype=jnp.int32)[:, None, None] * span
    positions = jnp.broadcast_to(
        at_block + jnp.arange(span, dtype=jnp.int32), (groups, seqs, span)
    ).reshape(tokens)
    cosine, sine = angle_tables(positions, RD)
    cosine = jnp.concatenate([cosine] * 4, axis=1)
    sine = jnp.concatenate([-sine, sine] * 2, axis=1)
    joint_weight = jnp.concatenate([ldown_all, wq[:, HD:], wq[:, :HD]], axis=1)
    h_one, query, key, value, latent, normed_lat, factor_lat = project(
        x_all, joint_weight, lup, gain_attn, gain_lat, cosine, sine
    )
    probs_attn, heads_s = attend(query, key, value, segments, scale, groups, seqs, span)
    heads_own = heads_to_tokens(heads_s, span, 3).reshape(own, HEADS * VD)

    x_second = x_low.astype(f32) + right_product(heads_own, out_t)
    normed_two, factor_two = norm_parts(x_second)
    (h_two,) = ring_gather([(normed_two * gain_moe).astype(bf16)], [], 2)

    cot_all = gather_rows(cot_own, EXPERT)

    chunks = 4
    chunk = tokens // chunks
    blocks = chunk // span
    slots = blocks * capacity
    slot_at = jnp.arange(slots, dtype=jnp.int32)
    token_at = jnp.arange(chunk, dtype=jnp.int32)
    select = (
        (slot_at[:, None] // capacity == token_at[None, :] // span)[None]
        & (
            (slot_at % capacity).astype(f32)[None, :, None]
            == code.reshape(chunks, chunk)[:, None, :]
        )
    ).astype(bf16)
    select = lax.optimization_barrier(select)

    def to_slots(values):
        return einsum("cst,ctd->csd", select, values.reshape(chunks, chunk, -1)).astype(bf16).reshape(
            chunks * slots, -1
        )

    pre = product(h_two, gate_up_router)
    shared_a = pre[:, :hidden_own]
    shared_b = pre[:, hidden_own : 2 * hidden_own]
    gate_probs = jax.nn.softmax(pre[:, 2 * hidden_own :], axis=-1)
    shared_hidden = (jax.nn.silu(shared_a) * shared_b).astype(bf16)
    mine = (jnp.arange(experts, dtype=jnp.int32) == place).astype(f32)
    own_prob = jnp.sum(gate_probs * mine, axis=-1)
    slot_prob = jnp.sum(
        select.astype(f32) * own_prob.reshape(chunks, 1, chunk), axis=-1
    ).reshape(chunks * slots, 1)
    expert_in = to_slots(h_two)
    gate_pre = product(expert_in, gate_w)
    up_pre = product(expert_in, up_w)
    expert_hidden = (jax.nn.silu(gate_pre) * up_pre).astype(bf16)
    expert_out = product(expert_hidden, down_w).astype(bf16).astype(f32)
    partial = combine(
        select, (slot_prob * expert_out).astype(bf16), shared_hidden, sdown, COLS_ROWS
    )
    result = x_second + scatter_rows(partial, EXPERT).astype(f32)
    result = result.astype(bf16).reshape(seqs, span, width)

    grad_slots = to_slots(cot_all)
    hidden_grad = right_product(cot_all, sdown)
    sdown_grad = left_product(shared_hidden, cot_all)
    shared_a_grad = (hidden_grad * shared_b * silu_slope(shared_a)).astype(bf16)
    shared_b_grad = (hidden_grad * jax.nn.silu(shared_a)).astype(bf16)
    grad_wide = grad_slots.astype(f32)
    slot_grad = (slot_prob * grad_wide).astype(bf16)
    match = jnp.sum(grad_wide * expert_out, axis=-1).reshape(chunks, slots, 1)
    prob_grad = jnp.sum(select.astype(f32) * match, axis=1).reshape(tokens, 1)
    logit_grad = (gate_probs * prob_grad * (mine - own_prob[:, None])).astype(bf16)
    pre_grad = jnp.concatenate([shared_a_grad, shared_b_grad, logit_grad], axis=1)
    expert_hidden_grad = right_product(slot_grad, down_w)
    expert_a_grad = (expert_hidden_grad * up_pre * silu_slope(gate_pre)).astype(bf16)
    expert_b_grad = (expert_hidden_grad * jax.nn.silu(gate_pre)).astype(bf16)
    in_grad = right_product(expert_a_grad, gate_w) + right_product(expert_b_grad, up_w)
    in_grad = in_grad.astype(bf16)
    h_two_partial = combine(select, in_grad, pre_grad, gate_up_router, COLS_COLS)
    routed_down_grad = dp_scatter_product(expert_hidden, slot_grad)
    routed_gate_grad = dp_scatter_product(expert_in, expert_a_grad)
    routed_up_grad = dp_scatter_product(expert_in, expert_b_grad)
    (h_two_grad,) = ring_scatter([by_owner(h_two_partial)], 4)
    pre_weight_grad = left_product(h_two, pre_grad)
    sdown_owned = dp_scatter(sdown_grad)
    gate_up_owned = dp_scatter(pre_weight_grad[:, : 2 * hidden_own]).astype(bf16)
    router_grad = pre_weight_grad[:, 2 * hidden_own :]

    gmoe_grad = jnp.sum(h_two_grad * normed_two, axis=0)
    x_second_grad = cot_own.astype(f32) + norm_back(h_two_grad * gain_moe, normed_two, factor_two)
    attn_low = x_second_grad.astype(bf16)
    heads_grad = product(attn_low, out_t).astype(bf16)
    grad_s = tokens_to_heads(heads_grad.reshape(seqs, span, HEADS * VD), 5)
    low_all = gather_rows(attn_low, EXPERT)
    gate_up_owned = expert_swap(
        gate_up_owned.reshape(groups, rows, 2 * hidden_own)
    )

    def owned_columns(value):
        return (
            value.reshape(groups, rows, replicas, part)
            .transpose(1, 2, 0, 3)
            .reshape(rows, replicas * groups * part)
        )

    sgate_owned = owned_columns(gate_up_owned[:, :, :hidden_own]).astype(f32)
    sup_owned = owned_columns(gate_up_owned[:, :, hidden_own:]).astype(f32)
    query_grad, pair_grad = attend_back(
        probs_attn, grad_s, heads_s, query, key, value, scale, groups, span
    )
    joint_grad, h_one_partial, lup_grad, glat_grad = project_back(
        query_grad, pair_grad, joint_weight, lup, gain_lat, cosine, sine,
        latent, normed_lat, factor_lat,
    )
    joint_weight_grad = left_product(h_one, joint_grad)
    gattn_grad = jnp.sum(joint_weight_grad * joint_weight.astype(f32), axis=1) / gain_attn
    out_grad = left_product(low_all, by_block(heads_s))
    down_at = RANK + RD
    back_grad = jnp.concatenate(
        [
            joint_weight_grad[:, down_at + RD :],
            out_grad,
            joint_weight_grad[:, down_at : down_at + RD],
            lup_grad.reshape(width, -1),
        ],
        axis=1,
    )
    back_grad = dp_scatter(back_grad).astype(bf16)
    back_owned = expert_swap(back_grad.reshape(groups, rows, -1)).astype(f32)
    q_owned = jnp.concatenate(
        [back_owned[:, :, :HD], back_owned[:, :, HD + VD : HD + VD + RD]], axis=2
    )
    q_owned = q_owned.transpose(1, 0, 2).reshape(rows, HEADS * QD)
    out_owned = back_owned[:, :, HD : HD + VD].transpose(0, 2, 1).reshape(HEADS * VD, rows)
    lup_owned = back_owned[:, :, HD + VD + RD :].reshape(groups, lup_rows, HD + VD)
    lup_owned = lup_owned.transpose(1, 0, 2).reshape(lup_rows, HEADS * (HD + VD))
    glat_column = jnp.pad(
        glat_grad.reshape(-1, latent_gain.shape[0]), ((0, 0), (0, pad))
    ).reshape(-1)
    lane = jnp.arange(128, dtype=jnp.int32)
    small_grad = jnp.pad(router_grad, ((0, 0), (0, 128 - experts)))
    for at_lane, column in enumerate((gattn_grad, gmoe_grad, glat_column)):
        small_grad = jnp.where(lane == experts + at_lane, column[:, None], small_grad)

    def by_row_owner(value):
        return value.astype(bf16).reshape(replicas, groups, rows, -1)

    ldown_owned, small_owned, h_one_grad = ring_scatter(
        [
            by_row_owner(joint_weight_grad[:, :down_at]),
            by_row_owner(small_grad),
            by_owner(h_one_partial),
        ],
        6,
    )
    normed_own, factor_own = norm_parts(x_low.astype(f32))
    input_grad = x_second_grad + norm_back(h_one_grad * gain_attn, normed_own, factor_own)
    input_grad = input_grad.astype(bf16).reshape(seqs, span, width)
    small_owned = dp_scatter(
        jnp.concatenate([ldown_owned, small_owned], axis=2).reshape(replicas * rows, -1)
    )
    ldown_owned = small_owned[:, :down_at]
    router_owned = small_owned[:, down_at : down_at + experts]
    gain_owned = small_owned[:, down_at + experts :]
    return (
        result,
        input_grad,
        q_owned,
        ldown_owned,
        lup_owned,
        out_owned,
        gain_owned[:, 0],
        gain_owned[: latent_gain.shape[0], 2],
        router_owned,
        sgate_owned,
        sup_owned,
        sdown_owned,
        gain_owned[:, 1],
        routed_gate_grad[None],
        routed_up_grad[None],
        routed_down_grad[None],
    )


def solution(mesh):
    return jax.shard_map(
        per_device,
        mesh=mesh,
        in_specs=(
            TOKENS, P(DP, None), TOKENS, P(DP, EXPERT), TOKENS,
            ROWS, ROWS, ROWS, P(None, BOTH), P(BOTH), P(BOTH),
            ROWS, ROWS, ROWS, ROWS, P(BOTH), ROUTED, ROUTED, ROUTED,
        ),
        out_specs=(
            TOKENS, TOKENS, ROWS, ROWS, ROWS, P(None, BOTH), P(BOTH), P(BOTH),
            ROWS, ROWS, ROWS, ROWS, P(BOTH), ROUTED, ROUTED, ROUTED,
        ),
        check_vma=False,
    )
```

```python
import functools
import math

import jax
import jax.numpy as jnp
from jax import lax
from jax.experimental import pallas as pl
from jax.experimental.pallas import tpu as pltpu
from jax.sharding import PartitionSpec as P

HEADS = 16
HD = 128
RD = 64
VD = 128
RANK = 512
TOP = 6

epsilon = 1e-06
masked_score = -1e30
DP = "dp"
EXPERT = "expert"
BOTH = (DP, EXPERT)
TOKENS = P(DP, EXPERT, None)
ROWS = P(BOTH, None)
ROUTED = P(EXPERT, DP, None)
f32 = jnp.float32
bf16 = jnp.bfloat16


def product(left, right):
    return jnp.dot(left, right, preferred_element_type=f32)


def left_product(left, right):
    return lax.dot_general(left, right, (((0,), (0,)), ((), ())), preferred_element_type=f32)


def right_product(left, right):
    return lax.dot_general(left, right, (((1,), (1,)), ((), ())), preferred_element_type=f32)


def einsum(spec, left, right):
    return jnp.einsum(spec, left, right, preferred_element_type=f32)


def norm_parts(values):
    factor = lax.rsqrt(jnp.mean(values * values, axis=-1, keepdims=True) + epsilon)
    return (values * factor, factor)


def norm_back(grad_normed, normed, factor):
    return factor * (grad_normed - normed * jnp.mean(grad_normed * normed, axis=-1, keepdims=True))


def angle_tables(positions, width):
    half = width // 2
    freqs = jnp.power(10000.0, -2.0 * jnp.arange(half, dtype=f32) / width)
    angles = positions.astype(f32)[:, None] * freqs[None, :]
    return (jnp.cos(angles), jnp.sin(angles))


def silu_slope(pre):
    sigma = jax.nn.sigmoid(pre)
    return sigma * (1.0 + pre * (1.0 - sigma))


def dp_swap(value):
    return lax.ppermute(value, DP, [(0, 1), (1, 0)])


def ordered(value, other):
    first = lax.axis_index(DP) == 0
    return jnp.concatenate(
        [jnp.where(first, value, other), jnp.where(first, other, value)], axis=0
    )


def dp_gather(value):
    if lax.axis_size(DP) == 2:
        return ordered(value, dp_swap(value))
    return lax.all_gather(value, DP, axis=0, tiled=True)


def dp_scatter_product(left, right):
    if lax.axis_size(DP) == 2:
        first = lax.axis_index(DP) == 0
        half = left.shape[1] // 2
        low, high = left[:, :half], left[:, half:]
        sent = left_product(jnp.where(first, high, low), right).astype(bf16)
        other = dp_swap(sent)
        return left_product(jnp.where(first, low, high), right) + other.astype(f32)
    return dp_scatter(left_product(left, right))


def dp_scatter(value):
    if lax.axis_size(DP) == 2:
        rows = value.shape[0] // 2
        at = lax.axis_index(DP)
        sent = lax.dynamic_slice_in_dim(value, (1 - at) * rows, rows, 0)
        kept = lax.dynamic_slice_in_dim(value, at * rows, rows, 0)
        return kept + dp_swap(sent.astype(bf16)).astype(f32)
    return lax.psum_scatter(
        value.astype(bf16), DP, scatter_dimension=0, tiled=True
    ).astype(f32)


def expert_swap(value):
    return lax.all_to_all(value, EXPERT, split_axis=0, concat_axis=0, tiled=True)


def gather_rows(value, axes):
    return lax.all_gather(value, axes, axis=0, tiled=True)


def scatter_rows(value, axes):
    return lax.psum_scatter(value, axes, scatter_dimension=0, tiled=True)


MESH = pl.DeviceIdType.MESH


def at_expert(index):
    return {EXPERT: index}


def grid_place():
    me = lax.axis_index(EXPERT)
    return me, me // 4, (me // 2) % 2, me % 2


def greet_neighbours(me, line, pair, core):
    partner = me + 1 - 2 * core
    mate = me + 2 - 4 * pair
    barrier = pltpu.get_barrier_semaphore()
    for other in (partner, mate):
        pl.semaphore_signal(barrier, inc=1, device_id=at_expert(other), device_id_type=MESH)

    @pl.when(line < 3)
    def _():
        pl.semaphore_signal(barrier, inc=1, device_id=at_expert(me + 4), device_id_type=MESH)

    @pl.when(line > 0)
    def _():
        pl.semaphore_signal(barrier, inc=1, device_id=at_expert(me - 4), device_id_type=MESH)

    pl.semaphore_wait(barrier, 3 + jnp.where((line > 0) & (line < 3), 1, 0))
    return partner, mate


def greet_all(me, mirrored=False):
    barrier = pltpu.get_barrier_semaphore()
    if mirrored:
        other = 1 - lax.axis_index(DP)
        pl.semaphore_signal(barrier, inc=1, device_id={DP: other}, device_id_type=MESH)
    for step in range(1, 16):
        pl.semaphore_signal(
            barrier, inc=1, device_id=at_expert((me + step) % 16), device_id_type=MESH
        )
    pl.semaphore_wait(barrier, 15 + mirrored)


def halves(rows):
    return (pl.ds(0, rows // 2), pl.ds(rows // 2, rows // 2)) if rows % 32 == 0 else (pl.ds(0, rows),)


def gather_kernel(k, m, mirrored, *refs):
    x_refs, swap_refs = refs[:k], refs[k : k + m]
    outs, swap_outs = refs[k + m : 2 * k + m], refs[2 * k + m : 2 * (k + m)]
    mirrors = refs[2 * (k + m) : 2 * (k + m) + m * mirrored]
    own_sem, send_sem, recv_sem, swap_send, swap_recv, mirror_sem = refs[
        2 * (k + m) + m * mirrored :
    ]
    pieces = [
        (a, at)
        for a in range(k)
        for at in (halves(x_refs[a].shape[0]) if len(x_refs[a].shape) == 2 else (None,))
    ]
    n = len(pieces)
    me, line, pair, core = grid_place()
    if m:
        greet_all(me, mirrored)
        partner, mate = me + 1 - 2 * core, me + 2 - 4 * pair
    else:
        partner, mate = greet_neighbours(me, line, pair, core)

    def held(i):
        a, at = pieces[i]
        return x_refs[a] if at is None else x_refs[a].at[at, :]

    def slot(i, origin):
        a, at = pieces[i]
        return outs[a].at[:, origin] if at is None else outs[a].at[origin, at, :]

    def own_copy(i):
        if i < n:
            return pltpu.make_async_copy(held(i), slot(i, me), own_sem.at[i])
        i -= n
        return pltpu.make_async_copy(
            swap_refs[i].at[me], swap_outs[i].at[me], own_sem.at[n + i]
        )

    def copy(i, source, origin, way, to):
        return pltpu.make_async_remote_copy(
            src_ref=source,
            dst_ref=slot(i, origin),
            send_sem=send_sem.at[i, origin, way],
            recv_sem=recv_sem.at[i, origin],
            device_id=at_expert(to),
            device_id_type=MESH,
        )

    def swap_copy(i, step):
        to = (me + step) % 16
        return pltpu.make_async_remote_copy(
            src_ref=swap_refs[i].at[to],
            dst_ref=swap_outs[i].at[me],
            send_sem=swap_send.at[i, step],
            recv_sem=swap_recv.at[i, step],
            device_id=at_expert(to),
            device_id_type=MESH,
        )

    def arrived(i, origin):
        copy(i, slot(i, origin), origin, 0, partner).wait_recv()

    def mirror_copy(i):
        return pltpu.make_async_remote_copy(
            src_ref=swap_outs[i],
            dst_ref=mirrors[i],
            send_sem=mirror_sem.at[i, 0],
            recv_sem=mirror_sem.at[i, 1],
            device_id={DP: 1 - lax.axis_index(DP)},
            device_id_type=MESH,
        )

    def swaps_done():
        for i in range(m):
            for step in range(1, 16):
                swap_copy(i, step).wait_recv()
            own_copy(n + i).wait()
            if mirrored:
                mirror_copy(i).start()

    def along(i, origin, source, upward, downward, act):
        if upward:

            @pl.when(line < 3)
            def _():
                act(copy(i, source, origin, 0, me + 4))

        if downward:

            @pl.when(line > 0)
            def _():
                act(copy(i, source, origin, 1, me - 4))

        act(copy(i, source, origin, 2, mate))
        act(copy(i, source, origin, 3, partner))

    def walk(act, wait, between):
        for far in range(1, 5):
            if far == 3:
                between()
            if far < 4:

                @pl.when(line >= far)
                def _():
                    origin = me - 4 * far
                    for i in range(n):
                        wait(i, origin)
                        along(i, origin, slot(i, origin), True, False, act)

                @pl.when(line + far <= 3)
                def _():
                    origin = me + 4 * far
                    for i in range(n):
                        wait(i, origin)
                        along(i, origin, slot(i, origin), False, True, act)

            for sign in (-1, 1) if far > 1 else (1,):
                step = sign * (far - 1)

                @pl.when((line + step >= 0) & (line + step <= 3))
                def _():
                    origin = mate + 4 * step
                    for i in range(n):
                        wait(i, origin)
                        act(copy(i, slot(i, origin), origin, 3, partner))

    def start(c):
        c.start()

    def sent(c):
        c.wait_send()

    for i in range(n):
        along(i, me, held(i), True, True, start)
    for i in range(m):
        for step in range(1, 16):
            swap_copy(i, step).start()
    for i in range(n + m):
        own_copy(i).start()
    walk(start, arrived, swaps_done)
    for i in range(n):
        for index in range(8):
            arrived(i, 2 * index + 1 - core)
    for i in range(n):
        along(i, me, held(i), True, True, sent)
    walk(sent, lambda i, origin: None, lambda: None)
    for i in range(m):
        for step in range(1, 16):
            swap_copy(i, step).wait_send()
        if mirrored:
            mirror_copy(i).wait()
    for i in range(n):
        own_copy(i).wait()


def ring_gather(values, swaps, collective, mirrored=False):
    k, m = len(values), len(swaps)
    n = sum(len(halves(v.shape[0])) if v.ndim == 2 else 1 for v in values)
    sent = 2 * (15 * sum(v.size for v in values) + sum(v.size for v in swaps))
    sems = pltpu.SemaphoreType.DMA
    anywhere = pl.BlockSpec(memory_space=pl.ANY)
    shapes = [(16,) + v.shape if v.ndim == 2 else v.shape[:1] + (16,) + v.shape[1:] for v in values]
    shapes += [v.shape for v in swaps] * (1 + mirrored)
    outs = pl.pallas_call(
        functools.partial(gather_kernel, k, m, mirrored),
        out_shape=[jax.ShapeDtypeStruct(shape, bf16) for shape in shapes],
        in_specs=[pl.BlockSpec(memory_space=pltpu.VMEM)] * (k + m),
        out_specs=[anywhere] * len(shapes),
        scratch_shapes=[
            sems((n + m,)),
            sems((n, 16, 4)),
            sems((n, 16)),
            sems((max(m, 1), 16)),
            sems((max(m, 1), 16)),
            sems((max(m, 1), 2)),
        ],
        compiler_params=pltpu.CompilerParams(collective_id=collective, has_side_effects=True),
        cost_estimate=pl.CostEstimate(flops=0, bytes_accessed=16 * sent, transcendentals=0),
    )(*values, *swaps)
    return [o.reshape(-1, o.shape[-1]) for o in outs[:k]] + list(outs[k:])


def scatter_pieces(shapes):
    return [
        (a, at)
        for a, shape in enumerate(shapes)
        for at in (halves(shape[0]) if len(shape) == 2 else (None,))
    ]


def scatter_kernel(k, *refs):
    pieces = scatter_pieces([ref.shape for ref in refs[k : 2 * k]])
    n = len(pieces)
    parts = [
        (refs[a], refs[k + a] if at is None else refs[k + a].at[at, :])
        + refs[2 * k + 5 * i : 2 * k + 5 * i + 5]
        for i, (a, at) in enumerate(pieces)
    ]
    (
        core_send, core_recv, mate_send, mate_recv, up_send, up_recv, down_send, down_recv,
    ) = refs[2 * k + 5 * n :]
    me, line, pair, core = grid_place()
    partner, mate = greet_neighbours(me, line, pair, core)

    def block(i, dest):
        ref, at = parts[i][0], pieces[i][1]
        return ref.at[:, dest] if at is None else ref.at[dest, at, :]

    def remote(source, target, send, recv, to):
        return pltpu.make_async_remote_copy(
            src_ref=source, dst_ref=target, send_sem=send, recv_sem=recv,
            device_id=at_expert(to), device_id_type=MESH,
        )

    def core_copy(i, index):
        return remote(
            block(i, 2 * index + 1 - core), parts[i][2].at[index],
            core_send.at[i, index], core_recv.at[i, index], partner,
        )

    def mate_copy(i, dest):
        return remote(
            parts[i][6].at[2 * dest + 1 - pair], parts[i][3].at[dest],
            mate_send.at[i, dest], mate_recv.at[i, dest], mate,
        )

    def up_copy(i, dest):
        return remote(
            parts[i][6].at[2 * dest + pair], parts[i][4].at[dest],
            up_send.at[i, dest], up_recv.at[i, dest], me + 4,
        )

    def down_copy(i, dest):
        return remote(
            parts[i][6].at[2 * dest + pair], parts[i][5].at[dest],
            down_send.at[i, dest], down_recv.at[i, dest], me - 4,
        )

    def add(target, left, right):
        if len(left.shape) == 3:
            for i in range(left.shape[0]):
                add(target.at[i], left.at[i], right.at[i])
            return
        tile = min(16, left.shape[0])

        @pl.loop(0, left.shape[0] // tile)
        def _(i):
            at = pl.ds(pl.multiple_of(i * tile, tile), tile)
            target[at, :] = (left[at, :].astype(f32) + right[at, :].astype(f32)).astype(
                target.dtype
            )

    def farthest(act):
        for far in (3, 2, 1, 0):
            for step in (-far, far) if far else (0,):

                @pl.when((line + step >= 0) & (line + step <= 3))
                def _():
                    for i in range(n):
                        act(i, line + step, step)

    def send_core(i, dest, step):
        core_copy(i, 2 * dest + 1 - pair).start()

    def send_core_own(i, dest, step):
        core_copy(i, 2 * dest + pair).start()

    def chip_sum(i, index):
        core_copy(i, index).wait_recv()
        add(parts[i][6].at[index], block(i, 2 * index + core), parts[i][2].at[index])

    def to_mate(i, dest, step):
        chip_sum(i, 2 * dest + 1 - pair)
        mate_copy(i, dest).start()

    def keep(i, dest, step):
        chip_sum(i, 2 * dest + pair)

    def along(i, dest, step):
        out, up_in, down_in, total = parts[i][1], parts[i][4], parts[i][5], parts[i][6]
        mine = total.at[2 * dest + pair]
        mate_copy(i, dest).wait_recv()
        if step == 0:
            add(out, mine, parts[i][3].at[dest])
            mine = out
        else:
            add(mine, mine, parts[i][3].at[dest])
        if step >= 0:

            @pl.when(line > 0)
            def _():
                up_copy(i, dest).wait_recv()
                add(mine, mine, up_in.at[dest])

        if step <= 0:

            @pl.when(line < 3)
            def _():
                down_copy(i, dest).wait_recv()
                add(mine, mine, down_in.at[dest])

        if step > 0:
            up_copy(i, dest).start()
        elif step < 0:
            down_copy(i, dest).start()

    def finish(i, dest, step):
        mate_copy(i, dest).wait_send()
        core_copy(i, 2 * dest + 1 - pair).wait_send()
        core_copy(i, 2 * dest + pair).wait_send()
        if step > 0:
            up_copy(i, dest).wait_send()
        elif step < 0:
            down_copy(i, dest).wait_send()

    for act in (send_core, send_core_own, to_mate, keep, along, finish):
        farthest(act)


def ring_scatter(values, collective):
    count = len(values)
    shapes = [v.shape[1:] if len(v.shape) == 3 else v.shape[:1] + v.shape[2:] for v in values]
    pieces = scatter_pieces(shapes)
    n = len(pieces)
    parts = [
        shapes[a] if at is None else (at.size,) + shapes[a][1:] for a, at in pieces
    ]
    buffers = [pltpu.VMEM((k,) + s, bf16) for s in parts for k in (8, 4, 4, 4, 8)]
    sent = 30 * sum(math.prod(s) for s in shapes)
    vmem = pl.BlockSpec(memory_space=pltpu.VMEM)
    return pl.pallas_call(
        functools.partial(scatter_kernel, count),
        out_shape=[jax.ShapeDtypeStruct(s, f32) for s in shapes],
        in_specs=[vmem] * count,
        out_specs=[vmem] * count,
        scratch_shapes=buffers
        + [pltpu.SemaphoreType.DMA((n, k)) for k in (8, 8, 4, 4, 4, 4, 4, 4)],
        compiler_params=pltpu.CompilerParams(collective_id=collective, has_side_effects=True),
        cost_estimate=pl.CostEstimate(flops=0, bytes_accessed=16 * sent, transcendentals=0),
    )(*values)


def swap_kernel(source, target, x_ref, out_ref, own_sem, send_sem, recv_sem):
    me = lax.axis_index(EXPERT)
    greet_all(me)

    def copy(step):
        to = (me + step) % 16
        return pltpu.make_async_remote_copy(
            src_ref=source(x_ref, to),
            dst_ref=target(out_ref, me),
            send_sem=send_sem.at[step],
            recv_sem=recv_sem.at[step],
            device_id=at_expert(to),
            device_id_type=MESH,
        )

    for step in range(1, 16):
        copy(step).start()
    own = pltpu.make_async_copy(source(x_ref, me), target(out_ref, me), own_sem)
    own.start()
    for step in range(1, 16):
        copy(step).wait()
    own.wait()


def swap_call(source, target, value, shape, collective):
    sent = value.size * 2
    return pl.pallas_call(
        functools.partial(swap_kernel, source, target),
        out_shape=jax.ShapeDtypeStruct(shape, value.dtype),
        in_specs=[pl.BlockSpec(memory_space=pltpu.VMEM)],
        out_specs=pl.BlockSpec(memory_space=pltpu.VMEM),
        scratch_shapes=[
            pltpu.SemaphoreType.DMA,
            pltpu.SemaphoreType.DMA((16,)),
            pltpu.SemaphoreType.DMA((16,)),
        ],
        compiler_params=pltpu.CompilerParams(collective_id=collective, has_side_effects=True),
        cost_estimate=pl.CostEstimate(flops=0, bytes_accessed=64 * sent, transcendentals=0),
    )(value)


def block_rows(span):
    return lambda ref, at: ref.at[:, pl.ds(pl.multiple_of(at * span, span), span), :]


def head_columns(columns):
    return lambda ref, at: ref.at[:, :, pl.ds(pl.multiple_of(at * columns, columns), columns)]


def heads_to_tokens(value, span, collective):
    seqs = value.shape[0]
    return swap_call(
        block_rows(span), head_columns(VD), value, (seqs, span, HEADS * VD), collective
    )


def tokens_to_heads(value, collective):
    seqs, span, _ = value.shape
    return swap_call(
        head_columns(VD), block_rows(span), value, (seqs, span * HEADS, VD), collective
    )


def matmul(left, right, dims):
    return lax.dot_general(left, right, (dims, ((), ())), preferred_element_type=f32)


ROWS_ROWS = ((0,), (0,))
COLS_COLS = ((1,), (1,))
COLS_ROWS = ((1,), (0,))


def full(shape):
    return pl.BlockSpec(shape, lambda *_: (0,) * len(shape), pipeline_mode=pl.Buffered(1))


def tiled(rows, columns):
    return pl.BlockSpec((rows, columns), lambda i: (i, 0))


def estimate(flops, nbytes):
    return pl.CostEstimate(
        flops=int(flops), bytes_accessed=int(nbytes), transcendentals=0
    )


def combine_kernel(dims, select_ref, slot_ref, left_ref, right_ref, out_ref):
    routed = matmul(select_ref[0], slot_ref[0], ROWS_ROWS)
    out_ref[...] = (routed + matmul(left_ref[...], right_ref[...], dims)).astype(bf16)


def combine(select, slot_rows, left, right, dims):
    chunks, slots, chunk = select.shape
    width = slot_rows.shape[-1]
    tile = 256
    per = chunk // tile
    inner = left.shape[1]
    return pl.pallas_call(
        functools.partial(combine_kernel, dims),
        grid=(chunks, per),
        in_specs=[
            pl.BlockSpec((1, slots, tile), lambda c, t: (c, 0, t)),
            pl.BlockSpec((1, slots, width), lambda c, t: (c, 0, 0)),
            pl.BlockSpec((tile, inner), lambda c, t: (c * per + t, 0)),
            full(right.shape),
        ],
        out_specs=pl.BlockSpec((tile, width), lambda c, t: (c * per + t, 0)),
        out_shape=jax.ShapeDtypeStruct((chunks * chunk, width), bf16),
        cost_estimate=estimate(
            2 * chunks * chunk * width * (slots + inner), 4 * chunks * chunk * width
        ),
    )(select, slot_rows.reshape(chunks, slots, width), left, right)


def turn(values, cosine, sine):
    lane = lax.broadcasted_iota(jnp.int32, values.shape, 1)
    other = jnp.where(lane % 64 < 32, pltpu.roll(values, 96, 1), pltpu.roll(values, 32, 1))
    return values * cosine + other * sine


def project_kernel(
    x_ref, down_ref, weight_ref, lup_ref, gain_ref, gain_lat_ref, cos_ref, sin_ref,
    h_ref, query_ref, key_ref, value_ref, latent_ref, normed_ref, factor_ref,
):
    x = x_ref[...].astype(f32)
    factor = lax.rsqrt(jnp.mean(x * x, axis=-1, keepdims=True) + epsilon)
    h = (x * factor * gain_ref[...]).astype(bf16)
    h_ref[...] = h
    raw = matmul(h, down_ref[...], COLS_ROWS)
    low = raw[:, :RANK]
    factor = lax.rsqrt(jnp.mean(low * low, axis=-1, keepdims=True) + epsilon)
    normed = low * factor
    normed_ref[...] = normed
    factor_ref[...] = factor
    latent = (normed * gain_lat_ref[...]).astype(bf16)
    latent_ref[...] = latent
    expanded = matmul(latent, lup_ref[...], COLS_ROWS)
    rope = turn(raw[:, RANK : RANK + 128], cos_ref[...], sin_ref[...])
    lane = lax.broadcasted_iota(jnp.int32, rope.shape, 1)
    raw = matmul(h, weight_ref[...], COLS_ROWS)
    query_ref[:, :HD] = raw[:, :HD].astype(bf16)
    query_ref[:, HD:] = turn(raw[:, HD:], cos_ref[...], sin_ref[...]).astype(bf16)
    key_ref[:, :HD] = expanded[:, :HD].astype(bf16)
    key_ref[:, HD:] = jnp.where(lane < RD, rope, 0.0).astype(bf16)
    value_ref[...] = expanded[:, HD:].astype(bf16)


def project(x_all, down, weight, lup, gain, gain_lat, cosine, sine):
    tokens, width = x_all.shape
    tile = 256
    outs = [
        ((tokens, width), bf16),
        ((tokens, HD + 128), bf16),
        ((tokens, HD + 128), bf16),
        ((tokens, VD), bf16),
        ((tokens, RANK), bf16),
        ((tokens, RANK), f32),
        ((tokens, 1), f32),
    ]
    return pl.pallas_call(
        project_kernel,
        name="project",
        grid=(tokens // tile,),
        in_specs=[
            tiled(tile, width),
            full(down.shape),
            full(weight.shape),
            full(lup.shape),
            full((1, width)),
            full((1, RANK)),
            tiled(tile, 128),
            tiled(tile, 128),
        ],
        out_specs=[tiled(tile, s[1]) for s, _ in outs],
        out_shape=[jax.ShapeDtypeStruct(s, d) for s, d in outs],
        cost_estimate=estimate(2 * tokens * width * 1000, 5 * tokens * width),
    )(x_all, down, weight, lup, gain[None], gain_lat[None], cosine, sine)


def attend_kernel(scale, query_ref, key_ref, value_ref, row_ref, col_ref, probs_ref, out_ref):
    length = probs_ref.shape[1]
    tile = 256
    query = query_ref[...].reshape(length, -1)
    key = key_ref[...].reshape(length, -1)
    value = value_ref[...].reshape(length, -1)
    for at in range(0, length, tile):
        seen = at + tile
        scores = matmul(query[at:seen], key[:seen], COLS_COLS) * scale
        row = at + lax.broadcasted_iota(jnp.int32, scores.shape, 0)
        col = lax.broadcasted_iota(jnp.int32, scores.shape, 1)
        keep = (col <= row) & (row_ref[0, :, :seen] == col_ref[0, at:seen, :])
        scores = jnp.where(keep, scores, masked_score)
        weights = jnp.exp(scores - jnp.max(scores, axis=-1, keepdims=True))
        probs = (weights / jnp.sum(weights, axis=-1, keepdims=True)).astype(bf16)
        probs_ref[0, at:seen, :seen] = probs
        if seen < length:
            probs_ref[0, at:seen, seen:] = jnp.zeros((tile, length - seen), bf16)
        out_ref[0, at:seen, :] = matmul(probs, value[:seen], COLS_ROWS).astype(bf16)


def of_sequence(groups, span, columns):
    return pl.BlockSpec((groups, 1, span, columns), lambda s: (0, s, 0, 0))


def attend(query, key, value, segments, scale, groups, seqs, span):
    length = groups * span
    view = lambda v: v.reshape(groups, seqs, span, -1)
    return pl.pallas_call(
        functools.partial(attend_kernel, scale),
        name="attend",
        grid=(seqs,),
        in_specs=[
            of_sequence(groups, span, HD + 128),
            of_sequence(groups, span, HD + 128),
            of_sequence(groups, span, VD),
            pl.BlockSpec((1, 1, length), lambda s: (s, 0, 0)),
            pl.BlockSpec((1, length, 1), lambda s: (s, 0, 0)),
        ],
        out_specs=[
            pl.BlockSpec((1, length, length), lambda s: (s, 0, 0)),
            pl.BlockSpec((1, length, VD), lambda s: (s, 0, 0)),
        ],
        out_shape=[
            jax.ShapeDtypeStruct((seqs, length, length), bf16),
            jax.ShapeDtypeStruct((seqs, length, VD), bf16),
        ],
        cost_estimate=estimate(seqs * length * length * 500, seqs * length * length * 4),
    )(view(query), view(key), view(value), segments[:, None, :], segments[:, :, None])


def attend_back_kernel(
    scale, probs_ref, grad_ref, out_ref, query_ref, key_ref, value_ref, dq_ref, dkv_ref, acc_ref
):
    length = probs_ref.shape[1]
    tile = 256
    _, _, span, _ = query_ref.shape
    per = tile // span
    query = query_ref[...].reshape(length, -1)
    key = key_ref[...].reshape(length, -1)
    value = value_ref[...].reshape(length, -1)
    wide = query.shape[1]
    for at in reversed(range(0, length, tile)):
        seen = at + tile
        grad = grad_ref[0, at:seen, :]
        spread = jnp.sum(
            grad.astype(f32) * out_ref[0, at:seen, :].astype(f32), axis=-1, keepdims=True
        )
        probs = probs_ref[0, at:seen, :seen]
        back = matmul(grad, value[:seen], COLS_COLS) - spread
        score_grad = (probs.astype(f32) * back * scale).astype(bf16)
        dq = matmul(score_grad, key[:seen], COLS_ROWS)
        dq_ref[at // span : seen // span, 0] = dq.reshape(per, span, wide)
        dk = matmul(score_grad, query[at:seen], ROWS_ROWS)
        dv = matmul(probs, grad, ROWS_ROWS)
        if seen == length:
            acc_ref[:, :wide] = dk
            acc_ref[:, wide:] = dv
        else:
            acc_ref[:seen, :wide] += dk
            acc_ref[:seen, wide:] += dv
    dkv_ref[...] = acc_ref[...].reshape(dkv_ref.shape)


def attend_back(probs, grad, out, query, key, value, scale, groups, span):
    seqs, length, _ = probs.shape
    wide = HD + 128
    view = lambda v: v.reshape(groups, seqs, span, -1)
    by_seq = lambda n: pl.BlockSpec((1, length, n), lambda s: (s, 0, 0))
    dq, dkv = pl.pallas_call(
        functools.partial(attend_back_kernel, scale),
        name="attend_back",
        grid=(seqs,),
        in_specs=[
            by_seq(length),
            by_seq(VD),
            by_seq(VD),
            of_sequence(groups, span, wide),
            of_sequence(groups, span, wide),
            of_sequence(groups, span, VD),
        ],
        out_specs=[of_sequence(groups, span, wide), of_sequence(groups, span, wide + VD)],
        out_shape=[
            jax.ShapeDtypeStruct((groups, seqs, span, wide), f32),
            jax.ShapeDtypeStruct((groups, seqs, span, wide + VD), f32),
        ],
        scratch_shapes=[pltpu.VMEM((length, wide + VD), f32)],
        cost_estimate=estimate(seqs * length * length * 1000, seqs * length * length * 4),
    )(probs, grad, out, view(query), view(key), view(value))
    return dq.reshape(-1, wide), dkv.reshape(-1, wide + VD)


def project_back_kernel(
    dq_ref, dkv_ref, down_ref, weight_ref, lup_ref, gain_lat_ref, cos_ref, sin_ref,
    latent_ref, normed_ref, factor_ref, down_grad_ref, query_grad_ref, h_ref, lup_grad_ref, gain_grad_ref,
):
    dq = dq_ref[...]
    dkv = dkv_ref[...]
    key_rope = turn(dkv[:, HD : HD + 128], cos_ref[...], -sin_ref[...])
    query_rope = turn(dq[:, HD:], cos_ref[...], -sin_ref[...])
    expanded = jnp.concatenate([dkv[:, :HD], dkv[:, HD + 128 :]], axis=1).astype(bf16)
    latent_grad = matmul(expanded, lup_ref[...], COLS_COLS)
    normed = normed_ref[...]

    @pl.when(pl.program_id(0) == 0)
    def _():
        lup_grad_ref[...] = jnp.zeros_like(lup_grad_ref)
        gain_grad_ref[...] = jnp.zeros_like(gain_grad_ref)

    lup_grad_ref[...] += matmul(latent_ref[...], expanded, ROWS_ROWS)
    gain_grad_ref[...] += jnp.sum(latent_grad * normed, axis=0, keepdims=True)
    scaled = latent_grad * gain_lat_ref[...]
    down = factor_ref[...] * (
        scaled - normed * jnp.mean(scaled * normed, axis=-1, keepdims=True)
    )
    down = jnp.concatenate([down, key_rope], axis=1).astype(bf16)
    query = jnp.concatenate([dq[:, :HD], query_rope], axis=1).astype(bf16)
    down_grad_ref[...] = down
    query_grad_ref[...] = query
    back = matmul(down, down_ref[...], COLS_COLS) + matmul(query, weight_ref[...], COLS_COLS)
    h_ref[...] = back.astype(bf16)


def project_back(dq, dkv, down, weight, lup, gain_lat, cosine, sine, latent, normed, factor):
    tokens = dq.shape[0]
    width = weight.shape[0]
    tile = 256
    return pl.pallas_call(
        project_back_kernel,
        name="project_back",
        grid=(tokens // tile,),
        in_specs=[
            tiled(tile, dq.shape[1]),
            tiled(tile, dkv.shape[1]),
            full(down.shape),
            full(weight.shape),
            full(lup.shape),
            full((1, RANK)),
            tiled(tile, 128),
            tiled(tile, 128),
            tiled(tile, RANK),
            tiled(tile, RANK),
            tiled(tile, 1),
        ],
        out_specs=[
            tiled(tile, down.shape[1]),
            tiled(tile, weight.shape[1]),
            tiled(tile, width),
            pl.BlockSpec(lup.shape, lambda i: (0, 0)),
            pl.BlockSpec((1, RANK), lambda i: (0, 0)),
        ],
        out_shape=[
            jax.ShapeDtypeStruct((tokens, down.shape[1]), bf16),
            jax.ShapeDtypeStruct((tokens, weight.shape[1]), bf16),
            jax.ShapeDtypeStruct((tokens, width), bf16),
            jax.ShapeDtypeStruct(lup.shape, f32),
            jax.ShapeDtypeStruct((1, RANK), f32),
        ],
        cost_estimate=estimate(2 * tokens * width * 1000, 6 * tokens * width),
    )(dq, dkv, down, weight, lup, gain_lat[None], cosine, sine, latent, normed, factor)


def per_device(
    inputs,
    segments,
    expert_picks,
    priority,
    cotangent,
    query_weight,
    latent_down,
    latent_up,
    output_weight,
    attn_gain,
    latent_gain,
    router_weight,
    shared_gate,
    shared_up,
    shared_down,
    moe_gain,
    expert_gate,
    expert_up,
    expert_down,
):
    groups = lax.axis_size(EXPERT)
    replicas = lax.axis_size(DP)
    place = lax.axis_index(EXPERT)
    seqs, span, width = inputs.shape
    own = seqs * span
    tokens = own * groups
    experts = groups
    capacity = (9 * span * TOP + 8 * experts - 1) // (8 * experts)
    scale = 1.0 / math.sqrt(HD + RD)
    rows = query_weight.shape[0]
    part = shared_down.shape[0]
    hidden_own = part * replicas
    QD = HD + RD

    def by_owner(value):
        return value.astype(bf16).reshape(groups, own, -1)

    def by_block(value):
        return value.reshape(seqs, groups, span, -1).transpose(1, 0, 2, 3).reshape(tokens, -1)

    x_low = inputs.reshape(own, width)
    cot_own = cotangent.reshape(own, width)

    order = priority[:, None, :] < priority[:, :, None]
    hit = jnp.sum(
        (expert_picks[..., None] == jnp.arange(experts, dtype=jnp.int32)).astype(f32), axis=2
    )
    ranks = einsum("stu,sue->ste", order.astype(bf16), hit.astype(bf16))
    codes = jnp.where((hit > 0) & (ranks < capacity), ranks, -1.0).astype(bf16)

    pad = rows - latent_gain.shape[0]
    small = jnp.concatenate(
        [
            latent_down,
            router_weight,
            attn_gain[:, None],
            moe_gain[:, None],
            jnp.pad(latent_gain, (0, pad))[:, None],
            jnp.zeros((rows, 45), bf16),
        ],
        axis=1,
    )
    small = dp_gather(small).reshape(replicas, rows, -1)
    query_parts = query_weight.reshape(rows, HEADS, QD).transpose(1, 0, 2)
    lup_rows = latent_up.shape[0]
    code_rows = -(lup_rows + 1) % 16 + 1
    code_part = jnp.pad(
        codes.reshape(own, 1, experts).T, ((0, 0), (0, code_rows - 1), (0, HD + VD - own))
    )
    lup_parts = jnp.concatenate(
        [latent_up.reshape(lup_rows, HEADS, HD + VD).transpose(1, 0, 2), code_part], axis=1
    )
    small_all, x_all, *swapped = ring_gather(
        [small, x_low], [query_parts, lup_parts], 1, replicas == 2
    )
    router_all = small_all[:, RANK + RD : RANK + RD + experts]
    gains = small_all[:, RANK + RD + experts :].astype(f32)
    gain_attn = gains[:, 0]
    gain_moe = gains[:, 1]
    gain_lat = gains[:, 2].reshape(-1, rows)[:, : latent_gain.shape[0]].reshape(-1)

    def all_rows(at, cut):
        value = swapped[at][:, :cut].reshape(groups * cut, -1)
        if replicas != 2:
            return dp_gather(value)
        return ordered(value, swapped[at + 2][:, :cut].reshape(groups * cut, -1))

    wq = jnp.pad(all_rows(0, rows), ((0, 0), (0, 128 - RD)))
    lup = all_rows(1, lup_rows)
    code = swapped[1][:, lup_rows, :own].astype(f32).reshape(tokens)

    def columns_of(weight):
        return (
            weight.reshape(rows, replicas, groups, part)
            .transpose(2, 0, 1, 3)
            .reshape(groups, rows, hidden_own)
        )

    gate_up_parts = jnp.concatenate([columns_of(shared_gate), columns_of(shared_up)], axis=2)
    gate_up_swap = expert_swap(gate_up_parts)
    gate_up = dp_gather(gate_up_swap.reshape(groups * rows, 2 * hidden_own))
    gate_up_router = jnp.concatenate([gate_up, router_all], axis=1)
    sdown = dp_gather(shared_down)
    gate_w = dp_gather(expert_gate[0])
    up_w = dp_gather(expert_up[0])
    down_w = dp_gather(expert_down[0])
    out_rows = dp_gather(output_weight.T)
    out_t = gather_rows(out_rows, EXPERT)

    at_block = jnp.arange(groups, dtype=jnp.int32)[:, None, None] * span
    positions = jnp.broadcast_to(
        at_block + jnp.arange(span, dtype=jnp.int32), (groups, seqs, span)
    ).reshape(tokens)
    cosine, sine = angle_tables(positions, RD)
    cosine = jnp.concatenate([cosine] * 4, axis=1)
    sine = jnp.concatenate([-sine, sine] * 2, axis=1)
    h_one, query, key, value, latent, normed_lat, factor_lat = project(
        x_all, small_all, wq, lup, gain_attn, gain_lat, cosine, sine
    )
    probs_attn, heads_s = attend(query, key, value, segments, scale, groups, seqs, span)
    heads_own = heads_to_tokens(heads_s, span, 3).reshape(own, HEADS * VD)

    x_second = x_low.astype(f32) + right_product(heads_own, out_t).reshape(
        own, groups, replicas, rows
    ).transpose(0, 2, 1, 3).reshape(own, width)
    normed_two, factor_two = norm_parts(x_second)
    (h_two,) = ring_gather([(normed_two * gain_moe).astype(bf16)], [], 2)

    cot_all = gather_rows(cot_own, EXPERT)

    chunks = 4
    chunk = tokens // chunks
    blocks = chunk // span
    slots = blocks * capacity
    slot_at = jnp.arange(slots, dtype=jnp.int32)
    token_at = jnp.arange(chunk, dtype=jnp.int32)
    select = (
        (slot_at[:, None] // capacity == token_at[None, :] // span)[None]
        & (
            (slot_at % capacity).astype(f32)[None, :, None]
            == code.reshape(chunks, chunk)[:, None, :]
        )
    ).astype(bf16)
    select = lax.optimization_barrier(select)

    def to_slots(values):
        return einsum("cst,ctd->csd", select, values.reshape(chunks, chunk, -1)).astype(bf16).reshape(
            chunks * slots, -1
        )

    pre = product(h_two, gate_up_router)
    shared_a = pre[:, :hidden_own]
    shared_b = pre[:, hidden_own : 2 * hidden_own]
    gate_probs = jax.nn.softmax(pre[:, 2 * hidden_own :], axis=-1)
    shared_hidden = (jax.nn.silu(shared_a) * shared_b).astype(bf16)
    mine = (jnp.arange(experts, dtype=jnp.int32) == place).astype(f32)
    own_prob = jnp.sum(gate_probs * mine, axis=-1)
    slot_prob = jnp.sum(
        select.astype(f32) * own_prob.reshape(chunks, 1, chunk), axis=-1
    ).reshape(chunks * slots, 1)
    expert_in = to_slots(h_two)
    gate_pre = product(expert_in, gate_w)
    up_pre = product(expert_in, up_w)
    expert_hidden = (jax.nn.silu(gate_pre) * up_pre).astype(bf16)
    expert_out = product(expert_hidden, down_w).astype(bf16)
    expert_out = lax.optimization_barrier(expert_out).astype(f32)
    partial = combine(
        select, (slot_prob * expert_out).astype(bf16), shared_hidden, sdown, COLS_ROWS
    )
    result = x_second + scatter_rows(partial, EXPERT).astype(f32)
    result = result.astype(bf16).reshape(seqs, span, width)

    grad_slots = to_slots(cot_all)
    hidden_grad = right_product(cot_all, sdown)
    sdown_grad = left_product(shared_hidden, cot_all)
    shared_a_grad = (hidden_grad * shared_b * silu_slope(shared_a)).astype(bf16)
    shared_b_grad = (hidden_grad * jax.nn.silu(shared_a)).astype(bf16)
    grad_wide = grad_slots.astype(f32)
    slot_grad = (slot_prob * grad_wide).astype(bf16)
    match = jnp.sum(grad_wide * expert_out, axis=-1).reshape(chunks, slots, 1)
    prob_grad = jnp.sum(select.astype(f32) * match, axis=1).reshape(tokens, 1)
    logit_grad = (gate_probs * prob_grad * (mine - own_prob[:, None])).astype(bf16)
    pre_grad = jnp.concatenate([shared_a_grad, shared_b_grad, logit_grad], axis=1)
    expert_hidden_grad = right_product(slot_grad, down_w)
    expert_a_grad = (expert_hidden_grad * up_pre * silu_slope(gate_pre)).astype(bf16)
    expert_b_grad = (expert_hidden_grad * jax.nn.silu(gate_pre)).astype(bf16)
    in_grad = right_product(expert_a_grad, gate_w) + right_product(expert_b_grad, up_w)
    in_grad = in_grad.astype(bf16)
    h_two_partial = combine(select, in_grad, pre_grad, gate_up_router, COLS_COLS)
    routed_down_grad = dp_scatter_product(expert_hidden, slot_grad)
    routed_gate_grad = dp_scatter_product(expert_in, expert_a_grad)
    routed_up_grad = dp_scatter_product(expert_in, expert_b_grad)
    (h_two_grad,) = ring_scatter([by_owner(h_two_partial)], 4)
    pre_weight_grad = left_product(h_two, pre_grad)
    sdown_owned = dp_scatter(sdown_grad)
    gate_up_owned = dp_scatter(pre_weight_grad[:, : 2 * hidden_own]).astype(bf16)
    router_grad = pre_weight_grad[:, 2 * hidden_own :]

    gmoe_grad = jnp.sum(h_two_grad * normed_two, axis=0)
    x_second_grad = cot_own.astype(f32) + norm_back(h_two_grad * gain_moe, normed_two, factor_two)
    attn_low = x_second_grad.astype(bf16)
    low_parts = attn_low.reshape(own, replicas, groups, rows).transpose(0, 2, 1, 3)
    heads_grad = product(low_parts.reshape(own, width), out_t).astype(bf16)
    grad_s = tokens_to_heads(heads_grad.reshape(seqs, span, HEADS * VD), 5)
    low_all = gather_rows(attn_low, EXPERT)
    gate_up_owned = expert_swap(
        gate_up_owned.reshape(groups, rows, 2 * hidden_own)
    )

    def owned_columns(value):
        return (
            value.reshape(groups, rows, replicas, part)
            .transpose(1, 2, 0, 3)
            .reshape(rows, replicas * groups * part)
        )

    sgate_owned = owned_columns(gate_up_owned[:, :, :hidden_own]).astype(f32)
    sup_owned = owned_columns(gate_up_owned[:, :, hidden_own:]).astype(f32)
    query_grad, pair_grad = attend_back(
        probs_attn, grad_s, heads_s, query, key, value, scale, groups, span
    )
    down_grad, head_grad, h_one_partial, lup_grad, glat_grad = project_back(
        query_grad, pair_grad, small_all, wq, lup, gain_lat, cosine, sine,
        latent, normed_lat, factor_lat,
    )
    small_grad = left_product(h_one, down_grad)
    head_grad = left_product(h_one, head_grad)
    gattn_grad = jnp.sum(small_grad * small_all.astype(f32), axis=1)
    gattn_grad = (gattn_grad + jnp.sum(head_grad * wq.astype(f32), axis=1)) / gain_attn
    out_grad = left_product(low_all, by_block(heads_s))
    down_at = RANK + RD
    back_grad = jnp.concatenate(
        [
            head_grad[:, :HD],
            out_grad,
            head_grad[:, HD : HD + RD],
            lup_grad.reshape(width, -1),
        ],
        axis=1,
    )
    back_grad = dp_scatter(back_grad).astype(bf16)
    back_owned = expert_swap(back_grad.reshape(groups, rows, -1)).astype(f32)
    q_owned = jnp.concatenate(
        [back_owned[:, :, :HD], back_owned[:, :, HD + VD : HD + VD + RD]], axis=2
    )
    q_owned = q_owned.transpose(1, 0, 2).reshape(rows, HEADS * QD)
    out_owned = back_owned[:, :, HD : HD + VD].transpose(0, 2, 1).reshape(HEADS * VD, rows)
    lup_owned = back_owned[:, :, HD + VD + RD :].reshape(groups, lup_rows, HD + VD)
    lup_owned = lup_owned.transpose(1, 0, 2).reshape(lup_rows, HEADS * (HD + VD))
    glat_column = jnp.pad(
        glat_grad.reshape(-1, latent_gain.shape[0]), ((0, 0), (0, pad))
    ).reshape(-1)
    lane = jnp.arange(small_grad.shape[1], dtype=jnp.int32)
    small_grad = small_grad + jnp.pad(
        router_grad, ((0, 0), (down_at, small_grad.shape[1] - down_at - experts))
    )
    for at_lane, column in enumerate((gattn_grad, gmoe_grad, glat_column)):
        small_grad = jnp.where(lane == down_at + experts + at_lane, column[:, None], small_grad)

    def by_row_owner(value):
        return value.astype(bf16).reshape(replicas, groups, rows, -1)

    small_owned, h_one_grad = ring_scatter([by_row_owner(small_grad), by_owner(h_one_partial)], 6)
    normed_own, factor_own = norm_parts(x_low.astype(f32))
    input_grad = x_second_grad + norm_back(h_one_grad * gain_attn, normed_own, factor_own)
    input_grad = input_grad.astype(bf16).reshape(seqs, span, width)
    small_owned = dp_scatter(small_owned.reshape(replicas * rows, -1))
    ldown_owned = small_owned[:, :down_at]
    router_owned = small_owned[:, down_at : down_at + experts]
    gain_owned = small_owned[:, down_at + experts :]
    return (
        result,
        input_grad,
        q_owned,
        ldown_owned,
        lup_owned,
        out_owned,
        gain_owned[:, 0],
        gain_owned[: latent_gain.shape[0], 2],
        router_owned,
        sgate_owned,
        sup_owned,
        sdown_owned,
        gain_owned[:, 1],
        routed_gate_grad[None],
        routed_up_grad[None],
        routed_down_grad[None],
    )


def solution(mesh):
    return jax.shard_map(
        per_device,
        mesh=mesh,
        in_specs=(
            TOKENS, P(DP, None), TOKENS, P(DP, EXPERT), TOKENS,
            ROWS, ROWS, ROWS, P(None, BOTH), P(BOTH), P(BOTH),
            ROWS, ROWS, ROWS, ROWS, P(BOTH), ROUTED, ROUTED, ROUTED,
        ),
        out_specs=(
            TOKENS, TOKENS, ROWS, ROWS, ROWS, P(None, BOTH), P(BOTH), P(BOTH),
            ROWS, ROWS, ROWS, ROWS, P(BOTH), ROUTED, ROUTED, ROUTED,
        ),
        check_vma=False,
    )
```
